32 devices in a mesh: dp: 4 (over y, core), mp: 8 (over z, x).
Axes of the slice: x: 2, y: 2, z: 4, core: 2. Of those that a mesh axis runs over, the one named last changes fastest.
Arguments:
- tokens: bfloat16 [9216, 1024], P(('dp', 'mp')), may hold values from -6 to 6
- image_ids: int32 [9216], P('dp'), may hold values from 0 to 1, as said below
- lengths: int32 [4, 2], P('dp'), may hold values from 0 to 2304, as said below
- w_qkv: bfloat16 [3, 1024, 1024], P(None, None, 'mp'), may hold values from -0.1875 to 0.1875
- bias_query: float32 [1024], P('mp'), may hold values from -3 to 3
- bias_value: float32 [1024], P('mp'), may hold values from -0.3 to 0.3
- w_out: bfloat16 [1024, 1024], P('mp'), may hold values from -3 to 3
- w_up: bfloat16 [1024, 4096], P(None, 'mp'), may hold values from -0.1875 to 0.1875
- bias_up: float32 [4096], P('mp'), may hold values from -3 to 3
- w_down: bfloat16 [4096, 1024], P('mp'), may hold values from -0.09375 to 0.09375
- out_biases: float32 [2, 1024], replicated, may hold values from -2 to 2
- norm_gain: float32 [2, 1024], replicated, may hold values from 0.25 to 1.75
- norm_bias: float32 [2, 1024], replicated, may hold values from -2 to 2
- cotangent: bfloat16 [9216, 1024], P(('dp', 'mp')), may hold values from -6 to 6
Outputs:
- output: bfloat16 [9216, 1024], P(('dp', 'mp'))
- input_grad: bfloat16 [9216, 1024], P(('dp', 'mp'))
- grad_w_qkv: float32 [3, 1024, 1024], P(None, None, 'mp')
- grad_bias_query: float32 [1024], P('mp')
- grad_bias_value: float32 [1024], P('mp')
- grad_w_out: float32 [1024, 1024], P('mp')
- grad_w_up: float32 [1024, 4096], P(None, 'mp')
- grad_bias_up: float32 [4096], P('mp')
- grad_w_down: float32 [4096, 1024], P('mp')
- grad_out_biases: float32 [2, 1024], replicated
- grad_norm_gain: float32 [2, 1024], replicated
- grad_norm_bias: float32 [2, 1024], replicated
The draws below stay inside these ranges and needn't reach their ends.
Inputs may be any that keep to these rules, and one draw needn't show every extreme that they name: `image_ids`: within each group of 2304 rows (one group for each index of dp) the image numbers never fall: a group holds either one image over all its rows, or two images of 1152 rows each. lengths[g, k] counts the valid rows at the start of image k of group g: 2304 for an image that fills its group (the second entry is then 0), else 1024. Some group holds an image of 2304 rows.
All inputs are finite; a program needn't handle non-finite values.
Results may differ from the reference program's by a relative error of at most 0.02.
Values may be sent and summed in bfloat16 or wider, within the bound.
A program may use at most 128 MiB of HBM per device.

```python
import jax
import jax.numpy as jnp
from jax import lax

D = 1024
HEADS = 16
HEAD_DIM = 64
FF = 4096
SHORT = 1024
BLOCK = 768
SLOT = 1152
LONG = 2304
ROWS = 2304
TOKENS = 9216
N_DP = 4


def group_layout(key):
    kind_key = jax.random.fold_in(key, 11)
    pick_key = jax.random.fold_in(key, 12)
    layout = jax.random.randint(kind_key, (N_DP,), 0, 2)
    forced = jax.random.randint(pick_key, (), 0, N_DP)
    return jnp.where(jnp.arange(N_DP) == forced, 1, layout).astype(jnp.int32)


def draw_image_ids(key, part):
    layout = group_layout(key)
    slot_of_row = (jnp.arange(ROWS, dtype=jnp.int32) // SLOT).astype(jnp.int32)
    image_numbers = jnp.where(layout[:, None] == 1, 0, slot_of_row[None, :])
    return image_numbers.reshape(N_DP * ROWS).astype(jnp.int32)


def draw_lengths(key, part):
    layout = group_layout(key)
    long_entry = jnp.array([LONG, 0], dtype=jnp.int32)
    short_entry = jnp.array([SHORT, SHORT], dtype=jnp.int32)
    return jnp.where(layout[:, None] == 1, long_entry[None, :], short_entry[None, :]).astype(jnp.int32)


def level_of(stream_key, shape, shards, smallest, top_value):
    def one(position, blocks):
        draws = jax.random.uniform(jax.random.fold_in(jax.random.fold_in(stream_key, 6), position), (blocks,), jnp.float32, smallest / len(shards), top_value / len(shards))
        return jnp.repeat(jnp.exp(draws), shape[position] // blocks).reshape((-1,) + (1,) * (len(shape) - position - 1))

    loudness = one(*shards[0])
    for cut in shards[1:]:
        loudness = loudness * one(*cut)
    return loudness


def bell_draw(key, extent, deviation, bound, cuts=(), held_as=jnp.bfloat16):
    factor_of = level_of(key, extent, cuts, -0.22, 0.18) if cuts else 1.0
    drawn = jax.random.normal(key, extent, jnp.float32) * deviation * factor_of
    return jnp.minimum(jnp.maximum(drawn, -bound), bound).astype(held_as)


def setup_inputs(seed: int = 0) -> dict:
    key_of = jax.random.split(jax.random.key(seed), 15)
    tokens = bell_draw(key_of[0], (TOKENS, D), 1.0, 6.0, ((0, 32),))
    image_ids = draw_image_ids(jax.random.fold_in(key_of[14], 71), 0)
    lengths = draw_lengths(jax.random.fold_in(key_of[14], 71), 0)
    w_qkv = bell_draw(key_of[3], (3, D, D), D ** -0.5, 0.1875, ((2, 8),))
    bias_query = bell_draw(key_of[4], (D,), 0.5, 3.0, ((0, 8),), jnp.float32)
    bias_value = bell_draw(key_of[5], (D,), 0.05, 0.3, ((0, 8),), jnp.float32)
    w_out = bell_draw(key_of[6], (D, D), 4 ** -0.5, 3.0, ((0, 8),))
    w_up = bell_draw(key_of[7], (D, FF), D ** -0.5, 0.1875, ((1, 8),))
    bias_up = bell_draw(key_of[8], (FF,), 0.5, 3.0, ((0, 8),), jnp.float32)
    w_down = bell_draw(key_of[9], (FF, D), FF ** -0.5, 0.09375, ((0, 8),))
    out_biases = bell_draw(key_of[10], (2, D), 0.3, 2.0, (), jnp.float32)
    norm_gain = jnp.clip(1.0 + 0.15 * jax.random.normal(key_of[11], (2, D), jnp.float32), 0.25, 1.75)
    norm_bias = bell_draw(key_of[12], (2, D), 0.3, 2.0, (), jnp.float32)
    cotangent = bell_draw(key_of[13], (TOKENS, D), 1.0, 6.0, ((0, 32),))
    return {"tokens": tokens, "image_ids": image_ids, "lengths": lengths, "w_qkv": w_qkv, "bias_query": bias_query, "bias_value": bias_value, "w_out": w_out, "w_up": w_up, "bias_up": bias_up, "w_down": w_down, "out_biases": out_biases, "norm_gain": norm_gain, "norm_bias": norm_bias, "cotangent": cotangent}


@jax.custom_vjp
def low(v):
    return lax.optimization_barrier(v.astype(jnp.bfloat16)).astype(jnp.float32)

@jax.custom_vjp
def low_back(v):
    return v

def low_keep(v):
    return (low(v), None)

def low_pass(kept, grad):
    return (grad,)

def back_keep(v):
    return (v, None)

def back_low(kept, grad):
    return (low(grad),)
low.defvjp(low_keep, low_pass)
low_back.defvjp(back_keep, back_low)
epsilon = 1e-06
highest = lax.Precision.HIGHEST

def layer_norm(values, gain_vec, shift_vec):
    row_mean = lax.optimization_barrier(jnp.mean(values, axis=-1, keepdims=True))
    centered = values - row_mean
    variance = lax.optimization_barrier(jnp.mean(centered * centered, axis=-1, keepdims=True))
    return centered * lax.rsqrt(variance + epsilon) * gain_vec + shift_vec

def valid_rows(image_ids, group_lengths):
    total_rows = image_ids.shape[0]
    row_index = jnp.arange(total_rows, dtype=jnp.int32)
    member = image_ids[:, None] == jnp.arange(2, dtype=jnp.int32)[None, :]
    first_row = lax.optimization_barrier(jnp.min(jnp.where(member, row_index[:, None], total_rows), axis=0)).astype(jnp.int32)
    row_start = lax.optimization_barrier(jnp.sum(jnp.where(member, first_row[None, :], 0), axis=1)).astype(jnp.int32)
    row_limit = lax.optimization_barrier(jnp.sum(jnp.where(member, group_lengths[None, :], 0), axis=1)).astype(jnp.int32)
    return row_index - row_start < row_limit

def allowed_keys(first_query, image_ids, valid_mask):
    total_rows = image_ids.shape[0]
    row_index = jnp.arange(total_rows, dtype=jnp.int32)
    query_rows = first_query + jnp.arange(BLOCK, dtype=jnp.int32)
    query_ids = lax.dynamic_slice_in_dim(image_ids, first_query, BLOCK, 0)
    same_image = (query_ids[:, None] == image_ids[None, :]) & valid_mask[None, :]
    return same_image | (query_rows[:, None] == row_index[None, :])

def attention_group(queries, keys_all, values_all, image_ids, valid_mask):
    scale_factor = HEAD_DIM ** (-0.5)

    @jax.checkpoint
    def one_block(block_number):
        first_query = (block_number * BLOCK).astype(jnp.int32)
        query_block = lax.dynamic_slice_in_dim(queries, first_query, BLOCK, 0)
        scores = low_back(jnp.einsum('qhd,khd->hqk', query_block, keys_all, precision=highest) * scale_factor)
        allowed = allowed_keys(first_query, image_ids, valid_mask)
        scores = jnp.where(allowed[None, :, :], scores, -1e+30)
        probabilities = low(jax.nn.softmax(scores, axis=-1))
        return jnp.einsum('hqk,khd->qhd', probabilities, values_all, precision=highest)
    blocks = lax.map(one_block, jnp.arange(ROWS // BLOCK, dtype=jnp.int32))
    return blocks.reshape(ROWS, HEADS * HEAD_DIM)

def group_forward(inputs, image_ids, group_lengths, params):
    w_qkv, bias_query, bias_value, w_out, w_up, bias_up, w_down, out_biases, norm_gain, norm_bias = params
    valid_mask = valid_rows(image_ids, group_lengths)
    normed_one = low(layer_norm(inputs, norm_gain[0], norm_bias[0]))
    projected = jnp.einsum('rd,tde->tre', normed_one, w_qkv, precision=highest)
    queries = low_back(low(projected[0] + bias_query)).reshape(ROWS, HEADS, HEAD_DIM)
    keys_all = low_back(low(projected[1])).reshape(ROWS, HEADS, HEAD_DIM)
    values_all = low_back(low(projected[2] + bias_value)).reshape(ROWS, HEADS, HEAD_DIM)
    attended = low_back(low(attention_group(queries, keys_all, values_all, image_ids, valid_mask)))
    hidden_one = inputs + low_back(jnp.dot(attended, w_out, precision=highest)) + out_biases[0]
    normed_two = low(layer_norm(hidden_one, norm_gain[1], norm_bias[1]))
    pre_act = low_back(jnp.dot(normed_two, w_up, precision=highest) + bias_up)
    activated = low(jax.nn.gelu(pre_act, approximate=False))
    return hidden_one + low_back(jnp.dot(activated, w_down, precision=highest)) + out_biases[1]

def reference(tokens, image_ids, lengths, w_qkv, bias_query, bias_value, w_out, w_up, bias_up, w_down, out_biases, norm_gain, norm_bias, cotangent):
    float_args = (tokens.astype(jnp.float32), w_qkv.astype(jnp.float32), bias_query, bias_value, w_out.astype(jnp.float32), w_up.astype(jnp.float32), bias_up, w_down.astype(jnp.float32), out_biases, norm_gain, norm_bias)
    group_ids = image_ids.reshape(N_DP, ROWS)

    def forward(inputs, *params):

        @jax.checkpoint
        def one_group(totals, group_item):
            group_inputs, group_numbers, group_lengths = group_item
            return (totals, group_forward(group_inputs, group_numbers, group_lengths, params))
        _, outputs = lax.scan(one_group, jnp.zeros((), jnp.float32), (inputs.reshape(N_DP, ROWS, D), group_ids, lengths))
        return outputs.reshape(N_DP * ROWS, D)
    output_full, pullback = jax.vjp(forward, *float_args)
    valid_all = jax.vmap(valid_rows)(group_ids, lengths).reshape(N_DP * ROWS).astype(jnp.float32)
    gradients = pullback(cotangent.astype(jnp.float32) * valid_all[:, None])
    return (output_full.astype(jnp.bfloat16), gradients[0].astype(jnp.bfloat16), gradients[1], gradients[2], gradients[3], gradients[4], gradients[5], gradients[6], gradients[7], gradients[8], gradients[9], gradients[10])
```

```python
import functools

import jax
import jax.numpy as jnp
from jax import lax
from jax.experimental import pallas as pl
from jax.experimental.pallas import tpu as pltpu
from jax.sharding import PartitionSpec as P

HEAD_DIM = 64
LANES = 128
CHUNK = 768
MASKED = -1e30
MESH = pl.DeviceIdType.MESH
VMEM_BYTES = 62 << 20
BF = jnp.bfloat16
F32 = jnp.float32
NN = (((1,), (0,)), ((), ()))
NT = (((1,), (1,)), ((), ()))
TN = (((0,), (0,)), ((), ()))
SCALE = HEAD_DIM ** (-0.5)
epsilon = 1e-06


def dot(left, right, dims=NN):
    return lax.dot_general(left, right, dims, preferred_element_type=F32)


def layer_norm(values, gain_vec, shift_vec):
    row_mean = jnp.mean(values, axis=-1, keepdims=True)
    centered = values - row_mean
    variance = jnp.mean(centered * centered, axis=-1, keepdims=True)
    return centered * lax.rsqrt(variance + epsilon) * gain_vec + shift_vec


def exact_gelu(values):
    return jax.nn.gelu(values, approximate=False)


def valid_rows(image_ids, group_lengths):
    total_rows = image_ids.shape[0]
    row_index = jnp.arange(total_rows, dtype=jnp.int32)
    member = image_ids[:, None] == jnp.arange(2, dtype=jnp.int32)[None, :]
    first_row = jnp.min(jnp.where(member, row_index[:, None], total_rows), axis=0)
    row_start = jnp.sum(jnp.where(member, first_row[None, :], 0), axis=1)
    row_limit = jnp.sum(jnp.where(member, group_lengths[None, :], 0), axis=1)
    return row_index - row_start < row_limit


def mp_parts(n):
    chain = min(4, n)
    return chain, n // chain


def column_sum(values):
    ones = jnp.ones((8, values.shape[1]), BF)
    high = values.astype(BF)
    low = (values - high.astype(F32)).astype(BF)
    return dot(ones, high, NT) + dot(ones, low, NT)


def split_three(column):
    high = column.astype(BF)
    rest = column - high.astype(F32)
    middle = rest.astype(BF)
    return high, middle, (rest - middle.astype(F32)).astype(BF)


def attend_chunk(c, heads, q_ref, k_ref, v_ref, vt_ref, self_ref, att_ref, lse_ref):
    rows = pl.ds(pl.multiple_of(c * CHUNK, CHUNK), CHUNK)
    pieces = []
    scores = [dot(k_ref[h], q_ref[h, rows, :], NT) for h in range(heads)]
    for h in range(heads):
        own = q_ref[h, rows, :HEAD_DIM].astype(F32) * k_ref[h, rows, :HEAD_DIM].astype(F32)
        own = column_sum(own)[:1] + self_ref[:1, rows]
        top = jnp.maximum(jnp.max(scores[h], axis=0, keepdims=True), own)
        weights = jnp.exp(scores[h] - top).astype(BF)
        own_weight = jnp.exp(own - top).astype(BF).astype(F32)
        summed = dot(vt_ref[h], weights) + vt_ref[h, :, rows].astype(F32) * own_weight
        total = summed[HEAD_DIM : HEAD_DIM + 1]
        pieces.append(summed[:HEAD_DIM] / total)
        lse_ref[h, :, rows] = jnp.broadcast_to(top + jnp.log(total), (8, CHUNK))
    stacked = jnp.concatenate(pieces, axis=0) if heads > 1 else pieces[0]
    att_ref[rows, :] = stacked.T.astype(BF)


def front_kernel(
    n,
    tokens_ref,
    gain_ref,
    shift_ref,
    w_ref,
    bq_ref,
    bv_ref,
    tq_ref,
    tk_ref,
    self_ref,
    normed_ref,
    q_ref,
    k_ref,
    v_ref,
    lse_ref,
    att_ref,
    owned_ref,
    blocks,
    vt_ref,
    owned,
    ssz,
    rsz,
    ssx,
    rsx,
    ssa,
    rsa,
    local_sem,
):
    chain, cols = mp_parts(n)
    share, _ = tokens_ref.shape
    width = w_ref.shape[2]
    heads = width // HEAD_DIM
    dp, me = lax.axis_index("dp"), lax.axis_index("mp")
    a, b = me // cols, lax.rem(me, cols)

    barrier = pltpu.get_barrier_semaphore()
    for off in range(1, n):
        pl.semaphore_signal(
            barrier, inc=1, device_id=(dp, lax.rem(me + off, n)), device_id_type=MESH
        )
    pl.semaphore_wait(barrier, n - 1)

    normed = layer_norm(tokens_ref[...].astype(F32), gain_ref[...], shift_ref[...])
    blocks[me] = normed.astype(BF)

    def chain_copy(block, way):
        step = 1 if way == 0 else -1
        peer = jnp.clip(a + step, 0, chain - 1) * cols + b
        spot = blocks.at[block]
        return pltpu.make_async_remote_copy(
            src_ref=spot,
            dst_ref=spot,
            send_sem=ssz.at[way, block // cols],
            recv_sem=rsz.at[way, block // cols],
            device_id=(dp, peer),
            device_id_type=MESH,
        )

    def cross_copy(block, off):
        peer = a * cols + lax.rem(b + off, cols)
        spot = blocks.at[block]
        return pltpu.make_async_remote_copy(
            src_ref=spot,
            dst_ref=spot,
            send_sem=ssx.at[off, block // cols],
            recv_sem=rsx.at[off, block // cols],
            device_id=(dp, peer),
            device_id_type=MESH,
        )

    def project(block):
        rows = pl.ds(pl.multiple_of(block * share, share), share)
        values = blocks[block]
        out_q = (dot(values, w_ref[0]) + bq_ref[...]).astype(BF)
        out_k = dot(values, w_ref[1]).astype(BF)
        out_v = (dot(values, w_ref[2]) + bv_ref[...]).astype(BF)
        lane = lax.broadcasted_iota(jnp.int32, (share, LANES - HEAD_DIM), 1)
        tail_v = jnp.where(lane < 3, 1.0, 0.0).astype(BF)
        for h in range(heads):
            cut = slice(h * HEAD_DIM, (h + 1) * HEAD_DIM)
            q_ref[h, rows, :] = jnp.concatenate(
                [out_q[:, cut] * jnp.asarray(SCALE, BF), tq_ref[rows, :]], axis=1
            )
            k_ref[h, rows, :] = jnp.concatenate([out_k[:, cut], tk_ref[rows, :]], axis=1)
            v_ref[h, rows, :] = jnp.concatenate([out_v[:, cut], tail_v], axis=1)

    for way in (0, 1):

        @pl.when((a < chain - 1) if way == 0 else (a > 0))
        def _(way=way):
            chain_copy(me, way).start()

    for off in range(1, cols):
        cross_copy(me, off).start()
    project(me)

    def visit(step, _):
        for way in (0, 1):
            there = a - step if way == 0 else a + step
            inside = (there >= 0) & (there < chain)
            block = jnp.clip(there, 0, chain - 1) * cols + b

            @pl.when(inside)
            def _(way=way, block=block):
                chain_copy(block, way).wait_recv()

                @pl.when((a < chain - 1) if way == 0 else (a > 0))
                def _():
                    chain_copy(block, way).start()

                for off in range(1, cols):
                    cross_copy(block, off).start()

        def one(j, _):
            source = lax.rem(j, 2)
            lag = j // 2
            gone = step - jnp.minimum(lag, 1)
            there = jnp.where(source == 0, a - gone, a + gone)
            fresh = (gone > 0) | ((source == 0) & (lag > 0))
            inside = (there >= 0) & (there < chain) & fresh & (gone < chain)
            row = jnp.clip(there, 0, chain - 1)
            for off in range(1, cols):

                @pl.when(inside & (lag == off))
                def _(off=off):
                    cross_copy(row * cols + b, off).wait_recv()

            @pl.when(inside)
            def _():
                project(row * cols + lax.rem(b - lag + cols, cols))

            return 0

        lax.fori_loop(0, 2 * cols, one, 0)
        return 0

    lax.fori_loop(1, chain + 1, visit, 0)

    keep = pltpu.make_async_copy(blocks, normed_ref, local_sem.at[0])
    keep.start()

    def flip(c, _):
        rows = pl.ds(pl.multiple_of(c * CHUNK, CHUNK), CHUNK)
        for h in range(heads):
            vt_ref[h, :, rows] = v_ref[h, rows, :].astype(F32).T.astype(BF)
        return 0

    lax.fori_loop(0, n * share // CHUNK, flip, 0)

    def own_copy(target, source):
        return pltpu.make_async_remote_copy(
            src_ref=att_ref.at[pl.ds(pl.multiple_of(target * share, share), share)],
            dst_ref=owned.at[source],
            send_sem=ssa.at[target],
            recv_sem=rsa.at[source],
            device_id=(dp, target),
            device_id_type=MESH,
        )

    def attend(c, _):
        attend_chunk(c, heads, q_ref, k_ref, v_ref, vt_ref, self_ref, att_ref, lse_ref)

        def send(target, _):
            end = (target + 1) * share

            @pl.when((end <= (c + 1) * CHUNK) & (end > c * CHUNK) & (target != me))
            def _():
                own_copy(target, me).start()

            return 0

        lax.fori_loop(0, n, send, 0)
        return 0

    lax.fori_loop(0, n * share // CHUNK, attend, 0)
    owned[me] = att_ref[pl.ds(pl.multiple_of(me * share, share), share), :]

    def collect(other, _):
        @pl.when(other != me)
        def _():
            own_copy(other, me).wait_send()
            own_copy(me, other).wait_recv()

        return 0

    lax.fori_loop(0, n, collect, 0)
    owned_ref[...] = owned[...]
    keep.wait()

    def drain(row, _):
        for off in range(1, cols):
            cross_copy(row * cols + b, off).wait_send()

        @pl.when((row <= a) & (a < chain - 1))
        def _():
            chain_copy(row * cols + b, 0).wait_send()

        @pl.when((row >= a) & (a > 0))
        def _():
            chain_copy(row * cols + b, 1).wait_send()

        return 0

    lax.fori_loop(0, chain, drain, 0)


def front(n, tokens, gain, shift, w_qkv, bias_query, bias_value, tail_q, tail_k, self_bias):
    chain, cols = mp_parts(n)
    share, model = tokens.shape
    width = w_qkv.shape[2]
    heads = width // HEAD_DIM
    rows = n * share
    vmem = pl.BlockSpec(memory_space=pltpu.VMEM)
    anywhere = pl.BlockSpec(memory_space=pl.ANY)
    ext = jax.ShapeDtypeStruct((heads, rows, LANES), BF)
    dma = pltpu.SemaphoreType.DMA
    return pl.pallas_call(
        functools.partial(front_kernel, n),
        name="front",
        out_shape=(
            jax.ShapeDtypeStruct((n, share, model), BF),
            ext,
            ext,
            ext,
            jax.ShapeDtypeStruct((heads, 8, rows), F32),
            jax.ShapeDtypeStruct((rows, width), BF),
            jax.ShapeDtypeStruct((n, share, width), BF),
        ),
        in_specs=[vmem] * 9,
        out_specs=(anywhere,) + (vmem,) * 6,
        scratch_shapes=[
            pltpu.VMEM((n, share, model), BF),
            pltpu.VMEM((heads, LANES, rows), BF),
            pltpu.VMEM((n, share, width), BF),
            dma((2, chain)),
            dma((2, chain)),
            dma((cols, chain)),
            dma((cols, chain)),
            dma((n,)),
            dma((n,)),
            dma((1,)),
        ],
        compiler_params=pltpu.CompilerParams(
            collective_id=0, has_side_effects=True, vmem_limit_bytes=VMEM_BYTES
        ),
    )(
        tokens,
        gain[None, :],
        shift[None, :],
        w_qkv,
        bias_query[None, :],
        bias_value[None, :],
        tail_q,
        tail_k,
        self_bias,
    )


def attend_back_chunk(
    c, heads, q_ref, k_ref, v_ref, kt_ref, lse_ref, self_ref, att_ref, grad_ref, gq_ref, dk_ref, dv_ref
):
    rows = pl.ds(pl.multiple_of(c * CHUNK, CHUNK), CHUNK)
    grads = grad_ref[rows, :].astype(F32)
    products = grads * att_ref[rows, :].astype(F32)
    outs = []
    for h in range(heads):
        cut = slice(h * HEAD_DIM, (h + 1) * HEAD_DIM)
        inner = jnp.sum(products[:, cut], axis=1, keepdims=True)
        parts = split_three(-inner)
        lane = lax.broadcasted_iota(jnp.int32, (CHUNK, LANES - HEAD_DIM), 1)
        tail = jnp.zeros((CHUNK, LANES - HEAD_DIM), F32)
        for i, part in enumerate(parts):
            tail = jnp.where(lane == i, part.astype(F32), tail)
        grad_ext = jnp.concatenate([grads[:, cut], tail], axis=1).astype(BF)
        query = q_ref[h, rows, :]
        key_own = k_ref[h, rows, :]
        scores = dot(k_ref[h], query, NT)
        lse = lse_ref[h, :1, rows]
        probs = jnp.exp(scores - lse)
        shifted = dot(v_ref[h], grad_ext, NT)
        own = column_sum(query[:, :HEAD_DIM].astype(F32) * key_own[:, :HEAD_DIM].astype(F32))
        own_prob = jnp.exp(own + self_ref[:, rows] - lse)
        own_shifted = column_sum(v_ref[h, rows, :].astype(F32) * grad_ext.astype(F32))
        lower = lax.broadcasted_iota(jnp.int32, (8, CHUNK), 0) < 4
        both = jnp.where(lower, own_prob, own_prob * own_shifted).T
        own_prob, own_score = both[:, :1], both[:, 4:5]
        grad_scores = (probs * shifted).astype(BF)
        dv = dot(probs.astype(BF), grad_ext)
        dk = dot(grad_scores, query)
        dq = dot(kt_ref[h], grad_scores).T
        dq = (dq + own_score * key_own.astype(F32)) * SCALE
        outs.append(dq[:, :HEAD_DIM])

        @pl.when(c == 0)
        def _(h=h, dv=dv, dk=dk):
            dv_ref[h] = dv
            dk_ref[h] = dk

        @pl.when(c > 0)
        def _(h=h, dv=dv, dk=dk):
            dv_ref[h] += dv
            dk_ref[h] += dk

        dv_ref[h, rows, :] += own_prob * grad_ext.astype(F32)
        dk_ref[h, rows, :] += own_score * query.astype(F32)
    stacked = jnp.concatenate(outs, axis=1) if heads > 1 else outs[0]
    gq_ref[rows, :] = stacked.astype(BF)


def back_kernel(
    q_ref, k_ref, v_ref, lse_ref, self_ref, att_ref, grad_ref, gq_ref, gk_ref, gv_ref, kt_ref, dk_ref, dv_ref
):
    heads, total, _ = q_ref.shape

    def flip(c, _):
        rows = pl.ds(pl.multiple_of(c * CHUNK, CHUNK), CHUNK)
        for h in range(heads):
            kt_ref[h, :, rows] = k_ref[h, rows, :].astype(F32).T.astype(BF)
        return 0

    lax.fori_loop(0, total // CHUNK, flip, 0)

    def step(c, _):
        attend_back_chunk(
            c, heads, q_ref, k_ref, v_ref, kt_ref, lse_ref, self_ref, att_ref, grad_ref, gq_ref, dk_ref, dv_ref
        )
        return 0

    lax.fori_loop(0, total // CHUNK, step, 0)

    def finish(c, _):
        rows = pl.ds(pl.multiple_of(c * CHUNK, CHUNK), CHUNK)
        keys = [dk_ref[h, rows, :HEAD_DIM] for h in range(heads)]
        values = [dv_ref[h, rows, :HEAD_DIM] for h in range(heads)]
        gk_ref[rows, :] = (jnp.concatenate(keys, axis=1) if heads > 1 else keys[0]).astype(BF)
        gv_ref[rows, :] = (jnp.concatenate(values, axis=1) if heads > 1 else values[0]).astype(BF)
        return 0

    lax.fori_loop(0, total // CHUNK, finish, 0)


def attend_back(q_ext, k_ext, v_ext, lse, self_bias, attended, grad_attended):
    heads, rows, _ = q_ext.shape
    vmem = pl.BlockSpec(memory_space=pltpu.VMEM)
    out = jax.ShapeDtypeStruct(attended.shape, BF)
    return pl.pallas_call(
        back_kernel,
        name="attend_back",
        out_shape=(out, out, out),
        in_specs=[vmem] * 7,
        out_specs=(vmem,) * 3,
        scratch_shapes=[
            pltpu.VMEM((heads, LANES, rows), BF),
            pltpu.VMEM((heads, rows, LANES), F32),
            pltpu.VMEM((heads, rows, LANES), F32),
        ],
        compiler_params=pltpu.CompilerParams(vmem_limit_bytes=VMEM_BYTES),
    )(q_ext, k_ext, v_ext, lse, self_bias, attended, grad_attended)


def body(
    n,
    tokens,
    image_ids,
    lengths,
    w_qkv,
    bias_query,
    bias_value,
    w_out,
    w_up,
    bias_up,
    w_down,
    out_biases,
    norm_gain,
    norm_bias,
    cotangent,
):
    share_rows = tokens.shape[0]
    total_rows = image_ids.shape[0]
    model_index = lax.axis_index("mp")
    valid_mask = valid_rows(image_ids, lengths[0])
    own_valid = lax.dynamic_slice_in_dim(
        valid_mask.astype(F32), model_index * share_rows, share_rows, 0
    )
    spare = jnp.arange(LANES - HEAD_DIM, dtype=jnp.int32)[None, :]
    is_id = image_ids[:, None] == spare
    tail_q = jnp.where(is_id & (spare < 2), 1.0, 0.0).astype(BF)
    tail_k = jnp.where(spare < 2, jnp.where(is_id & valid_mask[:, None], 0.0, MASKED), 0.0)
    tail_k = tail_k.astype(BF)
    self_bias = jnp.broadcast_to(jnp.where(valid_mask, MASKED, 0.0)[None, :], (8, total_rows))

    inputs_f = tokens.astype(F32)
    gathered_one, q_ext, k_ext, v_ext, log_totals, attended, owned = front(
        n,
        tokens,
        norm_gain[0],
        norm_bias[0],
        w_qkv,
        bias_query,
        bias_value,
        tail_q,
        tail_k,
        self_bias,
    )
    gathered_one = gathered_one.reshape(total_rows, -1)
    owned = jnp.transpose(owned, (1, 0, 2)).reshape(share_rows, -1)
    w_out_all = lax.all_gather(w_out, "mp", axis=0, tiled=True)
    hidden_one = (
        inputs_f
        + jnp.dot(owned, w_out_all, preferred_element_type=F32)
        + out_biases[0]
    )
    normed_two = layer_norm(hidden_one, norm_gain[1], norm_bias[1]).astype(jnp.bfloat16)
    gathered_two = lax.all_gather(normed_two, "mp", axis=0, tiled=True)
    pre_act = jnp.dot(gathered_two, w_up, preferred_element_type=jnp.float32) + bias_up
    activated = exact_gelu(pre_act).astype(jnp.bfloat16)
    output_full = (
        hidden_one
        + lax.psum_scatter(
            jnp.dot(activated, w_down, preferred_element_type=jnp.float32).astype(jnp.bfloat16),
            "mp",
            scatter_dimension=0,
            tiled=True,
        ).astype(jnp.float32)
        + out_biases[1]
    )
    tokens_f = tokens.astype(jnp.float32)
    grad_out = cotangent.astype(jnp.float32) * own_valid[:, None]
    grad_mlp = lax.all_gather(grad_out.astype(jnp.bfloat16), "mp", axis=0, tiled=True)
    grad_w_down = jnp.einsum("rf,rd->fd", activated, grad_mlp, preferred_element_type=jnp.float32)
    grad_act = jnp.einsum("rd,fd->rf", grad_mlp, w_down, preferred_element_type=jnp.float32)
    _, gelu_back = jax.vjp(exact_gelu, pre_act)
    grad_pre = gelu_back(grad_act)[0].astype(jnp.bfloat16)
    grad_w_up = jnp.einsum("rd,rf->df", gathered_two, grad_pre, preferred_element_type=jnp.float32)
    grad_bias_up = jnp.sum(grad_pre, axis=0, dtype=jnp.float32)
    grad_normed_two = lax.psum_scatter(
        jnp.einsum("rf,df->rd", grad_pre, w_up, preferred_element_type=jnp.float32).astype(
            jnp.bfloat16
        ),
        "mp",
        scatter_dimension=0,
        tiled=True,
    ).astype(jnp.float32)
    _, norm_two_back = jax.vjp(layer_norm, hidden_one, norm_gain[1], norm_bias[1])
    grad_from_two, gain_two, shift_two = norm_two_back(grad_normed_two)
    grad_hidden = grad_out + grad_from_two
    grad_proj = lax.all_gather(grad_hidden.astype(jnp.bfloat16), "mp", axis=0, tiled=True)
    grad_w_out = jnp.einsum("re,rd->ed", attended, grad_proj, preferred_element_type=jnp.float32)
    grad_attended = jnp.einsum(
        "rd,ed->re", grad_proj, w_out, preferred_element_type=jnp.float32
    ).astype(jnp.bfloat16)
    grad_stack = jnp.stack(
        attend_back(q_ext, k_ext, v_ext, log_totals, self_bias, attended, grad_attended)
    )
    grad_w_qkv = jnp.einsum(
        "rd,tre->tde", gathered_one, grad_stack, preferred_element_type=jnp.float32
    )
    grad_bias_query = jnp.sum(grad_stack[0], axis=0, dtype=jnp.float32)
    grad_bias_value = jnp.sum(grad_stack[2], axis=0, dtype=jnp.float32)
    grad_normed_one = lax.psum_scatter(
        jnp.einsum("tre,tde->rd", grad_stack, w_qkv, preferred_element_type=jnp.float32).astype(
            jnp.bfloat16
        ),
        "mp",
        scatter_dimension=0,
        tiled=True,
    ).astype(jnp.float32)
    _, norm_one_back = jax.vjp(layer_norm, tokens_f, norm_gain[0], norm_bias[0])
    grad_from_one, gain_one, shift_one = norm_one_back(grad_normed_one)
    input_grad = (grad_hidden + grad_from_one).astype(jnp.bfloat16)
    grad_norm_gain, grad_norm_bias, grad_out_biases = lax.psum(
        (
            jnp.stack([gain_one, gain_two]),
            jnp.stack([shift_one, shift_two]),
            jnp.stack([jnp.sum(grad_hidden, axis=0), jnp.sum(grad_out, axis=0)]),
        ),
        ("dp", "mp"),
    )
    (
        grad_w_qkv,
        grad_bias_query,
        grad_bias_value,
        grad_w_out,
        grad_w_up,
        grad_bias_up,
        grad_w_down,
    ) = (
        lax.psum(grad_w_qkv.astype(jnp.bfloat16), "dp").astype(jnp.float32),
        lax.psum(grad_bias_query.astype(jnp.bfloat16), "dp").astype(jnp.float32),
        lax.psum(grad_bias_value.astype(jnp.bfloat16), "dp").astype(jnp.float32),
        lax.psum(grad_w_out.astype(jnp.bfloat16), "dp").astype(jnp.float32),
        lax.psum(grad_w_up.astype(jnp.bfloat16), "dp").astype(jnp.float32),
        lax.psum(grad_bias_up.astype(jnp.bfloat16), "dp").astype(jnp.float32),
        lax.psum(grad_w_down.astype(jnp.bfloat16), "dp").astype(jnp.float32),
    )
    return (
        output_full.astype(jnp.bfloat16),
        input_grad,
        grad_w_qkv,
        grad_bias_query,
        grad_bias_value,
        grad_w_out,
        grad_w_up,
        grad_bias_up,
        grad_w_down,
        grad_out_biases,
        grad_norm_gain,
        grad_norm_bias,
    )


def solution(mesh):
    in_specs = (
        P(("dp", "mp"), None),
        P("dp"),
        P("dp", None),
        P(None, None, "mp"),
        P("mp"),
        P("mp"),
        P("mp", None),
        P(None, "mp"),
        P("mp"),
        P("mp", None),
        P(),
        P(),
        P(),
        P(("dp", "mp"), None),
    )
    out_specs = (
        P(("dp", "mp"), None),
        P(("dp", "mp"), None),
        P(None, None, "mp"),
        P("mp"),
        P("mp"),
        P("mp", None),
        P(None, "mp"),
        P("mp"),
        P("mp", None),
        P(),
        P(),
        P(),
    )
    return jax.shard_map(
        functools.partial(body, mesh.shape["mp"]),
        mesh=mesh,
        in_specs=in_specs,
        out_specs=out_specs,
        check_vma=False,
    )
```

```python
import functools

import jax
import jax.numpy as jnp
from jax import lax
from jax.experimental import pallas as pl
from jax.experimental.pallas import tpu as pltpu
from jax.sharding import PartitionSpec as P

HEAD_DIM = 64
LANES = 128
CHUNK = 768
MASKED = -1e30
MESH = pl.DeviceIdType.MESH
VMEM_BYTES = 62 << 20
BF = jnp.bfloat16
F32 = jnp.float32
NN = (((1,), (0,)), ((), ()))
NT = (((1,), (1,)), ((), ()))
TN = (((0,), (0,)), ((), ()))
SCALE = HEAD_DIM ** (-0.5)
PARTS = 4
epsilon = 1e-06


def dot(left, right, dims=NN):
    return lax.dot_general(left, right, dims, preferred_element_type=F32)


def layer_norm(values, gain_vec, shift_vec):
    row_mean = jnp.mean(values, axis=-1, keepdims=True)
    centered = values - row_mean
    variance = jnp.mean(centered * centered, axis=-1, keepdims=True)
    return centered * lax.rsqrt(variance + epsilon) * gain_vec + shift_vec


def exact_gelu(values):
    return jax.nn.gelu(values, approximate=False)


def valid_rows(image_ids, group_lengths):
    total_rows = image_ids.shape[0]
    row_index = jnp.arange(total_rows, dtype=jnp.int32)
    member = image_ids[:, None] == jnp.arange(2, dtype=jnp.int32)[None, :]
    first_row = jnp.min(jnp.where(member, row_index[:, None], total_rows), axis=0)
    row_start = jnp.sum(jnp.where(member, first_row[None, :], 0), axis=1)
    row_limit = jnp.sum(jnp.where(member, group_lengths[None, :], 0), axis=1)
    return row_index - row_start < row_limit


def mp_parts(n):
    chain = min(4, n)
    return chain, n // chain


def column_sum(values):
    ones = jnp.ones((8, values.shape[1]), BF)
    high = values.astype(BF)
    low = (values - high.astype(F32)).astype(BF)
    return dot(ones, high, NT) + dot(ones, low, NT)


def split_three(column):
    high = column.astype(BF)
    rest = column - high.astype(F32)
    middle = rest.astype(BF)
    return high, middle, (rest - middle.astype(F32)).astype(BF)


def attend_chunk(c, heads, q_ref, k_ref, v_ref, vt_ref, self_ref, att_ref, lse_ref):
    rows = pl.ds(pl.multiple_of(c * CHUNK, CHUNK), CHUNK)
    pieces = []
    scores = [dot(k_ref[h], q_ref[h, rows, :], NT) for h in range(heads)]
    for h in range(heads):
        own = q_ref[h, rows, :HEAD_DIM].astype(F32) * k_ref[h, rows, :HEAD_DIM].astype(F32)
        own = column_sum(own)[:1] + self_ref[:1, rows]
        top = jnp.maximum(jnp.max(scores[h], axis=0, keepdims=True), own)
        weights = jnp.exp(scores[h] - top).astype(BF)
        own_weight = jnp.exp(own - top).astype(BF).astype(F32)
        summed = dot(vt_ref[h], weights) + vt_ref[h, :, rows].astype(F32) * own_weight
        total = summed[HEAD_DIM : HEAD_DIM + 1]
        pieces.append(summed[:HEAD_DIM] / total)
        lse_ref[h, :, rows] = jnp.broadcast_to(top + jnp.log(total), (8, CHUNK))
    stacked = jnp.concatenate(pieces, axis=0) if heads > 1 else pieces[0]
    att_ref[rows, :] = stacked.T.astype(BF)


def front_kernel(
    n,
    tokens_ref,
    gain_ref,
    shift_ref,
    w_ref,
    bq_ref,
    bv_ref,
    tq_ref,
    tk_ref,
    self_ref,
    up_ref,
    down_ref,
    out_ref,
    bup_ref,
    normed_ref,
    q_ref,
    k_ref,
    v_ref,
    lse_ref,
    att_ref,
    owned_ref,
    ups_ref,
    downs_ref,
    outs_ref,
    bups_ref,
    blocks,
    vt_ref,
    owned,
    ssz,
    rsz,
    ssx,
    rsx,
    ssa,
    rsa,
    wsz,
    wrz,
    wsx,
    wrx,
    gs,
    gr,
    os,
    orr,
    bs,
    br,
    local_sem,
):
    chain, cols = mp_parts(n)
    share, _ = tokens_ref.shape
    width = w_ref.shape[2]
    heads = width // HEAD_DIM
    hidden = up_ref.shape[1]
    up_rows, down_rows, out_rows = (r.shape[0] // PARTS for r in (up_ref, down_ref, out_ref))
    dp, a, b = lax.axis_index("dp"), lax.axis_index("mz"), lax.axis_index("mx")
    me = a * cols + b
    part = lax.rem(dp, PARTS)
    core_dp = dp + 1 - 2 * lax.rem(dp, 2)
    side_dp = dp + 2 - 4 * lax.rem(dp // 2, 2)
    core_part, side_part = lax.rem(core_dp, PARTS), lax.rem(side_dp, PARTS)
    far_part = PARTS - 1 - part

    barrier = pltpu.get_barrier_semaphore()
    for off in range(1, n):
        other = lax.rem(me + off, n)
        pl.semaphore_signal(
            barrier,
            inc=1,
            device_id=(dp, other // cols, lax.rem(other, cols)),
            device_id_type=MESH,
        )
    for peer in (core_dp, side_dp):
        pl.semaphore_signal(barrier, inc=1, device_id=(peer, a, b), device_id_type=MESH)
    pl.semaphore_wait(barrier, n + 1)

    def remote(src, dst, send, recv, device):
        return pltpu.make_async_remote_copy(
            src_ref=src,
            dst_ref=dst,
            send_sem=send,
            recv_sem=recv,
            device_id=device,
            device_id_type=MESH,
        )

    def span(index, size):
        return pl.ds(pl.multiple_of(index * size, size), size)

    def can(way):
        return (a < chain - 1) if way == 0 else (a > 0)

    def chain_peer(way):
        return (dp, jnp.clip(a + (1 if way == 0 else -1), 0, chain - 1), b)

    def cross_peer(off):
        return (dp, a, lax.rem(b + off, cols))

    def chain_copy(block, way):
        spot = blocks.at[block]
        sems = ssz.at[way, block // cols], rsz.at[way, block // cols]
        return remote(spot, spot, *sems, chain_peer(way))

    def cross_copy(block, off):
        spot = blocks.at[block]
        sems = ssx.at[off, block // cols], rsx.at[off, block // cols]
        return remote(spot, spot, *sems, cross_peer(off))

    def piece(i, row, of_part):
        if i == 0:
            return outs_ref.at[row * cols + b, span(of_part, out_rows)]
        if i == 1:
            return ups_ref.at[span(of_part, up_rows), span(row, hidden)]
        return downs_ref.at[span(row * PARTS + of_part, down_rows)]

    def own_piece(i):
        if i == 0:
            return out_ref.at[span(part, out_rows)]
        if i == 1:
            return up_ref.at[span(part, up_rows)]
        return down_ref.at[span(part, down_rows)]

    def weight_copy(i, row, way, own=False):
        spot = piece(i, row, part)
        sems = wsz.at[i, way, row], wrz.at[i, way, row]
        return remote(own_piece(i) if own else spot, spot, *sems, chain_peer(way))

    def out_cross(block, off, own=False):
        spot = outs_ref.at[block, span(part, out_rows)]
        sems = wsx.at[off, block // cols], wrx.at[off, block // cols]
        return remote(own_piece(0) if own else spot, spot, *sems, cross_peer(off))

    def group_copy(kind, i, row, arriving=False):
        sent = side_part if kind == 2 else part
        got = (side_part, core_part, far_part)[kind]
        spot = piece(i, row, got if arriving else sent)
        sems = gs.at[kind, i - 1, row], gr.at[kind, i - 1, row]
        return remote(spot, spot, *sems, (side_dp if kind == 0 else core_dp, a, b))

    def out_group(kind, arriving=False):
        sent = side_part if kind == 2 else part
        got = (side_part, core_part, far_part)[kind]
        spot = outs_ref.at[:, span(got if arriving else sent, out_rows)]
        return remote(spot, spot, os.at[kind], orr.at[kind], (side_dp if kind == 0 else core_dp, a, b))

    def bias_copy(off, arriving=False):
        spot = bups_ref.at[lax.rem(a - off + chain, chain) if arriving else a]
        return remote(bup_ref, spot, bs.at[off], br.at[off], (dp, lax.rem(a + off, chain), b))

    def start_own(way):
        for i in range(3):
            weight_copy(i, a, way, own=True).start()

    stay = [
        pltpu.make_async_copy(up_ref, ups_ref.at[:, span(a, hidden)], local_sem.at[1]),
        pltpu.make_async_copy(down_ref, downs_ref.at[span(a, hidden)], local_sem.at[2]),
        pltpu.make_async_copy(own_piece(0), piece(0, a, part), local_sem.at[3]),
        pltpu.make_async_copy(bup_ref, bups_ref.at[a], local_sem.at[4]),
    ]

    normed = layer_norm(tokens_ref[...].astype(F32), gain_ref[...], shift_ref[...])
    blocks[me] = normed.astype(BF)

    def project(block):
        rows = span(block, share)
        values = blocks[block]
        out_q = (dot(values, w_ref[0]) + bq_ref[...]).astype(BF)
        out_k = dot(values, w_ref[1]).astype(BF)
        out_v = (dot(values, w_ref[2]) + bv_ref[...]).astype(BF)
        lane = lax.broadcasted_iota(jnp.int32, (share, LANES - HEAD_DIM), 1)
        tail_v = jnp.where(lane < 3, 1.0, 0.0).astype(BF)
        for h in range(heads):
            cut = slice(h * HEAD_DIM, (h + 1) * HEAD_DIM)
            q_ref[h, rows, :] = jnp.concatenate(
                [out_q[:, cut] * jnp.asarray(SCALE, BF), tq_ref[rows, :]], axis=1
            )
            k_ref[h, rows, :] = jnp.concatenate([out_k[:, cut], tk_ref[rows, :]], axis=1)
            v_ref[h, rows, :] = jnp.concatenate([out_v[:, cut], tail_v], axis=1)

    for way in (0, 1):

        @pl.when(can(way))
        def _(way=way):
            chain_copy(me, way).start()

    for off in range(1, cols):
        cross_copy(me, off).start()
    for copy in stay:
        copy.start()

    @pl.when(a == 0)
    def _():
        start_own(0)

    @pl.when(a == chain - 1)
    def _():
        start_own(1)

    project(me)

    def visit(step, _):
        for way in (0, 1):
            there = a - step if way == 0 else a + step
            inside = (there >= 0) & (there < chain)
            block = jnp.clip(there, 0, chain - 1) * cols + b

            @pl.when(inside)
            def _(way=way, block=block):
                chain_copy(block, way).wait_recv()

                @pl.when(can(way))
                def _():
                    chain_copy(block, way).start()

                for off in range(1, cols):
                    cross_copy(block, off).start()

        @pl.when((step == a) & can(0))
        def _():
            start_own(0)

        @pl.when((step == chain - 1 - a) & can(1))
        def _():
            start_own(1)

        def one(j, _):
            source = lax.rem(j, 2)
            lag = j // 2
            gone = step - jnp.minimum(lag, 1)
            there = jnp.where(source == 0, a - gone, a + gone)
            fresh = (gone > 0) | ((source == 0) & (lag > 0))
            inside = (there >= 0) & (there < chain) & fresh & (gone < chain)
            row = jnp.clip(there, 0, chain - 1)
            for off in range(1, cols):

                @pl.when(inside & (lag == off))
                def _(off=off):
                    cross_copy(row * cols + lax.rem(b - off + cols, cols), off).wait_recv()

            @pl.when(inside)
            def _():
                project(row * cols + lax.rem(b - lag + cols, cols))

            return 0

        lax.fori_loop(0, 2 * cols, one, 0)
        return 0

    lax.fori_loop(1, chain + 1, visit, 0)

    keep = pltpu.make_async_copy(blocks, normed_ref, local_sem.at[0])
    keep.start()
    for off in range(1, cols):
        out_cross(me, off, own=True).start()
    for off in range(1, chain):
        bias_copy(off).start()

    def both_ways(step, act):
        for way in (0, 1):
            there = a - step if way == 0 else a + step

            @pl.when((there >= 0) & (there < chain))
            def _(way=way, there=there):
                act(way, jnp.clip(there, 0, chain - 1))

    def weights_pass(way, row):
        for i in range(3):
            weight_copy(i, row, way).wait_recv()

            @pl.when(can(way))
            def _(i=i):
                weight_copy(i, row, way).start()

            if i == 0:
                for off in range(1, cols):
                    out_cross(row * cols + b, off).start()
            else:
                group_copy(0, i, row).start()
                group_copy(1, i, row).start()

    def weights_side(way, row):
        for i in (1, 2):
            group_copy(0, i, row, arriving=True).wait_recv()
            group_copy(2, i, row).start()

    both_ways(1, weights_pass)

    def flip(c, _):
        rows = span(c, CHUNK)
        for h in range(heads):
            vt_ref[h, :, rows] = v_ref[h, rows, :].astype(F32).T.astype(BF)
        return 0

    lax.fori_loop(0, n * share // CHUNK, flip, 0)

    def own_copy(target, source):
        return remote(
            att_ref.at[span(target, share)],
            owned.at[source],
            ssa.at[target],
            rsa.at[source],
            (dp, target // cols, lax.rem(target, cols)),
        )

    def attend(c, _):
        attend_chunk(c, heads, q_ref, k_ref, v_ref, vt_ref, self_ref, att_ref, lse_ref)

        def send(target, _):
            end = (target + 1) * share

            @pl.when((end <= (c + 1) * CHUNK) & (end > c * CHUNK) & (target != me))
            def _():
                own_copy(target, me).start()

            return 0

        lax.fori_loop(0, n, send, 0)

        @pl.when(c > 0)
        def _():
            both_ways(c + 1, weights_pass)
            both_ways(c, weights_side)

        return 0

    lax.fori_loop(0, n * share // CHUNK, attend, 0)
    owned[me] = att_ref[span(me, share), :]

    def gather_out(row, _):
        for off in range(1, cols):
            out_cross(row * cols + lax.rem(b - off + cols, cols), off).wait_recv()
        return 0

    lax.fori_loop(0, chain, gather_out, 0)
    stay[2].wait()
    out_group(0).start()
    out_group(1).start()
    both_ways(chain - 1, weights_side)
    out_group(0, arriving=True).wait_recv()
    out_group(2).start()

    def collect(other, _):
        @pl.when(other != me)
        def _():
            own_copy(other, me).wait_send()
            own_copy(me, other).wait_recv()

        return 0

    lax.fori_loop(0, n, collect, 0)
    owned_ref[...] = owned[...]
    keep.wait()
    for i in (0, 1, 3):
        stay[i].wait()
    for off in range(1, chain):
        bias_copy(off).wait_send()
        bias_copy(off, arriving=True).wait_recv()
    for kind in range(3):
        out_group(kind).wait_send()
        if kind > 0:
            out_group(kind, arriving=True).wait_recv()

    def drain(row, _):
        for off in range(1, cols):
            cross_copy(row * cols + b, off).wait_send()
            out_cross(row * cols + b, off).wait_send()

        @pl.when((row <= a) & (a < chain - 1))
        def _():
            chain_copy(row * cols + b, 0).wait_send()
            for i in range(3):
                weight_copy(i, row, 0).wait_send()

        @pl.when((row >= a) & (a > 0))
        def _():
            chain_copy(row * cols + b, 1).wait_send()
            for i in range(3):
                weight_copy(i, row, 1).wait_send()

        @pl.when(row != a)
        def _():
            for i in (1, 2):
                for kind in range(3):
                    group_copy(kind, i, row).wait_send()
                    if kind > 0:
                        group_copy(kind, i, row, arriving=True).wait_recv()

        return 0

    lax.fori_loop(0, chain, drain, 0)


def front(n, tokens, gain, shift, w_qkv, bias_query, bias_value, tail_q, tail_k, self_bias, w_up, w_down, w_out, bias_up):
    chain, cols = mp_parts(n)
    share, model = tokens.shape
    width = w_qkv.shape[2]
    heads = width // HEAD_DIM
    hidden = w_up.shape[1]
    rows = n * share
    vmem = pl.BlockSpec(memory_space=pltpu.VMEM)
    anywhere = pl.BlockSpec(memory_space=pl.ANY)
    ext = jax.ShapeDtypeStruct((heads, rows, LANES), BF)
    dma = pltpu.SemaphoreType.DMA
    return pl.pallas_call(
        functools.partial(front_kernel, n),
        name="front",
        out_shape=(
            jax.ShapeDtypeStruct((n, share, model), BF),
            ext,
            ext,
            ext,
            jax.ShapeDtypeStruct((heads, 8, rows), F32),
            jax.ShapeDtypeStruct((rows, width), BF),
            jax.ShapeDtypeStruct((n, share, width), BF),
            jax.ShapeDtypeStruct((model, chain * hidden), BF),
            jax.ShapeDtypeStruct((chain * hidden, model), BF),
            jax.ShapeDtypeStruct((n, width, model), BF),
            jax.ShapeDtypeStruct((chain, 8, hidden), F32),
        ),
        in_specs=[vmem] * 13,
        out_specs=(anywhere,) + (vmem,) * 6 + (anywhere,) * 4,
        scratch_shapes=[
            pltpu.VMEM((n, share, model), BF),
            pltpu.VMEM((heads, LANES, rows), BF),
            pltpu.VMEM((n, share, width), BF),
            dma((2, chain)),
            dma((2, chain)),
            dma((cols, chain)),
            dma((cols, chain)),
            dma((n,)),
            dma((n,)),
            dma((3, 2, chain)),
            dma((3, 2, chain)),
            dma((cols, chain)),
            dma((cols, chain)),
            dma((3, 2, chain)),
            dma((3, 2, chain)),
            dma((3,)),
            dma((3,)),
            dma((chain,)),
            dma((chain,)),
            dma((5,)),
        ],
        compiler_params=pltpu.CompilerParams(
            collective_id=0, has_side_effects=True, vmem_limit_bytes=VMEM_BYTES
        ),
    )(
        tokens,
        gain[None, :],
        shift[None, :],
        w_qkv,
        bias_query[None, :],
        bias_value[None, :],
        tail_q,
        tail_k,
        self_bias,
        w_up,
        w_down,
        w_out,
        jnp.broadcast_to(bias_up[None, :], (8, hidden)),
    )


def attend_back_chunk(
    c, heads, q_ref, k_ref, v_ref, kt_ref, lse_ref, self_ref, att_ref, grad_ref, gq_ref, dk_ref, dv_ref
):
    rows = pl.ds(pl.multiple_of(c * CHUNK, CHUNK), CHUNK)
    grads = grad_ref[rows, :].astype(F32)
    products = grads * att_ref[rows, :].astype(F32)
    outs = []
    for h in range(heads):
        cut = slice(h * HEAD_DIM, (h + 1) * HEAD_DIM)
        inner = jnp.sum(products[:, cut], axis=1, keepdims=True)
        parts = split_three(-inner)
        lane = lax.broadcasted_iota(jnp.int32, (CHUNK, LANES - HEAD_DIM), 1)
        tail = jnp.zeros((CHUNK, LANES - HEAD_DIM), F32)
        for i, part in enumerate(parts):
            tail = jnp.where(lane == i, part.astype(F32), tail)
        grad_ext = jnp.concatenate([grads[:, cut], tail], axis=1).astype(BF)
        query = q_ref[h, rows, :]
        key_own = k_ref[h, rows, :]
        scores = dot(k_ref[h], query, NT)
        lse = lse_ref[h, :1, rows]
        probs = jnp.exp(scores - lse)
        shifted = dot(v_ref[h], grad_ext, NT)
        own = column_sum(query[:, :HEAD_DIM].astype(F32) * key_own[:, :HEAD_DIM].astype(F32))
        own_prob = jnp.exp(own + self_ref[:, rows] - lse)
        own_shifted = column_sum(v_ref[h, rows, :].astype(F32) * grad_ext.astype(F32))
        lower = lax.broadcasted_iota(jnp.int32, (8, CHUNK), 0) < 4
        both = jnp.where(lower, own_prob, own_prob * own_shifted).T
        own_prob, own_score = both[:, :1], both[:, 4:5]
        grad_scores = (probs * shifted).astype(BF)
        dv = dot(probs.astype(BF), grad_ext)
        dk = dot(grad_scores, query)
        dq = dot(kt_ref[h], grad_scores).T
        dq = (dq + own_score * key_own.astype(F32)) * SCALE
        outs.append(dq[:, :HEAD_DIM])

        @pl.when(c == 0)
        def _(h=h, dv=dv, dk=dk):
            dv_ref[h] = dv
            dk_ref[h] = dk

        @pl.when(c > 0)
        def _(h=h, dv=dv, dk=dk):
            dv_ref[h] += dv
            dk_ref[h] += dk

        dv_ref[h, rows, :] += own_prob * grad_ext.astype(F32)
        dk_ref[h, rows, :] += own_score * query.astype(F32)
    stacked = jnp.concatenate(outs, axis=1) if heads > 1 else outs[0]
    gq_ref[rows, :] = stacked.astype(BF)


def back_kernel(
    q_ref, k_ref, v_ref, lse_ref, self_ref, att_ref, grad_ref, gq_ref, gk_ref, gv_ref, kt_ref, dk_ref, dv_ref
):
    heads, total, _ = q_ref.shape

    def flip(c, _):
        rows = pl.ds(pl.multiple_of(c * CHUNK, CHUNK), CHUNK)
        for h in range(heads):
            kt_ref[h, :, rows] = k_ref[h, rows, :].astype(F32).T.astype(BF)
        return 0

    lax.fori_loop(0, total // CHUNK, flip, 0)

    def step(c, _):
        attend_back_chunk(
            c, heads, q_ref, k_ref, v_ref, kt_ref, lse_ref, self_ref, att_ref, grad_ref, gq_ref, dk_ref, dv_ref
        )
        return 0

    lax.fori_loop(0, total // CHUNK, step, 0)

    def finish(c, _):
        rows = pl.ds(pl.multiple_of(c * CHUNK, CHUNK), CHUNK)
        keys = [dk_ref[h, rows, :HEAD_DIM] for h in range(heads)]
        values = [dv_ref[h, rows, :HEAD_DIM] for h in range(heads)]
        gk_ref[rows, :] = (jnp.concatenate(keys, axis=1) if heads > 1 else keys[0]).astype(BF)
        gv_ref[rows, :] = (jnp.concatenate(values, axis=1) if heads > 1 else values[0]).astype(BF)
        return 0

    lax.fori_loop(0, total // CHUNK, finish, 0)


def attend_back(q_ext, k_ext, v_ext, lse, self_bias, attended, grad_attended):
    heads, rows, _ = q_ext.shape
    vmem = pl.BlockSpec(memory_space=pltpu.VMEM)
    out = jax.ShapeDtypeStruct(attended.shape, BF)
    return pl.pallas_call(
        back_kernel,
        name="attend_back",
        out_shape=(out, out, out),
        in_specs=[vmem] * 7,
        out_specs=(vmem,) * 3,
        scratch_shapes=[
            pltpu.VMEM((heads, LANES, rows), BF),
            pltpu.VMEM((heads, rows, LANES), F32),
            pltpu.VMEM((heads, rows, LANES), F32),
        ],
        compiler_params=pltpu.CompilerParams(vmem_limit_bytes=VMEM_BYTES),
    )(q_ext, k_ext, v_ext, lse, self_bias, attended, grad_attended)


def body(
    n,
    tokens,
    image_ids,
    lengths,
    w_qkv,
    bias_query,
    bias_value,
    w_out,
    w_up,
    bias_up,
    w_down,
    out_biases,
    norm_gain,
    norm_bias,
    cotangent,
):
    share_rows = tokens.shape[0]
    total_rows = image_ids.shape[0]
    a, b = lax.axis_index("mz"), lax.axis_index("mx")
    chain, cols = mp_parts(n)
    model_index = a * cols + b
    model, hidden = w_up.shape
    width = w_out.shape[0]
    ranks = ("dp", "mz", "mx")

    def shifted(values, off):
        return lax.ppermute(values, "mx", [(i, (i + off) % cols) for i in range(cols)])

    def pair_rows(values):
        return jnp.concatenate([values] + [shifted(values, off) for off in range(1, cols)])

    def pair_sum(partial):
        blocks = jnp.split(partial, cols)
        total = blocks[0].astype(F32)
        for off in range(1, cols):
            total = total + shifted(blocks[off].astype(BF), cols - off).astype(F32)
        return total

    valid_mask = valid_rows(image_ids, lengths[0])
    own_valid = lax.dynamic_slice_in_dim(
        valid_mask.astype(F32), model_index * share_rows, share_rows, 0
    )
    grad_out = cotangent.astype(F32) * own_valid[:, None]
    grad_mlp = pair_rows(grad_out.astype(BF))
    spare = jnp.arange(LANES - HEAD_DIM, dtype=jnp.int32)[None, :]
    is_id = image_ids[:, None] == spare
    tail_q = jnp.where(is_id & (spare < 2), 1.0, 0.0).astype(BF)
    tail_k = jnp.where(spare < 2, jnp.where(is_id & valid_mask[:, None], 0.0, MASKED), 0.0)
    tail_k = tail_k.astype(BF)
    self_bias = jnp.broadcast_to(jnp.where(valid_mask, MASKED, 0.0)[None, :], (8, total_rows))

    inputs_f = tokens.astype(F32)
    (
        gathered_one, q_ext, k_ext, v_ext, log_totals, attended, owned,
        up_all, down_all, out_all, bias_all,
    ) = front(
        n,
        tokens,
        norm_gain[0],
        norm_bias[0],
        w_qkv,
        bias_query,
        bias_value,
        tail_q,
        tail_k,
        self_bias,
        w_up,
        w_down,
        w_out,
        bias_up,
    )
    gathered_one = gathered_one.reshape(total_rows, -1)
    owned = jnp.transpose(owned, (1, 0, 2)).reshape(share_rows, -1)
    out_all = out_all.reshape(model, model)
    bias_all = bias_all[:, 0].reshape(-1)
    hidden_one = (
        inputs_f
        + jnp.dot(owned, out_all, preferred_element_type=F32)
        + out_biases[0]
    )
    normed_two = layer_norm(hidden_one, norm_gain[1], norm_bias[1]).astype(BF)
    rows_two = pair_rows(normed_two)
    pre_act = jnp.dot(rows_two, up_all, preferred_element_type=F32) + bias_all
    activated = exact_gelu(pre_act).astype(BF)
    grad_act = jnp.einsum("rd,fd->rf", grad_mlp, down_all, preferred_element_type=F32)
    _, gelu_back = jax.vjp(exact_gelu, pre_act)
    grad_pre = gelu_back(grad_act)[0].astype(BF)
    grad_normed_two = pair_sum(jnp.einsum("rf,df->rd", grad_pre, up_all, preferred_element_type=F32))
    output_full = (
        hidden_one
        + pair_sum(jnp.dot(activated, down_all, preferred_element_type=F32))
        + out_biases[1]
    )
    grad_up_all = jnp.einsum("rf,rd->fd", grad_pre, rows_two, preferred_element_type=F32)
    grad_down_all = jnp.einsum("rf,rd->fd", activated, grad_mlp, preferred_element_type=F32)
    grad_bias_up = jnp.sum(grad_pre, axis=0, dtype=F32)

    def spread_sum(values):
        part = lax.psum_scatter(
            values.astype(BF), ("mz", "dp"), scatter_dimension=0, tiled=True
        )
        return lax.all_gather(part, "dp", axis=0, tiled=True).astype(F32)

    grad_w_up = spread_sum(grad_up_all).T
    grad_w_down = spread_sum(grad_down_all)
    _, norm_two_back = jax.vjp(layer_norm, hidden_one, norm_gain[1], norm_bias[1])
    grad_from_two, gain_two, shift_two = norm_two_back(grad_normed_two)
    grad_hidden = grad_out + grad_from_two
    grad_proj = lax.all_gather(grad_hidden.astype(BF), ("mz", "mx"), axis=0, tiled=True)
    grad_w_out = jnp.einsum("re,rd->ed", attended, grad_proj, preferred_element_type=F32)
    grad_attended = jnp.einsum("rd,ed->re", grad_proj, w_out, preferred_element_type=F32).astype(BF)
    grad_stack = jnp.stack(
        attend_back(q_ext, k_ext, v_ext, log_totals, self_bias, attended, grad_attended)
    )
    grad_w_qkv = jnp.einsum("rd,tre->tde", gathered_one, grad_stack, preferred_element_type=F32)
    grad_bias_query = jnp.sum(grad_stack[0], axis=0, dtype=F32)
    grad_bias_value = jnp.sum(grad_stack[2], axis=0, dtype=F32)
    grad_normed_one = lax.psum_scatter(
        jnp.einsum("tre,tde->rd", grad_stack, w_qkv, preferred_element_type=F32).astype(BF),
        ("mz", "mx"),
        scatter_dimension=0,
        tiled=True,
    ).astype(F32)
    _, norm_one_back = jax.vjp(layer_norm, inputs_f, norm_gain[0], norm_bias[0])
    grad_from_one, gain_one, shift_one = norm_one_back(grad_normed_one)
    input_grad = (grad_hidden + grad_from_one).astype(BF)

    def placed(values, index, total):
        return lax.dynamic_update_slice_in_dim(
            jnp.zeros((total,), F32), values, index * values.shape[0], 0
        )

    small = [gain_one, gain_two, shift_one, shift_two]
    small += [jnp.sum(grad_hidden, axis=0), jnp.sum(grad_out, axis=0)]
    small += [placed(grad_bias_query, model_index, model), placed(grad_bias_value, model_index, model)]
    bias_rows = lax.dynamic_update_slice(
        jnp.zeros((chain, cols, hidden), F32), grad_bias_up.reshape(chain, 1, hidden), (0, b, 0)
    )
    small = jnp.concatenate([jnp.stack(small), bias_rows.reshape(-1, model)])
    small = lax.psum(small, ranks)
    grad_bias_up = lax.dynamic_slice_in_dim(small[8:].reshape(-1), model_index * hidden, hidden, 0)
    grad_bias_query, grad_bias_value = lax.dynamic_slice_in_dim(
        small[6:8], model_index * width, width, 1
    )
    grad_w_qkv, grad_w_out = (
        lax.psum(grad_w_qkv.astype(BF), "dp").astype(F32),
        lax.psum(grad_w_out.astype(BF), "dp").astype(F32),
    )
    return (
        output_full.astype(BF),
        input_grad,
        grad_w_qkv,
        grad_bias_query,
        grad_bias_value,
        grad_w_out,
        grad_w_up,
        grad_bias_up,
        grad_w_down,
        small[4:6],
        small[0:2],
        small[2:4],
    )


def solution(mesh):
    n = mesh.shape["mp"]
    chain, cols = mp_parts(n)
    split = jax.sharding.Mesh(
        mesh.devices.reshape(mesh.shape["dp"], chain, cols), ("dp", "mz", "mx")
    )
    mp = ("mz", "mx")
    every = ("dp",) + mp
    in_specs = (
        P(every, None),
        P("dp"),
        P("dp", None),
        P(None, None, mp),
        P(mp),
        P(mp),
        P(mp, None),
        P(None, mp),
        P(mp),
        P(mp, None),
        P(),
        P(),
        P(),
        P(every, None),
    )
    out_specs = (
        P(every, None),
        P(every, None),
        P(None, None, mp),
        P(mp),
        P(mp),
        P(mp, None),
        P(None, mp),
        P(mp),
        P(mp, None),
        P(),
        P(),
        P(),
    )
    return jax.shard_map(
        functools.partial(body, n),
        mesh=split,
        in_specs=in_specs,
        out_specs=out_specs,
        check_vma=False,
    )
```

```python
import functools
import types

import jax
import jax.numpy as jnp
from jax import lax
from jax.experimental import pallas as pl
from jax.experimental.pallas import tpu as pltpu
from jax.sharding import PartitionSpec as P

HEAD_DIM = 64
LANES = 128
CHUNK = 768
MASKED = -1e30
MESH = pl.DeviceIdType.MESH
VMEM_BYTES = 67_043_328
BF = jnp.bfloat16
F32 = jnp.float32
NN = (((1,), (0,)), ((), ()))
NT = (((1,), (1,)), ((), ()))
TN = (((0,), (0,)), ((), ()))
SCALE = HEAD_DIM ** (-0.5)
PARTS = 4
epsilon = 1e-06


def dot(left, right, dims=NN):
    return lax.dot_general(left, right, dims, preferred_element_type=F32)


def layer_norm(values, gain_vec, shift_vec):
    row_mean = jnp.mean(values, axis=-1, keepdims=True)
    centered = values - row_mean
    variance = jnp.mean(centered * centered, axis=-1, keepdims=True)
    return centered * lax.rsqrt(variance + epsilon) * gain_vec + shift_vec


def exact_gelu(values):
    return jax.nn.gelu(values, approximate=False)


def valid_rows(image_ids, group_lengths):
    total_rows = image_ids.shape[0]
    row_index = jnp.arange(total_rows, dtype=jnp.int32)
    member = image_ids[:, None] == jnp.arange(2, dtype=jnp.int32)[None, :]
    first_row = jnp.min(jnp.where(member, row_index[:, None], total_rows), axis=0)
    row_start = jnp.sum(jnp.where(member, first_row[None, :], 0), axis=1)
    row_limit = jnp.sum(jnp.where(member, group_lengths[None, :], 0), axis=1)
    return row_index - row_start < row_limit


def mp_parts(n):
    chain = min(4, n)
    return chain, n // chain


def column_sum(values):
    ones = jnp.ones((8, values.shape[1]), BF)
    high = values.astype(BF)
    low = (values - high.astype(F32)).astype(BF)
    return dot(ones, high, NT) + dot(ones, low, NT)


def split_three(column):
    high = column.astype(BF)
    rest = column - high.astype(F32)
    middle = rest.astype(BF)
    return high, middle, (rest - middle.astype(F32)).astype(BF)


def attend_chunk(c, heads, q_ref, k_ref, v_ref, vt_ref, self_ref, att_ref, lse_ref):
    rows = pl.ds(pl.multiple_of(c * CHUNK, CHUNK), CHUNK)
    pieces = []
    scores = [dot(k_ref[h], q_ref[h, rows, :], NT) for h in range(heads)]
    for h in range(heads):
        own = q_ref[h, rows, :HEAD_DIM].astype(F32) * k_ref[h, rows, :HEAD_DIM].astype(F32)
        own = column_sum(own)[:1] + self_ref[:1, rows]
        top = jnp.maximum(jnp.max(scores[h], axis=0, keepdims=True), own)
        weights = jnp.exp(scores[h] - top).astype(BF)
        own_weight = jnp.exp(own - top).astype(BF).astype(F32)
        summed = dot(vt_ref[h], weights) + vt_ref[h, :, rows].astype(F32) * own_weight
        total = summed[HEAD_DIM : HEAD_DIM + 1]
        pieces.append(summed[:HEAD_DIM] / total)
        lse_ref[h, :, rows] = jnp.broadcast_to(top + jnp.log(total), (8, CHUNK))
    stacked = jnp.concatenate(pieces, axis=0) if heads > 1 else pieces[0]
    att_ref[rows, :] = stacked.T.astype(BF)


def front_kernel(
    n,
    tokens_ref,
    gain_ref,
    shift_ref,
    w_ref,
    bq_ref,
    bv_ref,
    tq_ref,
    tk_ref,
    self_ref,
    up_ref,
    down_ref,
    out_ref,
    bup_ref,
    normed_ref,
    q_ref,
    k_ref,
    v_ref,
    lse_ref,
    att_ref,
    owned_ref,
    ups_ref,
    downs_ref,
    outs_ref,
    bups_ref,
    blocks,
    vt_ref,
    owned,
    ssz,
    rsz,
    ssx,
    rsx,
    ssa,
    rsa,
    wsz,
    wrz,
    wsx,
    wrx,
    gs,
    gr,
    os,
    orr,
    bs,
    br,
    local_sem,
):
    chain, cols = mp_parts(n)
    share, _ = tokens_ref.shape
    width = w_ref.shape[2]
    heads = width // HEAD_DIM
    hidden = up_ref.shape[1]
    up_rows, down_rows, out_rows = (r.shape[0] // PARTS for r in (up_ref, down_ref, out_ref))
    dg, dp = lax.axis_index("dg"), lax.axis_index("dp")
    a, b = lax.axis_index("mz"), lax.axis_index("mx")
    me = a * cols + b
    part = lax.rem(dp, PARTS)
    core_dp = dp + 1 - 2 * lax.rem(dp, 2)
    side_dp = dp + 2 - 4 * lax.rem(dp // 2, 2)
    core_part, side_part = lax.rem(core_dp, PARTS), lax.rem(side_dp, PARTS)
    far_part = PARTS - 1 - part

    barrier = pltpu.get_barrier_semaphore()
    for off in range(1, n):
        other = lax.rem(me + off, n)
        pl.semaphore_signal(
            barrier,
            inc=1,
            device_id=(dg, dp, other // cols, lax.rem(other, cols)),
            device_id_type=MESH,
        )
    for peer in (core_dp, side_dp):
        pl.semaphore_signal(barrier, inc=1, device_id=(dg, peer, a, b), device_id_type=MESH)
    pl.semaphore_wait(barrier, n + 1)

    def remote(src, dst, send, recv, device):
        return pltpu.make_async_remote_copy(
            src_ref=src,
            dst_ref=dst,
            send_sem=send,
            recv_sem=recv,
            device_id=(dg,) + device,
            device_id_type=MESH,
        )

    def span(index, size):
        return pl.ds(pl.multiple_of(index * size, size), size)

    def can(way):
        return (a < chain - 1) if way == 0 else (a > 0)

    def chain_peer(way):
        return (dp, jnp.clip(a + (1 if way == 0 else -1), 0, chain - 1), b)

    def cross_peer(off):
        return (dp, a, lax.rem(b + off, cols))

    def chain_copy(block, way):
        spot = blocks.at[block]
        sems = ssz.at[way, block // cols], rsz.at[way, block // cols]
        return remote(spot, spot, *sems, chain_peer(way))

    def cross_copy(block, off):
        spot = blocks.at[block]
        sems = ssx.at[off, block // cols], rsx.at[off, block // cols]
        return remote(spot, spot, *sems, cross_peer(off))

    def piece(i, row, of_part):
        if i == 0:
            return outs_ref.at[row * cols + b, span(of_part, out_rows)]
        if i == 1:
            return ups_ref.at[span(of_part, up_rows), span(row, hidden)]
        return downs_ref.at[span(row * PARTS + of_part, down_rows)]

    def own_piece(i):
        if i == 0:
            return out_ref.at[span(part, out_rows)]
        if i == 1:
            return up_ref.at[span(part, up_rows)]
        return down_ref.at[span(part, down_rows)]

    def weight_copy(i, row, way, own=False):
        spot = piece(i, row, part)
        sems = wsz.at[i, way, row], wrz.at[i, way, row]
        return remote(own_piece(i) if own else spot, spot, *sems, chain_peer(way))

    def out_cross(block, off, own=False):
        spot = outs_ref.at[block, span(part, out_rows)]
        sems = wsx.at[off, block // cols], wrx.at[off, block // cols]
        return remote(own_piece(0) if own else spot, spot, *sems, cross_peer(off))

    def group_copy(kind, i, row, arriving=False):
        sent = side_part if kind == 2 else part
        got = (side_part, core_part, far_part)[kind]
        spot = piece(i, row, got if arriving else sent)
        sems = gs.at[kind, i - 1, row], gr.at[kind, i - 1, row]
        return remote(spot, spot, *sems, (side_dp if kind == 0 else core_dp, a, b))

    def out_group(kind, arriving=False):
        sent = side_part if kind == 2 else part
        got = (side_part, core_part, far_part)[kind]
        spot = outs_ref.at[:, span(got if arriving else sent, out_rows)]
        return remote(spot, spot, os.at[kind], orr.at[kind], (side_dp if kind == 0 else core_dp, a, b))

    def bias_copy(off, arriving=False):
        spot = bups_ref.at[lax.rem(a - off + chain, chain) if arriving else a]
        return remote(bup_ref, spot, bs.at[off], br.at[off], (dp, lax.rem(a + off, chain), b))

    def start_own(way):
        for i in range(3):
            weight_copy(i, a, way, own=True).start()

    stay = [
        pltpu.make_async_copy(up_ref, ups_ref.at[:, span(a, hidden)], local_sem.at[1]),
        pltpu.make_async_copy(down_ref, downs_ref.at[span(a, hidden)], local_sem.at[2]),
        pltpu.make_async_copy(own_piece(0), piece(0, a, part), local_sem.at[3]),
        pltpu.make_async_copy(bup_ref, bups_ref.at[a], local_sem.at[4]),
    ]

    normed = layer_norm(tokens_ref[...].astype(F32), gain_ref[...], shift_ref[...])
    blocks[me] = normed.astype(BF)

    def project(block):
        rows = span(block, share)
        values = blocks[block]
        out_q = (dot(values, w_ref[0]) + bq_ref[...]).astype(BF)
        out_k = dot(values, w_ref[1]).astype(BF)
        out_v = (dot(values, w_ref[2]) + bv_ref[...]).astype(BF)
        lane = lax.broadcasted_iota(jnp.int32, (share, LANES - HEAD_DIM), 1)
        tail_v = jnp.where(lane < 3, 1.0, 0.0).astype(BF)
        for h in range(heads):
            cut = slice(h * HEAD_DIM, (h + 1) * HEAD_DIM)
            q_ref[h, rows, :] = jnp.concatenate(
                [out_q[:, cut] * jnp.asarray(SCALE, BF), tq_ref[rows, :]], axis=1
            )
            k_ref[h, rows, :] = jnp.concatenate([out_k[:, cut], tk_ref[rows, :]], axis=1)
            v_ref[h, rows, :] = jnp.concatenate([out_v[:, cut], tail_v], axis=1)

    for way in (0, 1):

        @pl.when(can(way))
        def _(way=way):
            chain_copy(me, way).start()

    for off in range(1, cols):
        cross_copy(me, off).start()
    for copy in stay:
        copy.start()

    @pl.when(a == 0)
    def _():
        start_own(0)

    @pl.when(a == chain - 1)
    def _():
        start_own(1)

    project(me)

    def visit(step, _):
        for way in (0, 1):
            there = a - step if way == 0 else a + step
            inside = (there >= 0) & (there < chain)
            block = jnp.clip(there, 0, chain - 1) * cols + b

            @pl.when(inside)
            def _(way=way, block=block):
                chain_copy(block, way).wait_recv()

                @pl.when(can(way))
                def _():
                    chain_copy(block, way).start()

                for off in range(1, cols):
                    cross_copy(block, off).start()

        @pl.when((step == a) & can(0))
        def _():
            start_own(0)

        @pl.when((step == chain - 1 - a) & can(1))
        def _():
            start_own(1)

        def one(j, _):
            source = lax.rem(j, 2)
            lag = j // 2
            gone = step - jnp.minimum(lag, 1)
            there = jnp.where(source == 0, a - gone, a + gone)
            fresh = (gone > 0) | ((source == 0) & (lag > 0))
            inside = (there >= 0) & (there < chain) & fresh & (gone < chain)
            row = jnp.clip(there, 0, chain - 1)
            for off in range(1, cols):

                @pl.when(inside & (lag == off))
                def _(off=off):
                    cross_copy(row * cols + lax.rem(b - off + cols, cols), off).wait_recv()

            @pl.when(inside)
            def _():
                project(row * cols + lax.rem(b - lag + cols, cols))

            return 0

        lax.fori_loop(0, 2 * cols, one, 0)
        return 0

    lax.fori_loop(1, chain + 1, visit, 0)

    keep = pltpu.make_async_copy(blocks, normed_ref, local_sem.at[0])
    keep.start()
    for off in range(1, cols):
        out_cross(me, off, own=True).start()
    for off in range(1, chain):
        bias_copy(off).start()

    def both_ways(step, act):
        for way in (0, 1):
            there = a - step if way == 0 else a + step

            @pl.when((there >= 0) & (there < chain))
            def _(way=way, there=there):
                act(way, jnp.clip(there, 0, chain - 1))

    def weights_pass(way, row):
        for i in range(3):
            weight_copy(i, row, way).wait_recv()

            @pl.when(can(way))
            def _(i=i):
                weight_copy(i, row, way).start()

            if i == 0:
                for off in range(1, cols):
                    out_cross(row * cols + b, off).start()
            else:
                group_copy(0, i, row).start()
                group_copy(1, i, row).start()

    def weights_side(way, row):
        for i in (1, 2):
            group_copy(0, i, row, arriving=True).wait_recv()
            group_copy(2, i, row).start()

    both_ways(1, weights_pass)

    def flip(c, _):
        rows = span(c, CHUNK)
        for h in range(heads):
            vt_ref[h, :, rows] = v_ref[h, rows, :].astype(F32).T.astype(BF)
        return 0

    lax.fori_loop(0, n * share // CHUNK, flip, 0)

    def own_copy(target, source):
        return remote(
            att_ref.at[span(target, share)],
            owned.at[source],
            ssa.at[target],
            rsa.at[source],
            (dp, target // cols, lax.rem(target, cols)),
        )

    def attend(c, _):
        attend_chunk(c, heads, q_ref, k_ref, v_ref, vt_ref, self_ref, att_ref, lse_ref)

        def send(target, _):
            end = (target + 1) * share

            @pl.when((end <= (c + 1) * CHUNK) & (end > c * CHUNK) & (target != me))
            def _():
                own_copy(target, me).start()

            return 0

        lax.fori_loop(0, n, send, 0)

        @pl.when(c > 0)
        def _():
            both_ways(c + 1, weights_pass)
            both_ways(c, weights_side)

        return 0

    lax.fori_loop(0, n * share // CHUNK, attend, 0)
    owned[me] = att_ref[span(me, share), :]

    def gather_out(row, _):
        for off in range(1, cols):
            out_cross(row * cols + lax.rem(b - off + cols, cols), off).wait_recv()
        return 0

    lax.fori_loop(0, chain, gather_out, 0)
    stay[2].wait()
    out_group(0).start()
    out_group(1).start()
    both_ways(chain - 1, weights_side)
    out_group(0, arriving=True).wait_recv()
    out_group(2).start()

    def collect(other, _):
        @pl.when(other != me)
        def _():
            own_copy(other, me).wait_send()
            own_copy(me, other).wait_recv()

        return 0

    lax.fori_loop(0, n, collect, 0)
    owned_ref[...] = owned[...]
    keep.wait()
    for i in (0, 1, 3):
        stay[i].wait()
    for off in range(1, chain):
        bias_copy(off).wait_send()
        bias_copy(off, arriving=True).wait_recv()
    for kind in range(3):
        out_group(kind).wait_send()
        if kind > 0:
            out_group(kind, arriving=True).wait_recv()

    def drain(row, _):
        for off in range(1, cols):
            cross_copy(row * cols + b, off).wait_send()
            out_cross(row * cols + b, off).wait_send()

        @pl.when((row <= a) & (a < chain - 1))
        def _():
            chain_copy(row * cols + b, 0).wait_send()
            for i in range(3):
                weight_copy(i, row, 0).wait_send()

        @pl.when((row >= a) & (a > 0))
        def _():
            chain_copy(row * cols + b, 1).wait_send()
            for i in range(3):
                weight_copy(i, row, 1).wait_send()

        @pl.when(row != a)
        def _():
            for i in (1, 2):
                for kind in range(3):
                    group_copy(kind, i, row).wait_send()
                    if kind > 0:
                        group_copy(kind, i, row, arriving=True).wait_recv()

        return 0

    lax.fori_loop(0, chain, drain, 0)


def front(n, tokens, gain, shift, w_qkv, bias_query, bias_value, tail_q, tail_k, self_bias, w_up, w_down, w_out, bias_up):
    chain, cols = mp_parts(n)
    share, model = tokens.shape
    width = w_qkv.shape[2]
    heads = width // HEAD_DIM
    hidden = w_up.shape[1]
    rows = n * share
    vmem = pl.BlockSpec(memory_space=pltpu.VMEM)
    anywhere = pl.BlockSpec(memory_space=pl.ANY)
    ext = jax.ShapeDtypeStruct((heads, rows, LANES), BF)
    dma = pltpu.SemaphoreType.DMA
    return pl.pallas_call(
        functools.partial(front_kernel, n),
        name="front",
        out_shape=(
            jax.ShapeDtypeStruct((n, share, model), BF),
            ext,
            ext,
            ext,
            jax.ShapeDtypeStruct((heads, 8, rows), F32),
            jax.ShapeDtypeStruct((rows, width), BF),
            jax.ShapeDtypeStruct((n, share, width), BF),
            jax.ShapeDtypeStruct((model, chain * hidden), BF),
            jax.ShapeDtypeStruct((chain * hidden, model), BF),
            jax.ShapeDtypeStruct((n, width, model), BF),
            jax.ShapeDtypeStruct((chain, 8, hidden), F32),
        ),
        in_specs=[vmem] * 13,
        out_specs=(anywhere,) + (vmem,) * 6 + (anywhere,) * 4,
        scratch_shapes=[
            pltpu.VMEM((n, share, model), BF),
            pltpu.VMEM((heads, LANES, rows), BF),
            pltpu.VMEM((n, share, width), BF),
            dma((2, chain)),
            dma((2, chain)),
            dma((cols, chain)),
            dma((cols, chain)),
            dma((n,)),
            dma((n,)),
            dma((3, 2, chain)),
            dma((3, 2, chain)),
            dma((cols, chain)),
            dma((cols, chain)),
            dma((3, 2, chain)),
            dma((3, 2, chain)),
            dma((3,)),
            dma((3,)),
            dma((chain,)),
            dma((chain,)),
            dma((5,)),
        ],
        compiler_params=pltpu.CompilerParams(
            collective_id=0, has_side_effects=True, vmem_limit_bytes=VMEM_BYTES
        ),
    )(
        tokens,
        gain[None, :],
        shift[None, :],
        w_qkv,
        bias_query[None, :],
        bias_value[None, :],
        tail_q,
        tail_k,
        self_bias,
        w_up,
        w_down,
        w_out,
        jnp.broadcast_to(bias_up[None, :], (8, hidden)),
    )


def attend_back_chunk(
    c, heads, q_ref, k_ref, v_ref, kt_ref, lse_ref, self_ref, att_ref, grad_ref, gq_ref, dk_ref, dv_ref
):
    rows = pl.ds(pl.multiple_of(c * CHUNK, CHUNK), CHUNK)
    grads = grad_ref[rows, :].astype(F32)
    products = grads * att_ref[rows, :].astype(F32)
    outs = []
    for h in range(heads):
        cut = slice(h * HEAD_DIM, (h + 1) * HEAD_DIM)
        inner = jnp.sum(products[:, cut], axis=1, keepdims=True)
        parts = split_three(-inner)
        lane = lax.broadcasted_iota(jnp.int32, (CHUNK, LANES - HEAD_DIM), 1)
        tail = jnp.zeros((CHUNK, LANES - HEAD_DIM), F32)
        for i, part in enumerate(parts):
            tail = jnp.where(lane == i, part.astype(F32), tail)
        grad_ext = jnp.concatenate([grads[:, cut], tail], axis=1).astype(BF)
        query = q_ref[h, rows, :]
        key_own = k_ref[h, rows, :]
        scores = dot(k_ref[h], query, NT)
        lse = lse_ref[h, :1, rows]
        probs = jnp.exp(scores - lse)
        shifted = dot(v_ref[h], grad_ext, NT)
        own = column_sum(query[:, :HEAD_DIM].astype(F32) * key_own[:, :HEAD_DIM].astype(F32))
        own_prob = jnp.exp(own + self_ref[:, rows] - lse)
        own_shifted = column_sum(v_ref[h, rows, :].astype(F32) * grad_ext.astype(F32))
        lower = lax.broadcasted_iota(jnp.int32, (8, CHUNK), 0) < 4
        both = jnp.where(lower, own_prob, own_prob * own_shifted).T
        own_prob, own_score = both[:, :1], both[:, 4:5]
        grad_scores = (probs * shifted).astype(BF)
        dv = dot(probs.astype(BF), grad_ext)
        dk = dot(grad_scores, query)
        dq = dot(kt_ref[h], grad_scores).T
        dq = (dq + own_score * key_own.astype(F32)) * SCALE
        outs.append(dq[:, :HEAD_DIM])

        @pl.when(c == 0)
        def _(h=h, dv=dv, dk=dk):
            dv_ref[h] = dv
            dk_ref[h] = dk

        @pl.when(c > 0)
        def _(h=h, dv=dv, dk=dk):
            dv_ref[h] += dv
            dk_ref[h] += dk

        dv_ref[h, rows, :] += own_prob * grad_ext.astype(F32)
        dk_ref[h, rows, :] += own_score * query.astype(F32)
    stacked = jnp.concatenate(outs, axis=1) if heads > 1 else outs[0]
    gq_ref[rows, :] = stacked.astype(BF)


REAR_REFS = (
    "gatt",
    "q",
    "k",
    "v",
    "lse",
    "self_bias",
    "att",
    "w",
    "normed",
    "tokens",
    "grad_hidden",
    "gain",
    "early",
    "up",
    "down",
    "out",
    "up_sum",
    "head_sum",
    "bias_out",
    "input_grad",
    "small_out",
    "grad",
    "kt",
    "dk",
    "dv",
    "gq",
    "gk",
    "gv",
    "kept",
    "pool_core",
    "pool_side",
    "way_in",
    "done",
    "out_in",
    "local",
    "local_in",
    "local_side",
    "local_done",
    "acc",
    "cross_in",
    "way_gn",
    "gn",
    "small",
    "small_in",
    "bias_sum",
    "bias_in",
    "sa",
    "ra",
    "so",
    "ro",
    "sc",
    "rc",
    "sk",
    "ss",
    "rs",
    "sz",
    "rz",
    "sg",
    "rg",
    "st",
    "rt",
    "sy",
    "ry",
    "sh",
    "rh",
    "sx",
    "rx",
    "sn",
    "rn",
    "sm",
    "rm",
    "sb",
    "rb",
    "sl",
)


def rear_kernel(n, *refs):
    r = types.SimpleNamespace(**dict(zip(REAR_REFS, refs)))
    chain, cols = mp_parts(n)
    heads, total, _ = r.q.shape
    _, share, width = r.gatt.shape
    model = r.w.shape[1]
    hidden = r.up.shape[0] // chain
    rows = hidden // PARTS
    dg, dp = lax.axis_index("dg"), lax.axis_index("dp")
    a, b = lax.axis_index("mz"), lax.axis_index("mx")
    me = a * cols + b
    part = lax.rem(dp, PARTS)
    core_dp = dp + 1 - 2 * lax.rem(dp, 2)
    side_dp = dp + 2 - 4 * lax.rem(dp // 2, 2)
    core_part, side_part = lax.rem(core_dp, PARTS), lax.rem(side_dp, PARTS)
    far_part = PARTS - 1 - part
    core_id, side_id = (core_dp, a, b), (side_dp, a, b)

    def mp_id(index):
        return dp, index // cols, lax.rem(index, cols)

    barrier = pltpu.get_barrier_semaphore()
    for off in range(1, n):
        pl.semaphore_signal(
            barrier, inc=1, device_id=(dg,) + mp_id(lax.rem(me + off, n)), device_id_type=MESH
        )
    for peer in (core_id, side_id):
        pl.semaphore_signal(barrier, inc=1, device_id=(dg,) + peer, device_id_type=MESH)
    pl.semaphore_wait(barrier, n + 1)

    def remote(src, dst, send, recv, device):
        return pltpu.make_async_remote_copy(
            src_ref=src,
            dst_ref=dst,
            send_sem=send,
            recv_sem=recv,
            device_id=(dg,) + device,
            device_id_type=MESH,
        )

    def span(index, size):
        return pl.ds(pl.multiple_of(index * size, size), size)

    def in_order(i):
        return jnp.where(lax.rem(i, 2) == 0, i // 2, chain - 1 - i // 2)

    def first_service(t):
        return chain - 1 - jnp.maximum(t, chain - 1 - t)

    def add_rows(dst, *terms):
        count = dst.shape[0]
        step = 32 if count % 32 == 0 else 16

        def one(i, _):
            cut = span(i, step)
            value = terms[0][cut, :].astype(F32)
            for term in terms[1:]:
                value = value + term[cut, :].astype(F32)
            dst[cut, :] = value.astype(dst.dtype)
            return 0

        lax.fori_loop(0, count // step, one, 0)

    def loop(count, act):
        def one(i, _):
            act(i)
            return 0

        lax.fori_loop(0, count, one, 0)

    def others(act):
        def one(m):
            @pl.when(m != me)
            def _():
                act(m)

        loop(n, one)

    def row_copy(target, source):
        return remote(
            r.gatt.at[target], r.grad.at[span(source, share)], r.sa.at[target], r.ra.at[source], mp_id(target)
        )

    def out_copy(target, source):
        return remote(r.out.at[target], r.out_in.at[source], r.so.at[target], r.ro.at[source], mp_id(target))

    def source_rows(i, t, which):
        return (r.up, r.down)[i].at[span(t * PARTS + which, rows)]

    def core_copy(t, slot, i):
        return remote(
            source_rows(i, t, far_part if slot else core_part),
            r.pool_core.at[span((t * 2 + slot) * 2 + i, rows)],
            r.sc.at[t, slot, i],
            r.rc.at[t, slot, i],
            core_id,
        )

    def keep_copy(t, slot, i):
        return pltpu.make_async_copy(
            source_rows(i, t, side_part if slot else part),
            r.kept.at[t, slot, pl.ds(i * rows, rows)],
            r.sk.at[t, slot, i],
        )

    def side_copy(t):
        return remote(r.kept.at[t, 1], r.pool_side.at[span(t, 2 * rows)], r.ss.at[t], r.rs.at[t], side_id)

    def chain_id(way):
        return dp, jnp.clip(a + (1 if way == 0 else -1), 0, chain - 1), b

    def hop_of(way):
        return a if way == 0 else chain - 1 - a

    def ahead(way, t):
        return (t > a) if way == 0 else (t < a)

    def chain_copy(flow, way, t, fresh=False):
        own, inbox, send, recv = flow
        spot = inbox.at[way, t]
        return remote(own(t) if fresh else spot, spot, send.at[way, t], recv.at[way, t], chain_id(way))

    def chain_service(flow, s, prepare):
        own, inbox = flow[:2]

        def one(i):
            t = in_order(i)

            @pl.when(s == first_service(t))
            def _():
                prepare(t)

            for way in (0, 1):
                hop = hop_of(way)
                active = ahead(way, t) & (s == first_service(t) + hop)

                @pl.when(active & (hop == 0))
                def _(way=way):
                    chain_copy(flow, way, t, fresh=True).start()

                @pl.when(active & (hop > 0))
                def _(way=way):
                    chain_copy(flow, way, t).wait_recv()
                    add_rows(inbox.at[way, t], inbox.at[way, t], own(t))
                    chain_copy(flow, way, t).start()

        loop(chain, one)

    def chain_finish(flow, dst):
        own, inbox = flow[:2]

        @pl.when(a > 0)
        def _():
            chain_copy(flow, 0, a).wait_recv()

        @pl.when(a < chain - 1)
        def _():
            chain_copy(flow, 1, a).wait_recv()

        @pl.when((a > 0) & (a < chain - 1))
        def _():
            add_rows(dst, own(a), inbox.at[0, a], inbox.at[1, a])

        @pl.when(a == 0)
        def _():
            add_rows(dst, own(a), inbox.at[1, a])

        @pl.when(a == chain - 1)
        def _():
            add_rows(dst, own(a), inbox.at[0, a])

    def chain_drain(flow):
        def one(t):
            for way in (0, 1):

                @pl.when(ahead(way, t))
                def _(way=way):
                    chain_copy(flow, way, t).wait_send()

        loop(chain, one)

    def share_copy(share_flow, kind, arriving=False):
        own, everyone, send, recv = share_flow
        sent = side_part if kind == 2 else part
        got = (side_part, core_part, far_part)[kind]
        spot = everyone.at[got if arriving else sent]
        src = spot if kind == 2 or arriving else own
        return remote(src, spot, send.at[kind], recv.at[kind], side_id if kind == 0 else core_id)

    weights = (lambda t: r.kept.at[t, 0], r.way_in, r.sz, r.rz)
    grads = (lambda t: r.pool_side.at[span(t, share)], r.way_gn, r.sn, r.rn)
    share_weights = (r.done, r.up_sum, r.sg, r.rg)
    share_local = (r.local_done, r.head_sum, r.sh, r.rh)

    def small_peers(stage):
        if stage == 0:
            return [core_id]
        if stage == 1:
            return [side_id]
        if stage == 2:
            return [(dp, a, lax.rem(b + off, cols)) for off in range(1, cols)]
        return [(dp, lax.rem(a + off, chain), b) for off in range(1, chain)]

    def small_copies(which, stage):
        src = r.early if which == 0 and stage == 0 else r.small.at[which, stage]
        return [
            remote(src, r.small_in.at[which, stage, i], r.sm.at[which, stage, i], r.rm.at[which, stage, i], peer)
            for i, peer in enumerate(small_peers(stage))
        ]

    def small_start(which, stage):
        for copy in small_copies(which, stage):
            copy.start()

    def small_sum(which, stage):
        value = r.early[...] if which == 0 and stage == 0 else r.small[which, stage]
        for i, copy in enumerate(small_copies(which, stage)):
            copy.wait_recv()
            value = value + r.small_in[which, stage, i]
        if stage < 3:
            r.small[which, stage + 1] = value
            small_start(which, stage + 1)
        else:
            r.small_out[which] = value

    def bias_copy(stage):
        return remote(
            r.bias_sum.at[stage], r.bias_in.at[stage], r.sb.at[stage], r.rb.at[stage], (core_id, side_id)[stage]
        )

    others(lambda m: row_copy(m, me).start())
    small_start(0, 0)

    def start_core(i):
        t = in_order(i)
        for slot in (1, 0):
            for k in (0, 1):
                core_copy(t, slot, k).start()
                keep_copy(t, slot, k).start()

    loop(chain, start_core)
    others(lambda m: out_copy(m, me).start())
    out_keep = pltpu.make_async_copy(r.out.at[me], r.out_in.at[me], r.sl.at[0])
    out_keep.start()
    r.grad[span(me, share), :] = r.gatt[me]

    def flip(c):
        cut = span(c, CHUNK)
        for h in range(heads):
            r.kt[h, :, cut] = r.k[h, cut, :].astype(F32).T.astype(BF)

    loop(total // CHUNK, flip)

    def core_sum(i):
        t = in_order(i)
        for slot in (1, 0):
            for k in (0, 1):
                keep_copy(t, slot, k).wait()
                core_copy(t, slot, k).wait_recv()
            add_rows(r.kept.at[t, slot], r.kept.at[t, slot], r.pool_core.at[span(t * 2 + slot, 2 * rows)])
            if slot == 1:
                side_copy(t).start()

    loop(chain, core_sum)
    small_sum(0, 0)
    others(lambda m: row_copy(me, m).wait_recv())

    def side_sum(t):
        side_copy(t).wait_recv()
        add_rows(r.kept.at[t, 0], r.kept.at[t, 0], r.pool_side.at[span(t, 2 * rows)])

    def attend(c):
        attend_back_chunk(
            c, heads, r.q, r.k, r.v, r.kt, r.lse, r.self_bias, r.att, r.grad, r.gq, r.dk, r.dv
        )
        chain_service(weights, c, side_sum)

    loop(total // CHUNK, attend)

    def finish(c):
        cut = span(c, CHUNK)
        for src, dst in ((r.dk, r.gk), (r.dv, r.gv)):
            parts = [src[h, cut, :HEAD_DIM] for h in range(heads)]
            dst[cut, :] = (jnp.concatenate(parts, axis=1) if heads > 1 else parts[0]).astype(BF)

    loop(total // CHUNK, finish)

    def partial_rows(block):
        cut = span(block, share)
        value = dot(r.gq[cut, :], r.w[0], NT) + dot(r.gk[cut, :], r.w[1], NT)
        return (value + dot(r.gv[cut, :], r.w[2], NT)).astype(BF)

    def cross_copy(lag, t):
        return remote(
            r.pool_core.at[span((lag - 1) * chain + t, share)],
            r.cross_in.at[lag - 1, t],
            r.sx.at[lag, t],
            r.rx.at[lag, t],
            (dp, a, lax.rem(b + lag, cols)),
        )

    def cross_part(i):
        t = in_order(i)

        def one(lag):
            r.pool_core[span(lag * chain + t, share), :] = partial_rows(t * cols + lax.rem(b + 1 + lag, cols))
            for fixed in range(1, cols):

                @pl.when(lag + 1 == fixed)
                def _(fixed=fixed):
                    cross_copy(fixed, t).start()

        loop(cols - 1, one)

    def own_part(t):
        r.pool_side[span(t, share), :] = partial_rows(t * cols + b)

    small_sum(0, 1)
    loop(chain, cross_part)
    loop(chain, own_part)
    chain_finish(weights, r.done)
    for kind in (0, 1):
        share_copy(share_weights, kind).start()
    weights_keep = pltpu.make_async_copy(r.done, r.up_sum.at[part], r.sl.at[1])
    weights_keep.start()

    def head_grads(c):
        cut = span(c, CHUNK)
        for t, src in enumerate((r.gq, r.gk, r.gv)):
            value = dot(src[cut, :], r.normed[cut, :], TN)

            @pl.when(c == 0)
            def _(t=t, value=value):
                r.acc[t] = value

            @pl.when(c > 0)
            def _(t=t, value=value):
                r.acc[t] += value

        ones = jnp.ones((8, CHUNK), BF)
        for t, src in ((0, r.gq), (1, r.gv)):
            value = dot(ones, src[cut, :])

            @pl.when(c == 0)
            def _(t=t, value=value):
                r.bias_sum[0, t] = value

            @pl.when(c > 0)
            def _(t=t, value=value):
                r.bias_sum[0, t] += value

    loop(total // CHUNK, head_grads)
    for t in range(3):
        r.local[1 + t] = r.acc[t].astype(BF)
    out_keep.wait()
    others(lambda m: out_copy(me, m).wait_recv())
    add_rows(r.local.at[0], *[r.out_in.at[m] for m in range(n)])

    def local_core(slot):
        return remote(
            r.local.at[far_part if slot else core_part], r.local_in.at[slot], r.st.at[slot], r.rt.at[slot], core_id
        )

    local_side = remote(r.local.at[side_part], r.local_side, r.sy.at[0], r.ry.at[0], side_id)
    for slot in (1, 0):
        local_core(slot).start()
    bias_copy(0).start()
    small_sum(0, 2)

    def cross_sum(t):
        for lag in range(1, cols):
            cross_copy(lag, t).wait_recv()
        own = grads[0](t)
        add_rows(own, own, *[r.cross_in.at[lag - 1, t] for lag in range(1, cols)])

    chain_service(grads, 0, cross_sum)
    for slot in (1, 0):
        local_core(slot).wait_recv()
        spot = r.local.at[side_part if slot else part]
        add_rows(spot, spot, r.local_in.at[slot])
        if slot == 1:
            local_side.start()
    bias_copy(0).wait_recv()
    r.bias_sum[1] = r.bias_sum[0] + r.bias_in[0]
    bias_copy(1).start()
    share_copy(share_weights, 0, arriving=True).wait_recv()
    share_copy(share_weights, 2).start()
    chain_service(grads, 1, cross_sum)
    local_side.wait_recv()
    bias_copy(1).wait_recv()
    r.bias_out[...] = r.bias_sum[1] + r.bias_in[1]
    add_rows(r.local_done, r.local.at[part], r.local_side)
    for kind in (0, 1):
        share_copy(share_local, kind).start()
    local_keep = pltpu.make_async_copy(r.local_done, r.head_sum.at[part], r.sl.at[2])
    local_keep.start()

    def later(s, _):
        chain_service(grads, s, cross_sum)
        return 0

    lax.fori_loop(2, chain - 1, later, 0)
    share_copy(share_local, 0, arriving=True).wait_recv()
    share_copy(share_local, 2).start()
    chain_finish(grads, r.gn)
    step = 32 if share % 32 == 0 else 16

    def norm_back(i, sums):
        cut = span(i, step)
        values = r.tokens[cut, :].astype(F32)
        grad = r.gn[cut, :]
        centered = values - jnp.mean(values, axis=-1, keepdims=True)
        scale = lax.rsqrt(jnp.mean(centered * centered, axis=-1, keepdims=True) + epsilon)
        unit = centered * scale
        scaled = grad * r.gain[...]
        along = jnp.mean(scaled * unit, axis=-1, keepdims=True)
        back = (scaled - jnp.mean(scaled, axis=-1, keepdims=True) - unit * along) * scale
        r.input_grad[cut, :] = (r.grad_hidden[cut, :] + back).astype(BF)
        gains = jnp.sum(grad * unit, axis=0, keepdims=True)
        return sums[0] + gains, sums[1] + jnp.sum(grad, axis=0, keepdims=True)

    zero = jnp.zeros((1, model), F32)
    gains, shifts = lax.fori_loop(0, share // step, norm_back, (zero, zero))
    upper = lax.broadcasted_iota(jnp.int32, (8, model), 0) == 0
    r.small[1, 0] = jnp.where(upper, gains, shifts)
    small_start(1, 0)
    small_sum(0, 3)
    for stage in range(4):
        small_sum(1, stage)

    weights_keep.wait()
    local_keep.wait()
    for flow in (share_weights, share_local):
        for kind in range(3):
            share_copy(flow, kind).wait_send()
            if kind > 0:
                share_copy(flow, kind, arriving=True).wait_recv()
    for slot in (1, 0):
        local_core(slot).wait_send()
    local_side.wait_send()
    for stage in range(2):
        bias_copy(stage).wait_send()
    for which in range(2):
        for stage in range(4):
            for copy in small_copies(which, stage):
                copy.wait_send()
    others(lambda m: row_copy(m, me).wait_send())
    others(lambda m: out_copy(m, me).wait_send())
    chain_drain(weights)
    chain_drain(grads)

    def drain(t):
        side_copy(t).wait_send()
        for slot in (1, 0):
            for k in (0, 1):
                core_copy(t, slot, k).wait_send()
        for lag in range(1, cols):
            cross_copy(lag, t).wait_send()

    loop(chain, drain)


def rear(
    n, grad_rows, q_ext, k_ext, v_ext, lse, self_bias, attended, w_qkv, normed, tokens, grad_hidden, gain, early,
    grad_up, grad_down, grad_out,
):
    chain, cols = mp_parts(n)
    heads, total, _ = q_ext.shape
    _, share, width = grad_rows.shape
    model = w_qkv.shape[1]
    rows = 2 * (grad_up.shape[0] // chain // PARTS)
    vmem = pl.BlockSpec(memory_space=pltpu.VMEM)
    anywhere = pl.BlockSpec(memory_space=pl.ANY)
    dma = pltpu.SemaphoreType.DMA
    head = pltpu.VMEM((total, width), BF)
    most = max(chain, cols) - 1
    return pl.pallas_call(
        functools.partial(rear_kernel, n),
        name="rear",
        out_shape=(
            jax.ShapeDtypeStruct((PARTS, rows, model), BF),
            jax.ShapeDtypeStruct((PARTS, width, model), BF),
            jax.ShapeDtypeStruct((2, 8, width), F32),
            jax.ShapeDtypeStruct((share, model), BF),
            jax.ShapeDtypeStruct((2, 8, model), F32),
        ),
        in_specs=[vmem] * 13 + [anywhere] * 3,
        out_specs=(anywhere, anywhere, vmem, vmem, vmem),
        scratch_shapes=[
            head,
            pltpu.VMEM((heads, LANES, total), BF),
            pltpu.VMEM((heads, total, LANES), F32),
            pltpu.VMEM((heads, total, LANES), F32),
            head,
            head,
            head,
            pltpu.VMEM((chain, 2, rows, model), BF),
            pltpu.VMEM((max(chain * 2 * rows, (cols - 1) * chain * share), model), BF),
            pltpu.VMEM((max(chain * rows, chain * share), model), BF),
            pltpu.VMEM((2, chain, rows, model), BF),
            pltpu.VMEM((rows, model), BF),
            pltpu.VMEM((n, width, model), BF),
            pltpu.VMEM((PARTS, width, model), BF),
            pltpu.VMEM((2, width, model), BF),
            pltpu.VMEM((width, model), BF),
            pltpu.VMEM((width, model), BF),
            pltpu.VMEM((3, width, model), F32),
            pltpu.VMEM((cols - 1, chain, share, model), BF),
            pltpu.VMEM((2, chain, share, model), BF),
            pltpu.VMEM((share, model), F32),
            pltpu.VMEM((2, 4, 8, model), F32),
            pltpu.VMEM((2, 4, most, 8, model), F32),
            pltpu.VMEM((2, 2, 8, width), F32),
            pltpu.VMEM((2, 2, 8, width), F32),
            dma((n,)),
            dma((n,)),
            dma((n,)),
            dma((n,)),
            dma((chain, 2, 2)),
            dma((chain, 2, 2)),
            dma((chain, 2, 2)),
            dma((chain,)),
            dma((chain,)),
            dma((2, chain)),
            dma((2, chain)),
            dma((3,)),
            dma((3,)),
            dma((2,)),
            dma((2,)),
            dma((1,)),
            dma((1,)),
            dma((3,)),
            dma((3,)),
            dma((cols, chain)),
            dma((cols, chain)),
            dma((2, chain)),
            dma((2, chain)),
            dma((2, 4, most)),
            dma((2, 4, most)),
            dma((2,)),
            dma((2,)),
            dma((3,)),
        ],
        compiler_params=pltpu.CompilerParams(
            collective_id=1, has_side_effects=True, vmem_limit_bytes=VMEM_BYTES
        ),
    )(
        grad_rows, q_ext, k_ext, v_ext, lse, self_bias, attended, w_qkv, normed, tokens, grad_hidden,
        gain[None, :], early, grad_up, grad_down, grad_out,
    )


def body(
    n,
    groups,
    tokens,
    image_ids,
    lengths,
    w_qkv,
    bias_query,
    bias_value,
    w_out,
    w_up,
    bias_up,
    w_down,
    out_biases,
    norm_gain,
    norm_bias,
    cotangent,
):
    share_rows = tokens.shape[0]
    total_rows = image_ids.shape[0]
    a, b = lax.axis_index("mz"), lax.axis_index("mx")
    chain, cols = mp_parts(n)
    model_index = a * cols + b
    model, hidden = w_up.shape
    width = w_out.shape[0]

    def shifted(values, off):
        return lax.ppermute(values, "mx", [(i, (i + off) % cols) for i in range(cols)])

    def pair_rows(values):
        return jnp.concatenate([values] + [shifted(values, off) for off in range(1, cols)])

    def pair_sum(partial):
        blocks = jnp.split(partial, cols)
        total = blocks[0].astype(F32)
        for off in range(1, cols):
            total = total + shifted(blocks[off].astype(BF), cols - off).astype(F32)
        return total

    valid_mask = valid_rows(image_ids, lengths[0])
    own_valid = lax.dynamic_slice_in_dim(
        valid_mask.astype(F32), model_index * share_rows, share_rows, 0
    )
    grad_out = cotangent.astype(F32) * own_valid[:, None]
    grad_mlp = pair_rows(grad_out.astype(BF))
    spare = jnp.arange(LANES - HEAD_DIM, dtype=jnp.int32)[None, :]
    is_id = image_ids[:, None] == spare
    tail_q = jnp.where(is_id & (spare < 2), 1.0, 0.0).astype(BF)
    tail_k = jnp.where(spare < 2, jnp.where(is_id & valid_mask[:, None], 0.0, MASKED), 0.0)
    tail_k = tail_k.astype(BF)
    self_bias = jnp.broadcast_to(jnp.where(valid_mask, MASKED, 0.0)[None, :], (8, total_rows))

    inputs_f = tokens.astype(F32)
    (
        gathered_one, q_ext, k_ext, v_ext, log_totals, attended, owned,
        up_all, down_all, out_all, bias_all,
    ) = front(
        n,
        tokens,
        norm_gain[0],
        norm_bias[0],
        w_qkv,
        bias_query,
        bias_value,
        tail_q,
        tail_k,
        self_bias,
        w_up,
        w_down,
        w_out,
        bias_up,
    )
    gathered_one = gathered_one.reshape(total_rows, -1)
    owned = jnp.transpose(owned, (1, 0, 2)).reshape(share_rows, -1)
    out_all = out_all.reshape(model, model)
    bias_all = bias_all[:, 0].reshape(-1)
    hidden_one = (
        inputs_f
        + jnp.dot(owned, out_all, preferred_element_type=F32)
        + out_biases[0]
    )
    normed_two = layer_norm(hidden_one, norm_gain[1], norm_bias[1]).astype(BF)
    rows_two = pair_rows(normed_two)
    pre_act = jnp.dot(rows_two, up_all, preferred_element_type=F32) + bias_all
    activated = exact_gelu(pre_act).astype(BF)
    grad_act = jnp.einsum("rd,fd->rf", grad_mlp, down_all, preferred_element_type=F32)
    _, gelu_back = jax.vjp(exact_gelu, pre_act)
    grad_pre = gelu_back(grad_act)[0].astype(BF)
    grad_normed_two = pair_sum(jnp.einsum("rf,df->rd", grad_pre, up_all, preferred_element_type=F32))
    output_full = (
        hidden_one
        + pair_sum(jnp.dot(activated, down_all, preferred_element_type=F32))
        + out_biases[1]
    )
    grad_up_all = jnp.einsum("rf,rd->fd", grad_pre, rows_two, preferred_element_type=F32)
    grad_down_all = jnp.einsum("rf,rd->fd", activated, grad_mlp, preferred_element_type=F32)
    grad_bias_up = jnp.sum(grad_pre, axis=0, dtype=F32)

    _, norm_two_back = jax.vjp(layer_norm, hidden_one, norm_gain[1], norm_bias[1])
    grad_from_two, gain_two, shift_two = norm_two_back(grad_normed_two)
    grad_hidden = grad_out + grad_from_two
    grad_proj = grad_hidden.astype(BF)
    grad_w_out = jnp.einsum("re,rd->ed", owned, grad_proj, preferred_element_type=F32).astype(BF)
    grad_rows = jnp.einsum(
        "rd,ned->nre", grad_proj, out_all.reshape(n, width, model), preferred_element_type=F32
    ).astype(BF)
    bias_rows = lax.dynamic_update_slice(
        jnp.zeros((chain, cols, hidden), F32), grad_bias_up.reshape(chain, 1, hidden), (0, b, 0)
    )
    early = [gain_two, shift_two, jnp.sum(grad_hidden, axis=0), jnp.sum(grad_out, axis=0)]
    early = jnp.concatenate([jnp.stack(early), bias_rows.reshape(-1, model)])
    hidden_sum, head_sum, bias_sum, input_grad, small = rear(
        n,
        grad_rows,
        q_ext,
        k_ext,
        v_ext,
        log_totals,
        self_bias,
        attended,
        w_qkv,
        gathered_one,
        tokens,
        grad_hidden,
        norm_gain[0],
        early,
        grad_up_all.astype(BF),
        grad_down_all.astype(BF),
        grad_w_out.reshape(n, width, model),
    )
    if groups > 1:
        hidden_sum, head_sum, bias_sum, small = lax.psum((hidden_sum, head_sum, bias_sum, small), "dg")
    half = hidden // PARTS
    grad_w_up = hidden_sum[:, :half].reshape(hidden, model).T.astype(F32)
    grad_w_down = hidden_sum[:, half:].reshape(hidden, model).astype(F32)
    grad_w_out = head_sum[0].astype(F32)
    grad_w_qkv = jnp.transpose(head_sum[1:], (0, 2, 1)).astype(F32)
    grad_bias_query, grad_bias_value = bias_sum[:, 0]
    grad_bias_up = lax.dynamic_slice_in_dim(
        small[0, 4:].reshape(-1), model_index * hidden, hidden, 0
    )
    return (
        output_full.astype(BF),
        input_grad,
        grad_w_qkv,
        grad_bias_query,
        grad_bias_value,
        grad_w_out,
        grad_w_up,
        grad_bias_up,
        grad_w_down,
        small[0, 2:4],
        jnp.stack([small[1, 0], small[0, 0]]),
        jnp.stack([small[1, 1], small[0, 1]]),
    )


def solution(mesh):
    n = mesh.shape["mp"]
    chain, cols = mp_parts(n)
    groups = mesh.shape["dp"] // PARTS
    dp, mp = ("dg", "dp"), ("mz", "mx")
    every = dp + mp
    split = jax.sharding.Mesh(mesh.devices.reshape(groups, PARTS, chain, cols), every)
    in_specs = (
        P(every, None),
        P(dp),
        P(dp, None),
        P(None, None, mp),
        P(mp),
        P(mp),
        P(mp, None),
        P(None, mp),
        P(mp),
        P(mp, None),
        P(),
        P(),
        P(),
        P(every, None),
    )
    out_specs = (
        P(every, None),
        P(every, None),
        P(None, None, mp),
        P(mp),
        P(mp),
        P(mp, None),
        P(None, mp),
        P(mp),
        P(mp, None),
        P(),
        P(),
        P(),
    )
    return jax.shard_map(
        functools.partial(body, n, groups),
        mesh=split,
        in_specs=in_specs,
        out_specs=out_specs,
        check_vma=False,
    )
```

```python
import functools
import types

import jax
import jax.numpy as jnp
from jax import lax
from jax.experimental import pallas as pl
from jax.experimental.pallas import tpu as pltpu
from jax.sharding import PartitionSpec as P

HEAD_DIM = 64
LANES = 128
CHUNK = 768
MASKED = -1e30
MESH = pl.DeviceIdType.MESH
VMEM_BYTES = 67_043_328
BF = jnp.bfloat16
F32 = jnp.float32
NN = (((1,), (0,)), ((), ()))
NT = (((1,), (1,)), ((), ()))
TN = (((0,), (0,)), ((), ()))
SCALE = HEAD_DIM ** (-0.5)
PARTS = 4
epsilon = 1e-06


def dot(left, right, dims=NN):
    return lax.dot_general(left, right, dims, preferred_element_type=F32)


def layer_norm(values, gain_vec, shift_vec):
    row_mean = jnp.mean(values, axis=-1, keepdims=True)
    centered = values - row_mean
    variance = jnp.mean(centered * centered, axis=-1, keepdims=True)
    return centered * lax.rsqrt(variance + epsilon) * gain_vec + shift_vec


def exact_gelu(values):
    return jax.nn.gelu(values, approximate=False)


def valid_rows(image_ids, group_lengths):
    total_rows = image_ids.shape[0]
    row_index = jnp.arange(total_rows, dtype=jnp.int32)
    member = image_ids[:, None] == jnp.arange(2, dtype=jnp.int32)[None, :]
    first_row = jnp.min(jnp.where(member, row_index[:, None], total_rows), axis=0)
    row_start = jnp.sum(jnp.where(member, first_row[None, :], 0), axis=1)
    row_limit = jnp.sum(jnp.where(member, group_lengths[None, :], 0), axis=1)
    return row_index - row_start < row_limit


def mp_parts(n):
    chain = min(4, n)
    return chain, n // chain


def column_sum(values):
    ones = jnp.ones((8, values.shape[1]), BF)
    high = values.astype(BF)
    low = (values - high.astype(F32)).astype(BF)
    return dot(ones, high, NT) + dot(ones, low, NT)


def split_three(column):
    high = column.astype(BF)
    rest = column - high.astype(F32)
    middle = rest.astype(BF)
    return high, middle, (rest - middle.astype(F32)).astype(BF)


def attend_chunk(c, heads, q_ref, k_ref, v_ref, vt_ref, self_ref, att_ref, lse_ref):
    rows = pl.ds(pl.multiple_of(c * CHUNK, CHUNK), CHUNK)
    pieces = []
    scores = [dot(k_ref[h], q_ref[h, rows, :], NT) for h in range(heads)]
    for h in range(heads):
        own = q_ref[h, rows, :HEAD_DIM].astype(F32) * k_ref[h, rows, :HEAD_DIM].astype(F32)
        own = column_sum(own)[:1] + self_ref[:1, rows]
        top = jnp.maximum(jnp.max(scores[h], axis=0, keepdims=True), own)
        weights = jnp.exp(scores[h] - top).astype(BF)
        own_weight = jnp.exp(own - top).astype(BF).astype(F32)
        summed = dot(vt_ref[h], weights) + vt_ref[h, :, rows].astype(F32) * own_weight
        total = summed[HEAD_DIM : HEAD_DIM + 1]
        pieces.append(summed[:HEAD_DIM] / total)
        lse_ref[h, :, rows] = jnp.broadcast_to(top + jnp.log(total), (8, CHUNK))
    stacked = jnp.concatenate(pieces, axis=0) if heads > 1 else pieces[0]
    att_ref[rows, :] = stacked.T.astype(BF)


def front_kernel(
    n,
    tokens_ref,
    gain_ref,
    shift_ref,
    w_ref,
    bias_ref,
    tq_ref,
    tk_ref,
    self_ref,
    up_ref,
    down_ref,
    out_ref,
    bup_ref,
    normed_ref,
    q_ref,
    k_ref,
    v_ref,
    lse_ref,
    att_ref,
    owned_ref,
    ups_ref,
    downs_ref,
    outs_ref,
    bups_ref,
    peers_ref,
    blocks,
    peer_w,
    peer_b,
    proj_out,
    proj_in,
    vt_ref,
    owned,
    ssz,
    rsz,
    ssx,
    rsx,
    spw,
    rpw,
    spb,
    rpb,
    ssa,
    rsa,
    wsz,
    wrz,
    wsx,
    wrx,
    gs,
    gr,
    os,
    orr,
    bs,
    br,
    local_sem,
):
    chain, cols = mp_parts(n)
    share, _ = tokens_ref.shape
    width = w_ref.shape[2]
    heads = width // HEAD_DIM
    hidden = up_ref.shape[1]
    up_rows, down_rows, out_rows = (r.shape[0] // PARTS for r in (up_ref, down_ref, out_ref))
    dg, dp = lax.axis_index("dg"), lax.axis_index("dp")
    a, b = lax.axis_index("mz"), lax.axis_index("mx")
    me = a * cols + b
    part = lax.rem(dp, PARTS)
    core_dp = dp + 1 - 2 * lax.rem(dp, 2)
    side_dp = dp + 2 - 4 * lax.rem(dp // 2, 2)
    core_part, side_part = lax.rem(core_dp, PARTS), lax.rem(side_dp, PARTS)
    far_part = PARTS - 1 - part

    barrier = pltpu.get_barrier_semaphore()
    for off in range(1, n):
        other = lax.rem(me + off, n)
        pl.semaphore_signal(
            barrier,
            inc=1,
            device_id=(dg, dp, other // cols, lax.rem(other, cols)),
            device_id_type=MESH,
        )
    for peer in (core_dp, side_dp):
        pl.semaphore_signal(barrier, inc=1, device_id=(dg, peer, a, b), device_id_type=MESH)
    pl.semaphore_wait(barrier, n + 1)

    def remote(src, dst, send, recv, device):
        return pltpu.make_async_remote_copy(
            src_ref=src,
            dst_ref=dst,
            send_sem=send,
            recv_sem=recv,
            device_id=(dg,) + device,
            device_id_type=MESH,
        )

    def span(index, size):
        return pl.ds(pl.multiple_of(index * size, size), size)

    def can(way):
        return (a < chain - 1) if way == 0 else (a > 0)

    def chain_peer(way):
        return (dp, jnp.clip(a + (1 if way == 0 else -1), 0, chain - 1), b)

    def cross_peer(off):
        return (dp, a, lax.rem(b + off, cols))

    def back_peer(off):
        return (dp, a, lax.rem(b - off + cols, cols))

    def chain_copy(row, way):
        spot = blocks.at[row]
        return remote(spot, spot, ssz.at[way, row], rsz.at[way, row], chain_peer(way))

    def cross_copy(row, off):
        return remote(
            proj_out.at[off - 1, row],
            proj_in.at[off - 1, row],
            ssx.at[off, row],
            rsx.at[off, row],
            back_peer(off),
        )

    def peer_copies(off):
        return [
            remote(w_ref, peer_w.at[off - 1], spw.at[off], rpw.at[off], cross_peer(off)),
            remote(bias_ref, peer_b.at[off - 1], spb.at[off], rpb.at[off], cross_peer(off)),
        ]

    def piece(i, row, of_part):
        if i == 0:
            return outs_ref.at[row * cols + b, span(of_part, out_rows)]
        if i == 1:
            return ups_ref.at[span(of_part, up_rows), span(row, hidden)]
        return downs_ref.at[span(row * PARTS + of_part, down_rows)]

    def own_piece(i):
        if i == 0:
            return out_ref.at[span(part, out_rows)]
        if i == 1:
            return up_ref.at[span(part, up_rows)]
        return down_ref.at[span(part, down_rows)]

    def weight_copy(i, row, way, own=False):
        spot = piece(i, row, part)
        sems = wsz.at[i, way, row], wrz.at[i, way, row]
        return remote(own_piece(i) if own else spot, spot, *sems, chain_peer(way))

    def out_cross(block, off, own=False):
        spot = outs_ref.at[block, span(part, out_rows)]
        sems = wsx.at[off, block // cols], wrx.at[off, block // cols]
        return remote(own_piece(0) if own else spot, spot, *sems, cross_peer(off))

    def group_copy(kind, i, row, arriving=False):
        sent = side_part if kind == 2 else part
        got = (side_part, core_part, far_part)[kind]
        spot = piece(i, row, got if arriving else sent)
        sems = gs.at[kind, i - 1, row], gr.at[kind, i - 1, row]
        return remote(spot, spot, *sems, (side_dp if kind == 0 else core_dp, a, b))

    def out_group(kind, arriving=False):
        sent = side_part if kind == 2 else part
        got = (side_part, core_part, far_part)[kind]
        spot = outs_ref.at[:, span(got if arriving else sent, out_rows)]
        return remote(spot, spot, os.at[kind], orr.at[kind], (side_dp if kind == 0 else core_dp, a, b))

    def bias_copy(off, arriving=False):
        spot = bups_ref.at[lax.rem(a - off + chain, chain) if arriving else a]
        return remote(bup_ref, spot, bs.at[off], br.at[off], (dp, lax.rem(a + off, chain), b))

    def start_own(way):
        for i in range(3):
            weight_copy(i, a, way, own=True).start()

    stay = [
        pltpu.make_async_copy(up_ref, ups_ref.at[:, span(a, hidden)], local_sem.at[1]),
        pltpu.make_async_copy(down_ref, downs_ref.at[span(a, hidden)], local_sem.at[2]),
        pltpu.make_async_copy(own_piece(0), piece(0, a, part), local_sem.at[3]),
        pltpu.make_async_copy(bup_ref, bups_ref.at[a], local_sem.at[4]),
    ]

    for off in range(1, cols):
        for copy in peer_copies(off):
            copy.start()
    normed = layer_norm(tokens_ref[...].astype(F32), gain_ref[...], shift_ref[...])
    blocks[a] = normed.astype(BF)

    def place(block, out_q, out_k, out_v):
        rows = span(block, share)
        lane = lax.broadcasted_iota(jnp.int32, (share, LANES - HEAD_DIM), 1)
        tail_v = jnp.where(lane < 3, 1.0, 0.0).astype(BF)
        for h in range(heads):
            cut = slice(h * HEAD_DIM, (h + 1) * HEAD_DIM)
            q_ref[h, rows, :] = jnp.concatenate(
                [out_q[:, cut] * jnp.asarray(SCALE, BF), tq_ref[rows, :]], axis=1
            )
            k_ref[h, rows, :] = jnp.concatenate([out_k[:, cut], tk_ref[rows, :]], axis=1)
            v_ref[h, rows, :] = jnp.concatenate([out_v[:, cut], tail_v], axis=1)

    def project(row):
        values = blocks[row]
        place(
            row * cols + b,
            (dot(values, w_ref[0]) + bias_ref[0, :1]).astype(BF),
            dot(values, w_ref[1]).astype(BF),
            (dot(values, w_ref[2]) + bias_ref[1, :1]).astype(BF),
        )

    def project_peer(row):
        def one(slot, _):
            values = blocks[row]
            proj_out[slot, row, 0] = (dot(values, peer_w[slot, 0]) + peer_b[slot, 0, :1]).astype(BF)
            proj_out[slot, row, 1] = dot(values, peer_w[slot, 1]).astype(BF)
            proj_out[slot, row, 2] = (dot(values, peer_w[slot, 2]) + peer_b[slot, 1, :1]).astype(BF)
            return 0

        lax.fori_loop(0, cols - 1, one, 0)
        for off in range(1, cols):
            cross_copy(row, off).start()

    for way in (0, 1):

        @pl.when(can(way))
        def _(way=way):
            chain_copy(a, way).start()

    for copy in stay:
        copy.start()

    @pl.when(a == 0)
    def _():
        start_own(0)

    @pl.when(a == chain - 1)
    def _():
        start_own(1)

    project(a)

    def visit(step, _):
        for way in (0, 1):
            there = a - step if way == 0 else a + step
            inside = (there >= 0) & (there < chain)
            row = jnp.clip(there, 0, chain - 1)

            @pl.when(inside)
            def _(way=way, row=row):
                chain_copy(row, way).wait_recv()

                @pl.when(can(way))
                def _():
                    chain_copy(row, way).start()

        @pl.when((step == a) & can(0))
        def _():
            start_own(0)

        @pl.when((step == chain - 1 - a) & can(1))
        def _():
            start_own(1)

        @pl.when(step == 1)
        def _():
            for off in range(1, cols):
                for copy in peer_copies(off):
                    copy.wait_recv()

        def one(j, _):
            gone = step - jnp.where(j == 0, 1, 0)
            there = jnp.where(j == 1, a - gone, a + gone)

            @pl.when((there >= 0) & (there < chain) & ((j > 0) | (step == 1)))
            def _():
                @pl.when(j > 0)
                def _():
                    project(there)

                project_peer(there)

            return 0

        lax.fori_loop(0, 3, one, 0)
        return 0

    lax.fori_loop(1, chain, visit, 0)

    def receive(i, _):
        row = lax.rem(a + i, chain)
        for off in range(1, cols):
            cross_copy(row, off).wait_recv()
            block = row * cols + lax.rem(b + off, cols)
            place(block, *[proj_in[off - 1, row, t] for t in range(3)])
        return 0

    lax.fori_loop(0, chain, receive, 0)
    keep = pltpu.make_async_copy(blocks, normed_ref, local_sem.at[0])
    keep.start()
    keep_peers = pltpu.make_async_copy(peer_w, peers_ref, local_sem.at[5])
    keep_peers.start()
    for off in range(1, cols):
        out_cross(me, off, own=True).start()
    for off in range(1, chain):
        bias_copy(off).start()

    def both_ways(step, act):
        for way in (0, 1):
            there = a - step if way == 0 else a + step

            @pl.when((there >= 0) & (there < chain))
            def _(way=way, there=there):
                act(way, jnp.clip(there, 0, chain - 1))

    def weights_pass(way, row):
        for i in range(3):
            weight_copy(i, row, way).wait_recv()

            @pl.when(can(way))
            def _(i=i):
                weight_copy(i, row, way).start()

            if i == 0:
                for off in range(1, cols):
                    out_cross(row * cols + b, off).start()
            else:
                group_copy(0, i, row).start()
                group_copy(1, i, row).start()

    def weights_side(way, row):
        for i in (1, 2):
            group_copy(0, i, row, arriving=True).wait_recv()
            group_copy(2, i, row).start()

    both_ways(1, weights_pass)

    def flip(c, _):
        rows = span(c, CHUNK)
        for h in range(heads):
            vt_ref[h, :, rows] = v_ref[h, rows, :].astype(F32).T.astype(BF)
        return 0

    lax.fori_loop(0, n * share // CHUNK, flip, 0)

    def own_copy(target, source):
        return remote(
            att_ref.at[span(target, share)],
            owned.at[source],
            ssa.at[target],
            rsa.at[source],
            (dp, target // cols, lax.rem(target, cols)),
        )

    def attend(c, _):
        attend_chunk(c, heads, q_ref, k_ref, v_ref, vt_ref, self_ref, att_ref, lse_ref)

        def send(target, _):
            end = (target + 1) * share

            @pl.when((end <= (c + 1) * CHUNK) & (end > c * CHUNK) & (target != me))
            def _():
                own_copy(target, me).start()

            return 0

        lax.fori_loop(0, n, send, 0)

        @pl.when(c > 0)
        def _():
            both_ways(c + 1, weights_pass)
            both_ways(c, weights_side)

        return 0

    lax.fori_loop(0, n * share // CHUNK, attend, 0)
    owned[me] = att_ref[span(me, share), :]

    def gather_out(row, _):
        for off in range(1, cols):
            out_cross(row * cols + lax.rem(b - off + cols, cols), off).wait_recv()
        return 0

    lax.fori_loop(0, chain, gather_out, 0)
    stay[2].wait()
    out_group(0).start()
    out_group(1).start()
    both_ways(chain - 1, weights_side)
    out_group(0, arriving=True).wait_recv()
    out_group(2).start()

    def collect(other, _):
        @pl.when(other != me)
        def _():
            own_copy(other, me).wait_send()
            own_copy(me, other).wait_recv()

        return 0

    lax.fori_loop(0, n, collect, 0)
    owned_ref[...] = owned[...]
    keep.wait()
    keep_peers.wait()
    for off in range(1, cols):
        for copy in peer_copies(off):
            copy.wait_send()
    for i in (0, 1, 3):
        stay[i].wait()
    for off in range(1, chain):
        bias_copy(off).wait_send()
        bias_copy(off, arriving=True).wait_recv()
    for kind in range(3):
        out_group(kind).wait_send()
        if kind > 0:
            out_group(kind, arriving=True).wait_recv()

    def drain(row, _):
        for off in range(1, cols):
            cross_copy(row, off).wait_send()
            out_cross(row * cols + b, off).wait_send()

        @pl.when((row <= a) & (a < chain - 1))
        def _():
            chain_copy(row, 0).wait_send()
            for i in range(3):
                weight_copy(i, row, 0).wait_send()

        @pl.when((row >= a) & (a > 0))
        def _():
            chain_copy(row, 1).wait_send()
            for i in range(3):
                weight_copy(i, row, 1).wait_send()

        @pl.when(row != a)
        def _():
            for i in (1, 2):
                for kind in range(3):
                    group_copy(kind, i, row).wait_send()
                    if kind > 0:
                        group_copy(kind, i, row, arriving=True).wait_recv()

        return 0

    lax.fori_loop(0, chain, drain, 0)


def front(n, tokens, gain, shift, w_qkv, bias_query, bias_value, tail_q, tail_k, self_bias, w_up, w_down, w_out, bias_up):
    chain, cols = mp_parts(n)
    share, model = tokens.shape
    width = w_qkv.shape[2]
    heads = width // HEAD_DIM
    hidden = w_up.shape[1]
    rows = n * share
    vmem = pl.BlockSpec(memory_space=pltpu.VMEM)
    anywhere = pl.BlockSpec(memory_space=pl.ANY)
    ext = jax.ShapeDtypeStruct((heads, rows, LANES), BF)
    dma = pltpu.SemaphoreType.DMA
    return pl.pallas_call(
        functools.partial(front_kernel, n),
        name="front",
        out_shape=(
            jax.ShapeDtypeStruct((chain, share, model), BF),
            ext,
            ext,
            ext,
            jax.ShapeDtypeStruct((heads, 8, rows), F32),
            jax.ShapeDtypeStruct((rows, width), BF),
            jax.ShapeDtypeStruct((n, share, width), BF),
            jax.ShapeDtypeStruct((model, chain * hidden), BF),
            jax.ShapeDtypeStruct((chain * hidden, model), BF),
            jax.ShapeDtypeStruct((n, width, model), BF),
            jax.ShapeDtypeStruct((chain, 8, hidden), F32),
            jax.ShapeDtypeStruct((cols - 1,) + w_qkv.shape, BF),
        ),
        in_specs=[vmem] * 12,
        out_specs=(anywhere,) + (vmem,) * 6 + (anywhere,) * 5,
        scratch_shapes=[
            pltpu.VMEM((chain, share, model), BF),
            pltpu.VMEM((cols - 1,) + w_qkv.shape, BF),
            pltpu.VMEM((cols - 1, 2, 8, width), F32),
            pltpu.VMEM((cols - 1, chain, 3, share, width), BF),
            pltpu.VMEM((cols - 1, chain, 3, share, width), BF),
            pltpu.VMEM((heads, LANES, rows), BF),
            pltpu.VMEM((n, share, width), BF),
            dma((2, chain)),
            dma((2, chain)),
            dma((cols, chain)),
            dma((cols, chain)),
            dma((cols,)),
            dma((cols,)),
            dma((cols,)),
            dma((cols,)),
            dma((n,)),
            dma((n,)),
            dma((3, 2, chain)),
            dma((3, 2, chain)),
            dma((cols, chain)),
            dma((cols, chain)),
            dma((3, 2, chain)),
            dma((3, 2, chain)),
            dma((3,)),
            dma((3,)),
            dma((chain,)),
            dma((chain,)),
            dma((6,)),
        ],
        compiler_params=pltpu.CompilerParams(
            collective_id=0, has_side_effects=True, vmem_limit_bytes=VMEM_BYTES
        ),
    )(
        tokens,
        gain[None, :],
        shift[None, :],
        w_qkv,
        jnp.broadcast_to(jnp.stack([bias_query, bias_value])[:, None, :], (2, 8, width)),
        tail_q,
        tail_k,
        self_bias,
        w_up,
        w_down,
        w_out,
        jnp.broadcast_to(bias_up[None, :], (8, hidden)),
    )


def attend_back_chunk(
    c, heads, q_ref, k_ref, v_ref, kt_ref, lse_ref, self_ref, att_ref, grad_ref, gq_ref, dk_ref, dv_ref
):
    rows = pl.ds(pl.multiple_of(c * CHUNK, CHUNK), CHUNK)
    grads = grad_ref[rows, :].astype(F32)
    products = grads * att_ref[rows, :].astype(F32)
    outs = []
    for h in range(heads):
        cut = slice(h * HEAD_DIM, (h + 1) * HEAD_DIM)
        inner = jnp.sum(products[:, cut], axis=1, keepdims=True)
        parts = split_three(-inner)
        lane = lax.broadcasted_iota(jnp.int32, (CHUNK, LANES - HEAD_DIM), 1)
        tail = jnp.zeros((CHUNK, LANES - HEAD_DIM), F32)
        for i, part in enumerate(parts):
            tail = jnp.where(lane == i, part.astype(F32), tail)
        grad_ext = jnp.concatenate([grads[:, cut], tail], axis=1).astype(BF)
        query = q_ref[h, rows, :]
        key_own = k_ref[h, rows, :]
        scores = dot(k_ref[h], query, NT)
        lse = lse_ref[h, :1, rows]
        probs = jnp.exp(scores - lse)
        shifted = dot(v_ref[h], grad_ext, NT)
        own = column_sum(query[:, :HEAD_DIM].astype(F32) * key_own[:, :HEAD_DIM].astype(F32))
        own_prob = jnp.exp(own + self_ref[:, rows] - lse)
        own_shifted = column_sum(v_ref[h, rows, :].astype(F32) * grad_ext.astype(F32))
        lower = lax.broadcasted_iota(jnp.int32, (8, CHUNK), 0) < 4
        both = jnp.where(lower, own_prob, own_prob * own_shifted).T
        own_prob, own_score = both[:, :1], both[:, 4:5]
        grad_scores = (probs * shifted).astype(BF)
        dv = dot(probs.astype(BF), grad_ext)
        dk = dot(grad_scores, query)
        dq = dot(kt_ref[h], grad_scores).T
        dq = (dq + own_score * key_own.astype(F32)) * SCALE
        outs.append(dq[:, :HEAD_DIM])

        @pl.when(c == 0)
        def _(h=h, dv=dv, dk=dk):
            dv_ref[h] = dv
            dk_ref[h] = dk

        @pl.when(c > 0)
        def _(h=h, dv=dv, dk=dk):
            dv_ref[h] += dv
            dk_ref[h] += dk

        dv_ref[h, rows, :] += own_prob * grad_ext.astype(F32)
        dk_ref[h, rows, :] += own_score * query.astype(F32)
    stacked = jnp.concatenate(outs, axis=1) if heads > 1 else outs[0]
    gq_ref[rows, :] = stacked.astype(BF)


REAR_REFS = (
    "gatt",
    "q",
    "k",
    "v",
    "lse",
    "self_bias",
    "att",
    "w",
    "peer_w",
    "normed",
    "tokens",
    "grad_hidden",
    "gain",
    "early",
    "up",
    "down",
    "out",
    "up_sum",
    "head_sum",
    "bias_out",
    "input_grad",
    "small_out",
    "grad",
    "kt",
    "dk",
    "dv",
    "gq",
    "gk",
    "gv",
    "kept",
    "pool_core",
    "pool_side",
    "way_in",
    "done",
    "out_in",
    "local",
    "local_in",
    "local_side",
    "local_done",
    "acc",
    "peer_in",
    "peer_acc",
    "peer_got",
    "way_gn",
    "gn",
    "small",
    "small_in",
    "bias_sum",
    "bias_in",
    "sa",
    "ra",
    "so",
    "ro",
    "sc",
    "rc",
    "sk",
    "ss",
    "rs",
    "sz",
    "rz",
    "sg",
    "rg",
    "st",
    "rt",
    "sy",
    "ry",
    "sh",
    "rh",
    "sx",
    "rx",
    "sw",
    "rw",
    "sn",
    "rn",
    "sm",
    "rm",
    "sb",
    "rb",
    "sl",
)


def rear_kernel(n, *refs):
    r = types.SimpleNamespace(**dict(zip(REAR_REFS, refs)))
    chain, cols = mp_parts(n)
    heads, total, _ = r.q.shape
    _, share, width = r.gatt.shape
    model = r.w.shape[1]
    hidden = r.up.shape[0] // chain
    rows = hidden // PARTS
    dg, dp = lax.axis_index("dg"), lax.axis_index("dp")
    a, b = lax.axis_index("mz"), lax.axis_index("mx")
    me = a * cols + b
    part = lax.rem(dp, PARTS)
    core_dp = dp + 1 - 2 * lax.rem(dp, 2)
    side_dp = dp + 2 - 4 * lax.rem(dp // 2, 2)
    core_part, side_part = lax.rem(core_dp, PARTS), lax.rem(side_dp, PARTS)
    far_part = PARTS - 1 - part
    core_id, side_id = (core_dp, a, b), (side_dp, a, b)

    def mp_id(index):
        return dp, index // cols, lax.rem(index, cols)

    barrier = pltpu.get_barrier_semaphore()
    for off in range(1, n):
        pl.semaphore_signal(
            barrier, inc=1, device_id=(dg,) + mp_id(lax.rem(me + off, n)), device_id_type=MESH
        )
    for peer in (core_id, side_id):
        pl.semaphore_signal(barrier, inc=1, device_id=(dg,) + peer, device_id_type=MESH)
    pl.semaphore_wait(barrier, n + 1)

    def remote(src, dst, send, recv, device):
        return pltpu.make_async_remote_copy(
            src_ref=src,
            dst_ref=dst,
            send_sem=send,
            recv_sem=recv,
            device_id=(dg,) + device,
            device_id_type=MESH,
        )

    def span(index, size):
        return pl.ds(pl.multiple_of(index * size, size), size)

    def in_order(i):
        near = jnp.where(2 * a < chain, 1, 0)
        return jnp.where(lax.rem(i, 2) == near, i // 2, chain - 1 - i // 2)

    def first_service(t):
        return chain - 1 - jnp.maximum(t, chain - 1 - t)

    def add_rows(dst, *terms):
        count = dst.shape[0]
        step = 32 if count % 32 == 0 else 16

        def one(i, _):
            cut = span(i, step)
            value = terms[0][cut, :].astype(F32)
            for term in terms[1:]:
                value = value + term[cut, :].astype(F32)
            dst[cut, :] = value.astype(dst.dtype)
            return 0

        lax.fori_loop(0, count // step, one, 0)

    def loop(count, act):
        def one(i, _):
            act(i)
            return 0

        lax.fori_loop(0, count, one, 0)

    def others(act):
        def one(m):
            @pl.when(m != me)
            def _():
                act(m)

        loop(n, one)

    def row_copy(target, source):
        return remote(
            r.gatt.at[target], r.grad.at[span(source, share)], r.sa.at[target], r.ra.at[source], mp_id(target)
        )

    def out_copy(target, source):
        return remote(r.out.at[target], r.out_in.at[source], r.so.at[target], r.ro.at[source], mp_id(target))

    def source_rows(i, t, which):
        return (r.up, r.down)[i].at[span(t * PARTS + which, rows)]

    def core_copy(t, slot, i):
        return remote(
            source_rows(i, t, far_part if slot else core_part),
            r.pool_core.at[span((t * 2 + slot) * 2 + i, rows)],
            r.sc.at[t, slot, i],
            r.rc.at[t, slot, i],
            core_id,
        )

    def keep_copy(t, slot, i):
        return pltpu.make_async_copy(
            source_rows(i, t, side_part if slot else part),
            r.kept.at[t, slot, pl.ds(i * rows, rows)],
            r.sk.at[t, slot, i],
        )

    def side_copy(t):
        return remote(r.kept.at[t, 1], r.pool_side.at[span(t, 2 * rows)], r.ss.at[t], r.rs.at[t], side_id)

    def chain_id(way):
        return dp, jnp.clip(a + (1 if way == 0 else -1), 0, chain - 1), b

    def hop_of(way):
        return a if way == 0 else chain - 1 - a

    def ahead(way, t):
        return (t > a) if way == 0 else (t < a)

    def chain_copy(flow, way, t, fresh=False):
        own, inbox, send, recv = flow
        spot = inbox.at[way, t]
        return remote(own(t) if fresh else spot, spot, send.at[way, t], recv.at[way, t], chain_id(way))

    def chain_service(flow, s, prepare):
        own, inbox = flow[:2]

        def one(i):
            t = in_order(i)

            @pl.when(s == first_service(t))
            def _():
                prepare(t)

            for way in (0, 1):
                hop = hop_of(way)
                active = ahead(way, t) & (s == first_service(t) + hop)

                @pl.when(active & (hop == 0))
                def _(way=way):
                    chain_copy(flow, way, t, fresh=True).start()

                @pl.when(active & (hop > 0))
                def _(way=way):
                    chain_copy(flow, way, t).wait_recv()
                    add_rows(inbox.at[way, t], inbox.at[way, t], own(t))
                    chain_copy(flow, way, t).start()

        loop(chain, one)

    def chain_finish(flow, dst):
        own, inbox = flow[:2]

        @pl.when(a > 0)
        def _():
            chain_copy(flow, 0, a).wait_recv()

        @pl.when(a < chain - 1)
        def _():
            chain_copy(flow, 1, a).wait_recv()

        @pl.when((a > 0) & (a < chain - 1))
        def _():
            add_rows(dst, own(a), inbox.at[0, a], inbox.at[1, a])

        @pl.when(a == 0)
        def _():
            add_rows(dst, own(a), inbox.at[1, a])

        @pl.when(a == chain - 1)
        def _():
            add_rows(dst, own(a), inbox.at[0, a])

    def chain_drain(flow):
        def one(t):
            for way in (0, 1):

                @pl.when(ahead(way, t))
                def _(way=way):
                    chain_copy(flow, way, t).wait_send()

        loop(chain, one)

    def share_copy(share_flow, kind, arriving=False):
        own, everyone, send, recv = share_flow
        sent = side_part if kind == 2 else part
        got = (side_part, core_part, far_part)[kind]
        spot = everyone.at[got if arriving else sent]
        src = spot if kind == 2 or arriving else own
        return remote(src, spot, send.at[kind], recv.at[kind], side_id if kind == 0 else core_id)

    weights = (lambda t: r.kept.at[t, 0], r.way_in, r.sz, r.rz)
    grads = (lambda t: r.pool_side.at[span(t, share)], r.way_gn, r.sn, r.rn)
    share_weights = (r.done, r.up_sum, r.sg, r.rg)
    share_local = (r.local_done, r.head_sum, r.sh, r.rh)

    def small_peers(stage):
        if stage == 0:
            return [core_id]
        if stage == 1:
            return [side_id]
        if stage == 2:
            return [(dp, a, lax.rem(b + off, cols)) for off in range(1, cols)]
        return [(dp, lax.rem(a + off, chain), b) for off in range(1, chain)]

    def small_copies(which, stage):
        src = r.early if which == 0 and stage == 0 else r.small.at[which, stage]
        return [
            remote(src, r.small_in.at[which, stage, i], r.sm.at[which, stage, i], r.rm.at[which, stage, i], peer)
            for i, peer in enumerate(small_peers(stage))
        ]

    def small_start(which, stage):
        for copy in small_copies(which, stage):
            copy.start()

    def small_sum(which, stage):
        value = r.early[...] if which == 0 and stage == 0 else r.small[which, stage]
        for i, copy in enumerate(small_copies(which, stage)):
            copy.wait_recv()
            value = value + r.small_in[which, stage, i]
        if stage < 3:
            r.small[which, stage + 1] = value
            small_start(which, stage + 1)
        else:
            r.small_out[which] = value

    def bias_copy(stage):
        return remote(
            r.bias_sum.at[stage], r.bias_in.at[stage], r.sb.at[stage], r.rb.at[stage], (core_id, side_id)[stage]
        )

    others(lambda m: row_copy(m, me).start())
    small_start(0, 0)

    def start_core(i):
        t = in_order(i)
        for slot in (1, 0):
            for k in (0, 1):
                core_copy(t, slot, k).start()
                keep_copy(t, slot, k).start()

    loop(chain, start_core)
    others(lambda m: out_copy(m, me).start())
    out_keep = pltpu.make_async_copy(r.out.at[me], r.out_in.at[me], r.sl.at[0])
    out_keep.start()
    r.grad[span(me, share), :] = r.gatt[me]

    def flip(c):
        cut = span(c, CHUNK)
        for h in range(heads):
            r.kt[h, :, cut] = r.k[h, cut, :].astype(F32).T.astype(BF)

    loop(total // CHUNK, flip)

    def core_sum(i):
        t = in_order(i)
        for slot in (1, 0):
            for k in (0, 1):
                keep_copy(t, slot, k).wait()
                core_copy(t, slot, k).wait_recv()
            add_rows(r.kept.at[t, slot], r.kept.at[t, slot], r.pool_core.at[span(t * 2 + slot, 2 * rows)])
            if slot == 1:
                side_copy(t).start()

    loop(chain, core_sum)
    small_sum(0, 0)
    others(lambda m: row_copy(me, m).wait_recv())

    def side_sum(t):
        side_copy(t).wait_recv()
        add_rows(r.kept.at[t, 0], r.kept.at[t, 0], r.pool_side.at[span(t, 2 * rows)])

    def cross_copy(k, lag, t):
        return remote(
            (r.gq, r.gk, r.gv)[k].at[span(t * cols + lax.rem(b + lag, cols), share)],
            r.peer_in.at[lag - 1, k, t],
            r.sx.at[k, lag, t],
            r.rx.at[k, lag, t],
            (dp, a, lax.rem(b + lag, cols)),
        )

    def attend(c):
        attend_back_chunk(
            c, heads, r.q, r.k, r.v, r.kt, r.lse, r.self_bias, r.att, r.grad, r.gq, r.dk, r.dv
        )

        def send(t):
            for lag in range(1, cols):
                end = (t * cols + lax.rem(b + lag, cols) + 1) * share

                @pl.when((end <= (c + 1) * CHUNK) & (end > c * CHUNK))
                def _(lag=lag):
                    cross_copy(0, lag, t).start()

        loop(chain, send)
        chain_service(weights, c, side_sum)

    loop(total // CHUNK, attend)

    def finish(c):
        cut = span(c, CHUNK)
        for src, dst in ((r.dk, r.gk), (r.dv, r.gv)):
            parts = [src[h, cut, :HEAD_DIM] for h in range(heads)]
            dst[cut, :] = (jnp.concatenate(parts, axis=1) if heads > 1 else parts[0]).astype(BF)

    loop(total // CHUNK, finish)

    def send_rest(i):
        for k in (1, 2):
            for lag in range(1, cols):
                cross_copy(k, lag, in_order(i)).start()

    loop(chain, send_rest)

    small_sum(0, 1)

    def partial_rows(t):
        cut = span(t * cols + b, share)
        value = dot(r.gq[cut, :], r.w[0], NT) + dot(r.gk[cut, :], r.w[1], NT)
        value = value + dot(r.gv[cut, :], r.w[2], NT)
        for slot in range(cols - 1):
            for k in range(3):
                value = value + dot(r.peer_in[slot, k, t], r.peer_w[slot, k], NT)
        return value.astype(BF)

    def bias_rows(c):
        ones = jnp.ones((8, CHUNK), BF)
        for t, src in ((0, r.gq), (1, r.gv)):
            value = dot(ones, src[span(c, CHUNK), :])

            @pl.when(c == 0)
            def _(t=t, value=value):
                r.bias_sum[0, t] = value

            @pl.when(c > 0)
            def _(t=t, value=value):
                r.bias_sum[0, t] += value

    loop(total // CHUNK, bias_rows)
    bias_copy(0).start()

    def head_grads(rows_of):
        def one(t):
            for k in range(3):
                value = dot(rows_of(k, t), r.normed[t], TN)

                @pl.when(t == 0)
                def _(k=k, value=value):
                    r.acc[k] = value

                @pl.when(t > 0)
                def _(k=k, value=value):
                    r.acc[k] += value

        loop(chain, one)

    def head_copy(off):
        return remote(
            r.peer_acc.at[off - 1],
            r.peer_got.at[off - 1],
            r.sw.at[off],
            r.rw.at[off],
            (dp, a, lax.rem(b - off + cols, cols)),
        )

    def cross_sum(t):
        for k in range(3):
            for lag in range(1, cols):
                cross_copy(k, lag, t).wait_recv()
        own = grads[0](t)
        own[...] = partial_rows(t)

    chain_service(grads, 0, cross_sum)
    chain_finish(weights, r.done)
    for kind in (0, 1):
        share_copy(share_weights, kind).start()
    weights_keep = pltpu.make_async_copy(r.done, r.up_sum.at[part], r.sl.at[1])
    weights_keep.start()
    chain_service(grads, 1, cross_sum)
    for off in range(1, cols):
        head_grads(lambda k, t: r.peer_in[off - 1, k, t])
        r.peer_acc[off - 1] = r.acc[...].astype(BF)
        head_copy(off).start()
    head_grads(lambda k, t: (r.gq, r.gk, r.gv)[k][span(t * cols + b, share), :])
    out_keep.wait()
    others(lambda m: out_copy(me, m).wait_recv())
    add_rows(r.local.at[0], *[r.out_in.at[m] for m in range(n)])

    for k in range(3):
        total_k = r.acc[k]
        for off in range(1, cols):
            if k == 0:
                head_copy(off).wait_recv()
            total_k = total_k + r.peer_got[off - 1, k].astype(F32)
        r.local[1 + k] = total_k.astype(BF)

    def local_core(slot):
        return remote(
            r.local.at[far_part if slot else core_part], r.local_in.at[slot], r.st.at[slot], r.rt.at[slot], core_id
        )

    local_side = remote(r.local.at[side_part], r.local_side, r.sy.at[0], r.ry.at[0], side_id)
    for slot in (1, 0):
        local_core(slot).start()
    small_sum(0, 2)
    for slot in (1, 0):
        local_core(slot).wait_recv()
        spot = r.local.at[side_part if slot else part]
        add_rows(spot, spot, r.local_in.at[slot])
        if slot == 1:
            local_side.start()
    bias_copy(0).wait_recv()
    r.bias_sum[1] = r.bias_sum[0] + r.bias_in[0]
    bias_copy(1).start()
    share_copy(share_weights, 0, arriving=True).wait_recv()
    share_copy(share_weights, 2).start()

    def later(s, _):
        chain_service(grads, s, cross_sum)
        return 0

    lax.fori_loop(2, chain - 1, later, 0)
    local_side.wait_recv()
    bias_copy(1).wait_recv()
    r.bias_out[...] = r.bias_sum[1] + r.bias_in[1]
    add_rows(r.local_done, r.local.at[part], r.local_side)
    for kind in (0, 1):
        share_copy(share_local, kind).start()
    local_keep = pltpu.make_async_copy(r.local_done, r.head_sum.at[part], r.sl.at[2])
    local_keep.start()
    share_copy(share_local, 0, arriving=True).wait_recv()
    share_copy(share_local, 2).start()
    chain_finish(grads, r.gn)
    step = 32 if share % 32 == 0 else 16

    def norm_back(i, sums):
        cut = span(i, step)
        values = r.tokens[cut, :].astype(F32)
        grad = r.gn[cut, :]
        centered = values - jnp.mean(values, axis=-1, keepdims=True)
        scale = lax.rsqrt(jnp.mean(centered * centered, axis=-1, keepdims=True) + epsilon)
        unit = centered * scale
        scaled = grad * r.gain[...]
        along = jnp.mean(scaled * unit, axis=-1, keepdims=True)
        back = (scaled - jnp.mean(scaled, axis=-1, keepdims=True) - unit * along) * scale
        r.input_grad[cut, :] = (r.grad_hidden[cut, :] + back).astype(BF)
        gains = jnp.sum(grad * unit, axis=0, keepdims=True)
        return sums[0] + gains, sums[1] + jnp.sum(grad, axis=0, keepdims=True)

    zero = jnp.zeros((1, model), F32)
    gains, shifts = lax.fori_loop(0, share // step, norm_back, (zero, zero))
    upper = lax.broadcasted_iota(jnp.int32, (8, model), 0) == 0
    r.small[1, 0] = jnp.where(upper, gains, shifts)
    small_start(1, 0)
    small_sum(0, 3)
    for stage in range(4):
        small_sum(1, stage)

    weights_keep.wait()
    local_keep.wait()
    for flow in (share_weights, share_local):
        for kind in range(3):
            share_copy(flow, kind).wait_send()
            if kind > 0:
                share_copy(flow, kind, arriving=True).wait_recv()
    for slot in (1, 0):
        local_core(slot).wait_send()
    local_side.wait_send()
    for off in range(1, cols):
        head_copy(off).wait_send()
    for stage in range(2):
        bias_copy(stage).wait_send()
    for which in range(2):
        for stage in range(4):
            for copy in small_copies(which, stage):
                copy.wait_send()
    others(lambda m: row_copy(m, me).wait_send())
    others(lambda m: out_copy(m, me).wait_send())
    chain_drain(weights)
    chain_drain(grads)

    def drain(t):
        side_copy(t).wait_send()
        for slot in (1, 0):
            for k in (0, 1):
                core_copy(t, slot, k).wait_send()
        for lag in range(1, cols):
            for k in range(3):
                cross_copy(k, lag, t).wait_send()

    loop(chain, drain)


def rear(
    n, grad_rows, q_ext, k_ext, v_ext, lse, self_bias, attended, w_qkv, peer_w, normed, tokens, grad_hidden, gain,
    early, grad_up, grad_down, grad_out,
):
    chain, cols = mp_parts(n)
    heads, total, _ = q_ext.shape
    _, share, width = grad_rows.shape
    model = w_qkv.shape[1]
    rows = 2 * (grad_up.shape[0] // chain // PARTS)
    vmem = pl.BlockSpec(memory_space=pltpu.VMEM)
    anywhere = pl.BlockSpec(memory_space=pl.ANY)
    dma = pltpu.SemaphoreType.DMA
    head = pltpu.VMEM((total, width), BF)
    most = max(chain, cols) - 1
    return pl.pallas_call(
        functools.partial(rear_kernel, n),
        name="rear",
        out_shape=(
            jax.ShapeDtypeStruct((PARTS, rows, model), BF),
            jax.ShapeDtypeStruct((PARTS, width, model), BF),
            jax.ShapeDtypeStruct((2, 8, width), F32),
            jax.ShapeDtypeStruct((share, model), BF),
            jax.ShapeDtypeStruct((2, 8, model), F32),
        ),
        in_specs=[vmem] * 14 + [anywhere] * 3,
        out_specs=(anywhere, anywhere, vmem, vmem, vmem),
        scratch_shapes=[
            head,
            pltpu.VMEM((heads, LANES, total), BF),
            pltpu.VMEM((heads, total, LANES), F32),
            pltpu.VMEM((heads, total, LANES), F32),
            head,
            head,
            head,
            pltpu.VMEM((chain, 2, rows, model), BF),
            pltpu.VMEM((chain * 2 * rows, model), BF),
            pltpu.VMEM((max(chain * rows, chain * share), model), BF),
            pltpu.VMEM((2, chain, rows, model), BF),
            pltpu.VMEM((rows, model), BF),
            pltpu.VMEM((n, width, model), BF),
            pltpu.VMEM((PARTS, width, model), BF),
            pltpu.VMEM((2, width, model), BF),
            pltpu.VMEM((width, model), BF),
            pltpu.VMEM((width, model), BF),
            pltpu.VMEM((3, width, model), F32),
            pltpu.VMEM((cols - 1, 3, chain, share, width), BF),
            pltpu.VMEM((cols - 1, 3, width, model), BF),
            pltpu.VMEM((cols - 1, 3, width, model), BF),
            pltpu.VMEM((2, chain, share, model), BF),
            pltpu.VMEM((share, model), F32),
            pltpu.VMEM((2, 4, 8, model), F32),
            pltpu.VMEM((2, 4, most, 8, model), F32),
            pltpu.VMEM((2, 2, 8, width), F32),
            pltpu.VMEM((2, 2, 8, width), F32),
            dma((n,)),
            dma((n,)),
            dma((n,)),
            dma((n,)),
            dma((chain, 2, 2)),
            dma((chain, 2, 2)),
            dma((chain, 2, 2)),
            dma((chain,)),
            dma((chain,)),
            dma((2, chain)),
            dma((2, chain)),
            dma((3,)),
            dma((3,)),
            dma((2,)),
            dma((2,)),
            dma((1,)),
            dma((1,)),
            dma((3,)),
            dma((3,)),
            dma((3, cols, chain)),
            dma((3, cols, chain)),
            dma((cols,)),
            dma((cols,)),
            dma((2, chain)),
            dma((2, chain)),
            dma((2, 4, most)),
            dma((2, 4, most)),
            dma((2,)),
            dma((2,)),
            dma((3,)),
        ],
        compiler_params=pltpu.CompilerParams(
            collective_id=1, has_side_effects=True, vmem_limit_bytes=VMEM_BYTES
        ),
    )(
        grad_rows, q_ext, k_ext, v_ext, lse, self_bias, attended, w_qkv, peer_w, normed, tokens, grad_hidden,
        gain[None, :], early, grad_up, grad_down, grad_out,
    )


def body(
    n,
    groups,
    tokens,
    image_ids,
    lengths,
    w_qkv,
    bias_query,
    bias_value,
    w_out,
    w_up,
    bias_up,
    w_down,
    out_biases,
    norm_gain,
    norm_bias,
    cotangent,
):
    share_rows = tokens.shape[0]
    total_rows = image_ids.shape[0]
    a, b = lax.axis_index("mz"), lax.axis_index("mx")
    chain, cols = mp_parts(n)
    model_index = a * cols + b
    model, hidden = w_up.shape
    width = w_out.shape[0]

    def shifted(values, off):
        return lax.ppermute(values, "mx", [(i, (i + off) % cols) for i in range(cols)])

    def pair_rows(values):
        return jnp.concatenate([values] + [shifted(values, off) for off in range(1, cols)])

    def pair_sum(partial):
        blocks = jnp.split(partial, cols)
        total = blocks[0].astype(F32)
        for off in range(1, cols):
            total = total + shifted(blocks[off].astype(BF), cols - off).astype(F32)
        return total

    valid_mask = valid_rows(image_ids, lengths[0])
    own_valid = lax.dynamic_slice_in_dim(
        valid_mask.astype(F32), model_index * share_rows, share_rows, 0
    )
    grad_out = cotangent.astype(F32) * own_valid[:, None]
    grad_mlp = pair_rows(grad_out.astype(BF))
    spare = jnp.arange(LANES - HEAD_DIM, dtype=jnp.int32)[None, :]
    is_id = image_ids[:, None] == spare
    tail_q = jnp.where(is_id & (spare < 2), 1.0, 0.0).astype(BF)
    tail_k = jnp.where(spare < 2, jnp.where(is_id & valid_mask[:, None], 0.0, MASKED), 0.0)
    tail_k = tail_k.astype(BF)
    self_bias = jnp.broadcast_to(jnp.where(valid_mask, MASKED, 0.0)[None, :], (8, total_rows))

    inputs_f = tokens.astype(F32)
    (
        gathered_one, q_ext, k_ext, v_ext, log_totals, attended, owned,
        up_all, down_all, out_all, bias_all, peer_w,
    ) = front(
        n,
        tokens,
        norm_gain[0],
        norm_bias[0],
        w_qkv,
        bias_query,
        bias_value,
        tail_q,
        tail_k,
        self_bias,
        w_up,
        w_down,
        w_out,
        bias_up,
    )
    owned = jnp.transpose(owned, (1, 0, 2)).reshape(share_rows, -1)
    out_all = out_all.reshape(model, model)
    bias_all = bias_all[:, 0].reshape(-1)
    hidden_one = (
        inputs_f
        + jnp.dot(owned, out_all, preferred_element_type=F32)
        + out_biases[0]
    )
    normed_two = layer_norm(hidden_one, norm_gain[1], norm_bias[1]).astype(BF)
    rows_two = pair_rows(normed_two)
    pre_act = jnp.dot(rows_two, up_all, preferred_element_type=F32) + bias_all
    activated = exact_gelu(pre_act).astype(BF)
    grad_act = jnp.einsum("rd,fd->rf", grad_mlp, down_all, preferred_element_type=F32)
    _, gelu_back = jax.vjp(exact_gelu, pre_act)
    grad_pre = gelu_back(grad_act)[0].astype(BF)
    grad_normed_two = pair_sum(jnp.einsum("rf,df->rd", grad_pre, up_all, preferred_element_type=F32))
    output_full = (
        hidden_one
        + pair_sum(jnp.dot(activated, down_all, preferred_element_type=F32))
        + out_biases[1]
    )
    grad_up_all = jnp.einsum("rf,rd->fd", grad_pre, rows_two, preferred_element_type=F32)
    grad_down_all = jnp.einsum("rf,rd->fd", activated, grad_mlp, preferred_element_type=F32)
    grad_bias_up = jnp.sum(grad_pre, axis=0, dtype=F32)

    _, norm_two_back = jax.vjp(layer_norm, hidden_one, norm_gain[1], norm_bias[1])
    grad_from_two, gain_two, shift_two = norm_two_back(grad_normed_two)
    grad_hidden = grad_out + grad_from_two
    grad_proj = grad_hidden.astype(BF)
    grad_w_out = jnp.einsum("re,rd->ed", owned, grad_proj, preferred_element_type=F32).astype(BF)
    grad_rows = jnp.einsum(
        "rd,ned->nre", grad_proj, out_all.reshape(n, width, model), preferred_element_type=F32
    ).astype(BF)
    bias_rows = lax.dynamic_update_slice(
        jnp.zeros((chain, cols, hidden), F32), grad_bias_up.reshape(chain, 1, hidden), (0, b, 0)
    )
    early = [gain_two, shift_two, jnp.sum(grad_hidden, axis=0), jnp.sum(grad_out, axis=0)]
    early = jnp.concatenate([jnp.stack(early), bias_rows.reshape(-1, model)])
    hidden_sum, head_sum, bias_sum, input_grad, small = rear(
        n,
        grad_rows,
        q_ext,
        k_ext,
        v_ext,
        log_totals,
        self_bias,
        attended,
        w_qkv,
        peer_w,
        gathered_one,
        tokens,
        grad_hidden,
        norm_gain[0],
        early,
        grad_up_all.astype(BF),
        grad_down_all.astype(BF),
        grad_w_out.reshape(n, width, model),
    )
    if groups > 1:
        hidden_sum, head_sum, bias_sum, small = lax.psum((hidden_sum, head_sum, bias_sum, small), "dg")
    half = hidden // PARTS
    grad_w_up = hidden_sum[:, :half].reshape(hidden, model).T.astype(F32)
    grad_w_down = hidden_sum[:, half:].reshape(hidden, model).astype(F32)
    grad_w_out = head_sum[0].astype(F32)
    grad_w_qkv = jnp.transpose(head_sum[1:], (0, 2, 1)).astype(F32)
    grad_bias_query, grad_bias_value = bias_sum[:, 0]
    grad_bias_up = lax.dynamic_slice_in_dim(
        small[0, 4:].reshape(-1), model_index * hidden, hidden, 0
    )
    return (
        output_full.astype(BF),
        input_grad,
        grad_w_qkv,
        grad_bias_query,
        grad_bias_value,
        grad_w_out,
        grad_w_up,
        grad_bias_up,
        grad_w_down,
        small[0, 2:4],
        jnp.stack([small[1, 0], small[0, 0]]),
        jnp.stack([small[1, 1], small[0, 1]]),
    )


def solution(mesh):
    n = mesh.shape["mp"]
    chain, cols = mp_parts(n)
    groups = mesh.shape["dp"] // PARTS
    dp, mp = ("dg", "dp"), ("mz", "mx")
    every = dp + mp
    split = jax.sharding.Mesh(mesh.devices.reshape(groups, PARTS, chain, cols), every)
    in_specs = (
        P(every, None),
        P(dp),
        P(dp, None),
        P(None, None, mp),
        P(mp),
        P(mp),
        P(mp, None),
        P(None, mp),
        P(mp),
        P(mp, None),
        P(),
        P(),
        P(),
        P(every, None),
    )
    out_specs = (
        P(every, None),
        P(every, None),
        P(None, None, mp),
        P(mp),
        P(mp),
        P(mp, None),
        P(None, mp),
        P(mp),
        P(mp, None),
        P(),
        P(),
        P(),
    )
    return jax.shard_map(
        functools.partial(body, n, groups),
        mesh=split,
        in_specs=in_specs,
        out_specs=out_specs,
        check_vma=False,
    )
```

```python
import functools
import types

import jax
import jax.numpy as jnp
from jax import lax
from jax.experimental import pallas as pl
from jax.experimental.pallas import tpu as pltpu
from jax.sharding import PartitionSpec as P

HEAD_DIM = 64
LANES = 128
CHUNK = 768
MASKED = -1e30
MESH = pl.DeviceIdType.MESH
VMEM_BYTES = 67_043_328
BF = jnp.bfloat16
F32 = jnp.float32
NN = (((1,), (0,)), ((), ()))
NT = (((1,), (1,)), ((), ()))
TN = (((0,), (0,)), ((), ()))
SCALE = HEAD_DIM ** (-0.5)
PARTS = 4
epsilon = 1e-06


def dot(left, right, dims=NN):
    return lax.dot_general(left, right, dims, preferred_element_type=F32)


def layer_norm(values, gain_vec, shift_vec):
    row_mean = jnp.mean(values, axis=-1, keepdims=True)
    centered = values - row_mean
    variance = jnp.mean(centered * centered, axis=-1, keepdims=True)
    return centered * lax.rsqrt(variance + epsilon) * gain_vec + shift_vec


def exact_gelu(values):
    return jax.nn.gelu(values, approximate=False)


def mp_parts(n):
    chain = min(4, n)
    return chain, n // chain


def column_sum(values):
    ones = jnp.ones((8, values.shape[1]), BF)
    high = values.astype(BF)
    low = (values - high.astype(F32)).astype(BF)
    return dot(ones, high, NT) + dot(ones, low, NT)


def split_three(column):
    high = column.astype(BF)
    rest = column - high.astype(F32)
    middle = rest.astype(BF)
    return high, middle, (rest - middle.astype(F32)).astype(BF)


def attend_chunk(c, heads, q_ref, k_ref, v_ref, vt_ref, self_ref, att_ref, lse_ref):
    rows = pl.ds(pl.multiple_of(c * CHUNK, CHUNK), CHUNK)
    pieces = []
    scores = [dot(k_ref[h], q_ref[h, rows, :], NT) for h in range(heads)]
    for h in range(heads):
        own = q_ref[h, rows, :HEAD_DIM].astype(F32) * k_ref[h, rows, :HEAD_DIM].astype(F32)
        own = column_sum(own)[:1] + self_ref[:1, rows]
        top = jnp.maximum(jnp.max(scores[h], axis=0, keepdims=True), own)
        weights = jnp.exp(scores[h] - top).astype(BF)
        own_weight = jnp.exp(own - top).astype(BF).astype(F32)
        summed = dot(vt_ref[h], weights) + vt_ref[h, :, rows].astype(F32) * own_weight
        total = summed[HEAD_DIM : HEAD_DIM + 1]
        pieces.append(summed[:HEAD_DIM] / total)
        lse_ref[h, :, rows] = jnp.broadcast_to(top + jnp.log(total), (8, CHUNK))
    stacked = jnp.concatenate(pieces, axis=0) if heads > 1 else pieces[0]
    att_ref[rows, :] = stacked.T.astype(BF)


def front_kernel(
    n,
    ids_ref,
    lengths_ref,
    tokens_ref,
    cot_ref,
    gain_ref,
    shift_ref,
    out_bias_ref,
    w_ref,
    bias_ref,
    up_ref,
    down_ref,
    out_ref,
    bup_ref,
    normed_ref,
    q_ref,
    k_ref,
    v_ref,
    lse_ref,
    att_ref,
    owned_ref,
    ups_ref,
    downs_ref,
    outs_out,
    bups_ref,
    peers_ref,
    self_ref,
    hidden_ref,
    pair_two,
    pair_cot,
    blocks,
    outs_ref,
    two,
    cot,
    peer_w,
    peer_b,
    proj_out,
    proj_in,
    vt_ref,
    owned,
    ssz,
    rsz,
    ssx,
    rsx,
    spw,
    rpw,
    spb,
    rpb,
    ssa,
    rsa,
    wsz,
    wrz,
    wsx,
    wrx,
    gs,
    gr,
    os,
    orr,
    bs,
    br,
    spp,
    rpp,
    local_sem,
):
    chain, cols = mp_parts(n)
    share, _ = tokens_ref.shape
    width = w_ref.shape[2]
    heads = width // HEAD_DIM
    hidden = up_ref.shape[1]
    up_rows, down_rows, out_rows = (r.shape[0] // PARTS for r in (up_ref, down_ref, out_ref))
    dg, dp = lax.axis_index("dg"), lax.axis_index("dp")
    a, b = lax.axis_index("mz"), lax.axis_index("mx")
    me = a * cols + b
    part = lax.rem(dp, PARTS)
    core_dp = dp + 1 - 2 * lax.rem(dp, 2)
    side_dp = dp + 2 - 4 * lax.rem(dp // 2, 2)
    core_part, side_part = lax.rem(core_dp, PARTS), lax.rem(side_dp, PARTS)
    far_part = PARTS - 1 - part

    barrier = pltpu.get_barrier_semaphore()
    for off in range(1, n):
        other = lax.rem(me + off, n)
        pl.semaphore_signal(
            barrier,
            inc=1,
            device_id=(dg, dp, other // cols, lax.rem(other, cols)),
            device_id_type=MESH,
        )
    for peer in (core_dp, side_dp):
        pl.semaphore_signal(barrier, inc=1, device_id=(dg, peer, a, b), device_id_type=MESH)
    pl.semaphore_wait(barrier, n + 1)

    def remote(src, dst, send, recv, device):
        return pltpu.make_async_remote_copy(
            src_ref=src,
            dst_ref=dst,
            send_sem=send,
            recv_sem=recv,
            device_id=(dg,) + device,
            device_id_type=MESH,
        )

    def span(index, size):
        return pl.ds(pl.multiple_of(index * size, size), size)

    def can(way):
        return (a < chain - 1) if way == 0 else (a > 0)

    def chain_peer(way):
        return (dp, jnp.clip(a + (1 if way == 0 else -1), 0, chain - 1), b)

    def cross_peer(off):
        return (dp, a, lax.rem(b + off, cols))

    def back_peer(off):
        return (dp, a, lax.rem(b - off + cols, cols))

    def chain_copy(row, way):
        spot = blocks.at[row]
        return remote(spot, spot, ssz.at[way, row], rsz.at[way, row], chain_peer(way))

    def cross_copy(row, off):
        return remote(
            proj_out.at[off - 1, row],
            proj_in.at[off - 1, row],
            ssx.at[off, row],
            rsx.at[off, row],
            back_peer(off),
        )

    def peer_copies(off):
        return [
            remote(w_ref, peer_w.at[off - 1], spw.at[off], rpw.at[off], cross_peer(off)),
            remote(bias_ref, peer_b.at[off - 1], spb.at[off], rpb.at[off], cross_peer(off)),
        ]

    def piece(i, row, of_part):
        if i == 0:
            return outs_ref.at[row * cols + b, span(of_part, out_rows)]
        if i == 1:
            return ups_ref.at[span(of_part, up_rows), span(row, hidden)]
        return downs_ref.at[span(row * PARTS + of_part, down_rows)]

    def own_piece(i):
        if i == 0:
            return out_ref.at[span(part, out_rows)]
        if i == 1:
            return up_ref.at[span(part, up_rows)]
        return down_ref.at[span(part, down_rows)]

    def weight_copy(i, row, way, own=False):
        spot = piece(i, row, part)
        sems = wsz.at[i, way, row], wrz.at[i, way, row]
        return remote(own_piece(i) if own else spot, spot, *sems, chain_peer(way))

    def out_cross(block, off, own=False):
        spot = outs_ref.at[block, span(part, out_rows)]
        sems = wsx.at[off, block // cols], wrx.at[off, block // cols]
        return remote(own_piece(0) if own else spot, spot, *sems, cross_peer(off))

    def group_copy(kind, i, row, arriving=False):
        sent = side_part if kind == 2 else part
        got = (side_part, core_part, far_part)[kind]
        spot = piece(i, row, got if arriving else sent)
        sems = gs.at[kind, i - 1, row], gr.at[kind, i - 1, row]
        return remote(spot, spot, *sems, (side_dp if kind == 0 else core_dp, a, b))

    def out_group(kind, arriving=False):
        sent = side_part if kind == 2 else part
        got = (side_part, core_part, far_part)[kind]
        spot = outs_ref.at[:, span(got if arriving else sent, out_rows)]
        return remote(spot, spot, os.at[kind], orr.at[kind], (side_dp if kind == 0 else core_dp, a, b))

    def bias_copy(off, arriving=False):
        spot = bups_ref.at[lax.rem(a - off + chain, chain) if arriving else a]
        return remote(bup_ref, spot, bs.at[off], br.at[off], (dp, lax.rem(a + off, chain), b))

    def start_own(way):
        for i in (1, 2):
            weight_copy(i, a, way, own=True).start()

    stay = [
        pltpu.make_async_copy(up_ref, ups_ref.at[:, span(a, hidden)], local_sem.at[1]),
        pltpu.make_async_copy(down_ref, downs_ref.at[span(a, hidden)], local_sem.at[2]),
        pltpu.make_async_copy(own_piece(0), piece(0, a, part), local_sem.at[3]),
        pltpu.make_async_copy(bup_ref, bups_ref.at[a], local_sem.at[4]),
    ]

    for off in range(1, cols):
        for copy in peer_copies(off):
            copy.start()
    normed = layer_norm(tokens_ref[...].astype(F32), gain_ref[:1], shift_ref[:1])
    blocks[a] = normed.astype(BF)

    total = n * share
    slot = total // 2
    first_id, last_id = ids_ref[0], ids_ref[total - 1]
    first_length, last_length = (
        jnp.where(k == 0, lengths_ref[0, 0], lengths_ref[0, 1]) for k in (first_id, last_id)
    )
    last_start = jnp.where(first_id == last_id, 0, slot)

    def row_facts(index):
        late = index >= slot
        inside = index - jnp.where(late, last_start, 0) < jnp.where(late, last_length, first_length)
        return jnp.where(late, last_id, first_id), inside

    def place(block, out_q, out_k, out_v):
        rows = span(block, share)
        lane = lax.broadcasted_iota(jnp.int32, (share, LANES - HEAD_DIM), 1)
        image, inside = row_facts(
            block * share + lax.broadcasted_iota(jnp.int32, (share, LANES - HEAD_DIM), 0)
        )
        tail_q = jnp.where(lane == image, 1.0, 0.0).astype(BF)
        hidden_key = jnp.where((lane == image) & inside, 0.0, MASKED)
        tail_k = jnp.where(lane < 2, hidden_key, 0.0).astype(BF)
        tail_v = jnp.where(lane < 3, 1.0, 0.0).astype(BF)
        for h in range(heads):
            cut = slice(h * HEAD_DIM, (h + 1) * HEAD_DIM)
            q_ref[h, rows, :] = jnp.concatenate(
                [out_q[:, cut] * jnp.asarray(SCALE, BF), tail_q], axis=1
            )
            k_ref[h, rows, :] = jnp.concatenate([out_k[:, cut], tail_k], axis=1)
            v_ref[h, rows, :] = jnp.concatenate([out_v[:, cut], tail_v], axis=1)

    def project(row):
        values = blocks[row]
        place(
            row * cols + b,
            (dot(values, w_ref[0]) + bias_ref[0, :1]).astype(BF),
            dot(values, w_ref[1]).astype(BF),
            (dot(values, w_ref[2]) + bias_ref[1, :1]).astype(BF),
        )

    def project_peer(row):
        def one(slot, _):
            values = blocks[row]
            proj_out[slot, row, 0] = (dot(values, peer_w[slot, 0]) + peer_b[slot, 0, :1]).astype(BF)
            proj_out[slot, row, 1] = dot(values, peer_w[slot, 1]).astype(BF)
            proj_out[slot, row, 2] = (dot(values, peer_w[slot, 2]) + peer_b[slot, 1, :1]).astype(BF)
            return 0

        lax.fori_loop(0, cols - 1, one, 0)
        for off in range(1, cols):
            cross_copy(row, off).start()

    for way in (0, 1):

        @pl.when(can(way))
        def _(way=way):
            chain_copy(a, way).start()
            weight_copy(0, a, way, own=True).start()

    def pair_copy(i, off):
        src, dst = ((two, pair_two), (cot, pair_cot))[i]
        return remote(src, dst.at[off], spp.at[i, off], rpp.at[i, off], cross_peer(off))

    pair_stay = [
        pltpu.make_async_copy(two, pair_two.at[0], local_sem.at[6]),
        pltpu.make_async_copy(cot, pair_cot.at[0], local_sem.at[7]),
    ]
    for copy in stay:
        copy.start()

    @pl.when(a == 0)
    def _():
        start_own(0)

    @pl.when(a == chain - 1)
    def _():
        start_own(1)

    project(a)
    _, self_inside = row_facts(lax.broadcasted_iota(jnp.int32, (8, total), 1))
    self_ref[...] = jnp.where(self_inside, MASKED, 0.0)

    def mask_cot(i, _):
        cut = span(i, 16)
        _, inside = row_facts(
            me * share + i * 16 + lax.broadcasted_iota(jnp.int32, (16, cot.shape[1]), 0)
        )
        cot[cut, :] = jnp.where(inside, cot_ref[cut, :].astype(F32), 0.0).astype(BF)
        return 0

    lax.fori_loop(0, share // 16, mask_cot, 0)

    def visit(step, _):
        for way in (0, 1):
            there = a - step if way == 0 else a + step
            inside = (there >= 0) & (there < chain)
            row = jnp.clip(there, 0, chain - 1)

            @pl.when(inside)
            def _(way=way, row=row):
                chain_copy(row, way).wait_recv()

                @pl.when(can(way))
                def _():
                    chain_copy(row, way).start()

                weight_copy(0, row, way).wait_recv()

                @pl.when(can(way))
                def _():
                    weight_copy(0, row, way).start()

        @pl.when((step == a) & can(0))
        def _():
            start_own(0)

        @pl.when((step == chain - 1 - a) & can(1))
        def _():
            start_own(1)

        @pl.when(step == 1)
        def _():
            for off in range(1, cols):
                for copy in peer_copies(off):
                    copy.wait_recv()

        def one(j, _):
            gone = step - jnp.where(j == 0, 1, 0)
            there = jnp.where(j == 1, a - gone, a + gone)

            @pl.when((there >= 0) & (there < chain) & ((j > 0) | (step == 1)))
            def _():
                @pl.when(j > 0)
                def _():
                    project(there)

                project_peer(there)

            return 0

        lax.fori_loop(0, 3, one, 0)
        return 0

    lax.fori_loop(1, chain, visit, 0)

    stay[2].wait()
    for off in range(1, cols):
        out_cross(me, off, own=True).start()

    def out_send(i, _):
        row = lax.rem(a + i, chain)
        for off in range(1, cols):
            out_cross(row * cols + b, off).start()
        return 0

    lax.fori_loop(1, chain, out_send, 0)

    def receive(i, _):
        row = lax.rem(a + i, chain)
        for off in range(1, cols):
            cross_copy(row, off).wait_recv()
            block = row * cols + lax.rem(b + off, cols)
            place(block, *[proj_in[off - 1, row, t] for t in range(3)])
        return 0

    lax.fori_loop(0, chain, receive, 0)
    keep = pltpu.make_async_copy(blocks, normed_ref, local_sem.at[0])
    keep.start()
    keep_peers = pltpu.make_async_copy(peer_w, peers_ref, local_sem.at[5])
    keep_peers.start()

    def gather_out(row, _):
        for off in range(1, cols):
            out_cross(row * cols + lax.rem(b - off + cols, cols), off).wait_recv()
        return 0

    lax.fori_loop(0, chain, gather_out, 0)
    out_group(0).start()
    out_group(1).start()
    for off in range(1, chain):
        bias_copy(off).start()

    def both_ways(step, act):
        for way in (0, 1):
            there = a - step if way == 0 else a + step

            @pl.when((there >= 0) & (there < chain))
            def _(way=way, there=there):
                act(way, jnp.clip(there, 0, chain - 1))

    def weights_pass(way, row):
        for i in (1, 2):
            weight_copy(i, row, way).wait_recv()

            @pl.when(can(way))
            def _(i=i):
                weight_copy(i, row, way).start()

            group_copy(0, i, row).start()
            group_copy(1, i, row).start()

    def weights_side(way, row):
        for i in (1, 2):
            group_copy(0, i, row, arriving=True).wait_recv()
            group_copy(2, i, row).start()

    both_ways(1, weights_pass)

    def flip(c, _):
        rows = span(c, CHUNK)
        for h in range(heads):
            vt_ref[h, :, rows] = v_ref[h, rows, :].astype(F32).T.astype(BF)
        return 0

    lax.fori_loop(0, n * share // CHUNK, flip, 0)

    def own_copy(target, source):
        return remote(
            att_ref.at[span(target, share)],
            owned.at[source],
            ssa.at[target],
            rsa.at[source],
            (dp, target // cols, lax.rem(target, cols)),
        )

    def attend(c, _):
        attend_chunk(c, heads, q_ref, k_ref, v_ref, vt_ref, self_ref, att_ref, lse_ref)

        def send(target, _):
            end = (target + 1) * share

            @pl.when((end <= (c + 1) * CHUNK) & (end > c * CHUNK) & (target != me))
            def _():
                own_copy(target, me).start()

            return 0

        lax.fori_loop(0, n, send, 0)

        @pl.when(c == 0)
        def _():
            out_group(0, arriving=True).wait_recv()
            out_group(2).start()

        @pl.when(c > 0)
        def _():
            both_ways(c + 1, weights_pass)
            both_ways(c, weights_side)

        return 0

    lax.fori_loop(0, n * share // CHUNK, attend, 0)
    owned[me] = att_ref[span(me, share), :]
    for off in range(1, cols):
        pair_copy(1, off).start()
    pair_stay[1].start()
    for kind in (1, 2):
        out_group(kind, arriving=True).wait_recv()
    keep_out = pltpu.make_async_copy(outs_ref, outs_out, local_sem.at[3])
    keep_out.start()

    def collect(other, _):
        @pl.when(other != me)
        def _():
            own_copy(other, me).wait_send()
            own_copy(me, other).wait_recv()

        return 0

    lax.fori_loop(0, n, collect, 0)
    hidden_ref[...] = tokens_ref[...].astype(F32) + out_bias_ref[:1]

    def out_project(m, _):
        hidden_ref[...] += dot(owned[m], outs_ref[m])
        return 0

    lax.fori_loop(0, n, out_project, 0)

    def norm_two(i, _):
        cut = span(i, 16)
        two[cut, :] = layer_norm(hidden_ref[cut, :], gain_ref[1:], shift_ref[1:]).astype(BF)
        return 0

    lax.fori_loop(0, share // 16, norm_two, 0)
    for off in range(1, cols):
        pair_copy(0, off).start()
    pair_stay[0].start()
    both_ways(chain - 1, weights_side)
    owned_ref[...] = owned[...]
    for off in range(1, cols):
        for i in (0, 1):
            pair_copy(i, off).wait_send()
            pair_copy(i, off).wait_recv()
    for copy in pair_stay:
        copy.wait()
    keep_out.wait()
    keep.wait()
    keep_peers.wait()
    for off in range(1, cols):
        for copy in peer_copies(off):
            copy.wait_send()
    for i in (0, 1, 3):
        stay[i].wait()
    for off in range(1, chain):
        bias_copy(off).wait_send()
        bias_copy(off, arriving=True).wait_recv()
    for kind in range(3):
        out_group(kind).wait_send()

    def drain(row, _):
        for off in range(1, cols):
            cross_copy(row, off).wait_send()
            out_cross(row * cols + b, off).wait_send()

        @pl.when((row <= a) & (a < chain - 1))
        def _():
            chain_copy(row, 0).wait_send()
            for i in range(3):
                weight_copy(i, row, 0).wait_send()

        @pl.when((row >= a) & (a > 0))
        def _():
            chain_copy(row, 1).wait_send()
            for i in range(3):
                weight_copy(i, row, 1).wait_send()

        @pl.when(row != a)
        def _():
            for i in (1, 2):
                for kind in range(3):
                    group_copy(kind, i, row).wait_send()
                    if kind > 0:
                        group_copy(kind, i, row, arriving=True).wait_recv()

        return 0

    lax.fori_loop(0, chain, drain, 0)


def front(
    n, image_ids, lengths, tokens, cotangent, gain, shift, out_biases, w_qkv, bias_query, bias_value, w_up, w_down,
    w_out, bias_up,
):
    chain, cols = mp_parts(n)
    share, model = tokens.shape
    width = w_qkv.shape[2]
    heads = width // HEAD_DIM
    hidden = w_up.shape[1]
    rows = n * share
    vmem = pl.BlockSpec(memory_space=pltpu.VMEM)
    anywhere = pl.BlockSpec(memory_space=pl.ANY)
    ext = jax.ShapeDtypeStruct((heads, rows, LANES), BF)
    dma = pltpu.SemaphoreType.DMA
    return pl.pallas_call(
        functools.partial(front_kernel, n),
        name="front",
        out_shape=(
            jax.ShapeDtypeStruct((chain, share, model), BF),
            ext,
            ext,
            ext,
            jax.ShapeDtypeStruct((heads, 8, rows), F32),
            jax.ShapeDtypeStruct((rows, width), BF),
            jax.ShapeDtypeStruct((n, share, width), BF),
            jax.ShapeDtypeStruct((model, chain * hidden), BF),
            jax.ShapeDtypeStruct((chain * hidden, model), BF),
            jax.ShapeDtypeStruct((n, width, model), BF),
            jax.ShapeDtypeStruct((chain, 8, hidden), F32),
            jax.ShapeDtypeStruct((cols - 1,) + w_qkv.shape, BF),
            jax.ShapeDtypeStruct((8, rows), F32),
            jax.ShapeDtypeStruct((share, model), F32),
            jax.ShapeDtypeStruct((cols, share, model), BF),
            jax.ShapeDtypeStruct((cols, share, model), BF),
        ),
        in_specs=[pl.BlockSpec(memory_space=pltpu.SMEM)] * 2 + [vmem] * 11,
        out_specs=(anywhere,) + (vmem,) * 6 + (anywhere,) * 5 + (vmem,) * 2 + (anywhere,) * 2,
        scratch_shapes=[
            pltpu.VMEM((chain, share, model), BF),
            pltpu.VMEM((n, width, model), BF),
            pltpu.VMEM((share, model), BF),
            pltpu.VMEM((share, model), BF),
            pltpu.VMEM((cols - 1,) + w_qkv.shape, BF),
            pltpu.VMEM((cols - 1, 2, 8, width), F32),
            pltpu.VMEM((cols - 1, chain, 3, share, width), BF),
            pltpu.VMEM((cols - 1, chain, 3, share, width), BF),
            pltpu.VMEM((heads, LANES, rows), BF),
            pltpu.VMEM((n, share, width), BF),
            dma((2, chain)),
            dma((2, chain)),
            dma((cols, chain)),
            dma((cols, chain)),
            dma((cols,)),
            dma((cols,)),
            dma((cols,)),
            dma((cols,)),
            dma((n,)),
            dma((n,)),
            dma((3, 2, chain)),
            dma((3, 2, chain)),
            dma((cols, chain)),
            dma((cols, chain)),
            dma((3, 2, chain)),
            dma((3, 2, chain)),
            dma((3,)),
            dma((3,)),
            dma((chain,)),
            dma((chain,)),
            dma((2, cols)),
            dma((2, cols)),
            dma((8,)),
        ],
        compiler_params=pltpu.CompilerParams(
            collective_id=0, has_side_effects=True, vmem_limit_bytes=VMEM_BYTES
        ),
    )(
        image_ids,
        lengths,
        tokens,
        cotangent,
        gain,
        shift,
        out_biases,
        w_qkv,
        jnp.broadcast_to(jnp.stack([bias_query, bias_value])[:, None, :], (2, 8, width)),
        w_up,
        w_down,
        w_out,
        jnp.broadcast_to(bias_up[None, :], (8, hidden)),
    )


def attend_back_chunk(
    c, heads, q_ref, k_ref, v_ref, kt_ref, lse_ref, self_ref, att_ref, grad_ref, gq_ref, dk_ref, dv_ref
):
    rows = pl.ds(pl.multiple_of(c * CHUNK, CHUNK), CHUNK)
    grads = grad_ref[rows, :].astype(F32)
    products = grads * att_ref[rows, :].astype(F32)
    outs = []
    for h in range(heads):
        cut = slice(h * HEAD_DIM, (h + 1) * HEAD_DIM)
        inner = jnp.sum(products[:, cut], axis=1, keepdims=True)
        parts = split_three(-inner)
        lane = lax.broadcasted_iota(jnp.int32, (CHUNK, LANES - HEAD_DIM), 1)
        tail = jnp.zeros((CHUNK, LANES - HEAD_DIM), F32)
        for i, part in enumerate(parts):
            tail = jnp.where(lane == i, part.astype(F32), tail)
        grad_ext = jnp.concatenate([grads[:, cut], tail], axis=1).astype(BF)
        query = q_ref[h, rows, :]
        key_own = k_ref[h, rows, :]
        scores = dot(k_ref[h], query, NT)
        lse = lse_ref[h, :1, rows]
        probs = jnp.exp(scores - lse)
        shifted = dot(v_ref[h], grad_ext, NT)
        own = column_sum(query[:, :HEAD_DIM].astype(F32) * key_own[:, :HEAD_DIM].astype(F32))
        own_prob = jnp.exp(own + self_ref[:, rows] - lse)
        own_shifted = column_sum(v_ref[h, rows, :].astype(F32) * grad_ext.astype(F32))
        lower = lax.broadcasted_iota(jnp.int32, (8, CHUNK), 0) < 4
        both = jnp.where(lower, own_prob, own_prob * own_shifted).T
        own_prob, own_score = both[:, :1], both[:, 4:5]
        grad_scores = (probs * shifted).astype(BF)
        dv = dot(probs.astype(BF), grad_ext)
        dk = dot(grad_scores, query)
        dq = dot(kt_ref[h], grad_scores).T
        dq = (dq + own_score * key_own.astype(F32)) * SCALE
        outs.append(dq[:, :HEAD_DIM])

        @pl.when(c == 0)
        def _(h=h, dv=dv, dk=dk):
            dv_ref[h] = dv
            dk_ref[h] = dk

        @pl.when(c > 0)
        def _(h=h, dv=dv, dk=dk):
            dv_ref[h] += dv
            dk_ref[h] += dk

        dv_ref[h, rows, :] += own_prob * grad_ext.astype(F32)
        dk_ref[h, rows, :] += own_score * query.astype(F32)
    stacked = jnp.concatenate(outs, axis=1) if heads > 1 else outs[0]
    gq_ref[rows, :] = stacked.astype(BF)


REAR_REFS = (
    "gatt",
    "q",
    "k",
    "v",
    "lse",
    "self_bias",
    "att",
    "w",
    "peer_w",
    "normed",
    "tokens",
    "grad_hidden",
    "gain",
    "early",
    "up",
    "down",
    "out",
    "up_sum",
    "head_sum",
    "bias_out",
    "input_grad",
    "small_out",
    "grad",
    "kt",
    "dk",
    "dv",
    "gq",
    "gk",
    "gv",
    "kept",
    "pool_core",
    "pool_side",
    "way_in",
    "done",
    "out_in",
    "local",
    "local_in",
    "local_side",
    "local_done",
    "acc",
    "peer_in",
    "peer_acc",
    "peer_got",
    "way_gn",
    "gn",
    "small",
    "small_in",
    "bias_sum",
    "bias_in",
    "sa",
    "ra",
    "so",
    "ro",
    "sc",
    "rc",
    "sk",
    "ss",
    "rs",
    "sz",
    "rz",
    "sg",
    "rg",
    "st",
    "rt",
    "sy",
    "ry",
    "sh",
    "rh",
    "sx",
    "rx",
    "sw",
    "rw",
    "sn",
    "rn",
    "sm",
    "rm",
    "sb",
    "rb",
    "sl",
)


def rear_kernel(n, *refs):
    r = types.SimpleNamespace(**dict(zip(REAR_REFS, refs)))
    chain, cols = mp_parts(n)
    heads, total, _ = r.q.shape
    _, share, width = r.gatt.shape
    model = r.w.shape[1]
    hidden = r.up.shape[0] // chain
    rows = hidden // PARTS
    dg, dp = lax.axis_index("dg"), lax.axis_index("dp")
    a, b = lax.axis_index("mz"), lax.axis_index("mx")
    me = a * cols + b
    part = lax.rem(dp, PARTS)
    core_dp = dp + 1 - 2 * lax.rem(dp, 2)
    side_dp = dp + 2 - 4 * lax.rem(dp // 2, 2)
    core_part, side_part = lax.rem(core_dp, PARTS), lax.rem(side_dp, PARTS)
    far_part = PARTS - 1 - part
    core_id, side_id = (core_dp, a, b), (side_dp, a, b)
    far_id = (PARTS - 1 - dp, a, b)

    def mp_id(index):
        return dp, index // cols, lax.rem(index, cols)

    barrier = pltpu.get_barrier_semaphore()
    for off in range(1, n):
        pl.semaphore_signal(
            barrier, inc=1, device_id=(dg,) + mp_id(lax.rem(me + off, n)), device_id_type=MESH
        )
    for peer in (core_id, side_id, far_id):
        pl.semaphore_signal(barrier, inc=1, device_id=(dg,) + peer, device_id_type=MESH)
    pl.semaphore_wait(barrier, n + 2)

    def remote(src, dst, send, recv, device):
        return pltpu.make_async_remote_copy(
            src_ref=src,
            dst_ref=dst,
            send_sem=send,
            recv_sem=recv,
            device_id=(dg,) + device,
            device_id_type=MESH,
        )

    def span(index, size):
        return pl.ds(pl.multiple_of(index * size, size), size)

    def in_order(i):
        near = jnp.where(2 * a < chain, 1, 0)
        return jnp.where(lax.rem(i, 2) == near, i // 2, chain - 1 - i // 2)

    def first_service(t):
        return chain - 1 - jnp.maximum(t, chain - 1 - t)

    def add_rows(dst, *terms):
        count = dst.shape[0]
        step = 32 if count % 32 == 0 else 16

        def one(i, _):
            cut = span(i, step)
            value = terms[0][cut, :].astype(F32)
            for term in terms[1:]:
                value = value + term[cut, :].astype(F32)
            dst[cut, :] = value.astype(dst.dtype)
            return 0

        lax.fori_loop(0, count // step, one, 0)

    def loop(count, act):
        def one(i, _):
            act(i)
            return 0

        lax.fori_loop(0, count, one, 0)

    def others(act):
        def one(m):
            @pl.when(m != me)
            def _():
                act(m)

        loop(n, one)

    def row_copy(target, source):
        return remote(
            r.gatt.at[target], r.grad.at[span(source, share)], r.sa.at[target], r.ra.at[source], mp_id(target)
        )

    def out_copy(target, source):
        return remote(r.out.at[target], r.out_in.at[source], r.so.at[target], r.ro.at[source], mp_id(target))

    def source_rows(i, t, which):
        return (r.up, r.down)[i].at[span(t * PARTS + which, rows)]

    def core_copy(t, slot, i):
        return remote(
            source_rows(i, t, far_part if slot else core_part),
            r.pool_core.at[span((t * 2 + slot) * 2 + i, rows)],
            r.sc.at[t, slot, i],
            r.rc.at[t, slot, i],
            core_id,
        )

    def keep_copy(t, slot, i):
        return pltpu.make_async_copy(
            source_rows(i, t, side_part if slot else part),
            r.kept.at[t, slot, pl.ds(i * rows, rows)],
            r.sk.at[t, slot, i],
        )

    def side_copy(t):
        return remote(r.kept.at[t, 1], r.pool_side.at[span(t, 2 * rows)], r.ss.at[t], r.rs.at[t], side_id)

    def chain_id(way):
        return dp, jnp.clip(a + (1 if way == 0 else -1), 0, chain - 1), b

    def hop_of(way):
        return a if way == 0 else chain - 1 - a

    def ahead(way, t):
        return (t > a) if way == 0 else (t < a)

    def chain_copy(flow, way, t, fresh=False):
        own, inbox, send, recv = flow
        spot = inbox.at[way, t]
        return remote(own(t) if fresh else spot, spot, send.at[way, t], recv.at[way, t], chain_id(way))

    def chain_service(flow, s, prepare):
        own, inbox = flow[:2]

        def one(i):
            t = in_order(i)

            @pl.when(s == first_service(t))
            def _():
                prepare(t)

            for way in (0, 1):
                hop = hop_of(way)
                active = ahead(way, t) & (s == first_service(t) + hop)

                @pl.when(active & (hop == 0))
                def _(way=way):
                    chain_copy(flow, way, t, fresh=True).start()

                @pl.when(active & (hop > 0))
                def _(way=way):
                    chain_copy(flow, way, t).wait_recv()
                    add_rows(inbox.at[way, t], inbox.at[way, t], own(t))
                    chain_copy(flow, way, t).start()

        loop(chain, one)

    def chain_finish(flow, dst):
        own, inbox = flow[:2]

        @pl.when(a > 0)
        def _():
            chain_copy(flow, 0, a).wait_recv()

        @pl.when(a < chain - 1)
        def _():
            chain_copy(flow, 1, a).wait_recv()

        @pl.when((a > 0) & (a < chain - 1))
        def _():
            add_rows(dst, own(a), inbox.at[0, a], inbox.at[1, a])

        @pl.when(a == 0)
        def _():
            add_rows(dst, own(a), inbox.at[1, a])

        @pl.when(a == chain - 1)
        def _():
            add_rows(dst, own(a), inbox.at[0, a])

    def chain_drain(flow):
        def one(t):
            for way in (0, 1):

                @pl.when(ahead(way, t))
                def _(way=way):
                    chain_copy(flow, way, t).wait_send()

        loop(chain, one)

    def share_copy(share_flow, kind, arriving=False):
        own, everyone, send, recv = share_flow
        sent = side_part if kind == 2 else part
        got = (side_part, core_part, far_part)[kind]
        spot = everyone.at[got if arriving else sent]
        src = spot if kind == 2 or arriving else own
        return remote(src, spot, send.at[kind], recv.at[kind], side_id if kind == 0 else core_id)

    weights = (lambda t: r.kept.at[t, 0], r.way_in, r.sz, r.rz)
    grads = (lambda t: r.pool_side.at[span(t, share)], r.way_gn, r.sn, r.rn)
    share_weights = (r.done, r.up_sum, r.sg, r.rg)
    share_local = (r.local_done, r.head_sum, r.sh, r.rh)

    def small_peers(stage):
        if stage == 0:
            return [core_id, side_id, far_id]
        if stage == 1:
            return [(dp, a, lax.rem(b + off, cols)) for off in range(1, cols)]
        return [(dp, lax.rem(a + off, chain), b) for off in range(1, chain)]

    def small_copies(which, stage):
        src = r.early if which == 0 and stage == 0 else r.small.at[which, stage]
        return [
            remote(src, r.small_in.at[which, stage, i], r.sm.at[which, stage, i], r.rm.at[which, stage, i], peer)
            for i, peer in enumerate(small_peers(stage))
        ]

    def small_start(which, stage):
        for copy in small_copies(which, stage):
            copy.start()

    def small_sum(which, stage):
        value = r.early[...] if which == 0 and stage == 0 else r.small[which, stage]
        for i, copy in enumerate(small_copies(which, stage)):
            copy.wait_recv()
            value = value + r.small_in[which, stage, i]
        if stage < 2:
            r.small[which, stage + 1] = value
            small_start(which, stage + 1)
        else:
            r.small_out[which] = value

    def bias_copy(stage):
        return remote(
            r.bias_sum.at[stage], r.bias_in.at[stage], r.sb.at[stage], r.rb.at[stage], (core_id, side_id)[stage]
        )

    others(lambda m: row_copy(m, me).start())
    small_start(0, 0)

    def start_core(i):
        t = in_order(i)
        for slot in (1, 0):
            for k in (0, 1):
                core_copy(t, slot, k).start()
                keep_copy(t, slot, k).start()

    loop(chain, start_core)
    others(lambda m: out_copy(m, me).start())
    out_keep = pltpu.make_async_copy(r.out.at[me], r.out_in.at[me], r.sl.at[0])
    out_keep.start()
    r.grad[span(me, share), :] = r.gatt[me]

    def flip(c):
        cut = span(c, CHUNK)
        for h in range(heads):
            r.kt[h, :, cut] = r.k[h, cut, :].astype(F32).T.astype(BF)

    loop(total // CHUNK, flip)

    def core_sum(i):
        t = in_order(i)
        for slot in (1, 0):
            for k in (0, 1):
                keep_copy(t, slot, k).wait()
                core_copy(t, slot, k).wait_recv()
            add_rows(r.kept.at[t, slot], r.kept.at[t, slot], r.pool_core.at[span(t * 2 + slot, 2 * rows)])
            if slot == 1:
                side_copy(t).start()

    loop(chain, core_sum)
    others(lambda m: row_copy(me, m).wait_recv())

    def side_sum(t):
        side_copy(t).wait_recv()
        add_rows(r.kept.at[t, 0], r.kept.at[t, 0], r.pool_side.at[span(t, 2 * rows)])

    def cross_copy(k, lag, t):
        return remote(
            (r.gq, r.gk, r.gv)[k].at[span(t * cols + lax.rem(b + lag, cols), share)],
            r.peer_in.at[lag - 1, k, t],
            r.sx.at[k, lag, t],
            r.rx.at[k, lag, t],
            (dp, a, lax.rem(b + lag, cols)),
        )

    def attend(c):
        attend_back_chunk(
            c, heads, r.q, r.k, r.v, r.kt, r.lse, r.self_bias, r.att, r.grad, r.gq, r.dk, r.dv
        )

        def send(t):
            for lag in range(1, cols):
                end = (t * cols + lax.rem(b + lag, cols) + 1) * share

                @pl.when((end <= (c + 1) * CHUNK) & (end > c * CHUNK))
                def _(lag=lag):
                    cross_copy(0, lag, t).start()

        loop(chain, send)
        chain_service(weights, c, side_sum)

    loop(total // CHUNK, attend)

    def finish(c):
        cut = span(c, CHUNK)
        for src, dst in ((r.dk, r.gk), (r.dv, r.gv)):
            parts = [src[h, cut, :HEAD_DIM] for h in range(heads)]
            dst[cut, :] = (jnp.concatenate(parts, axis=1) if heads > 1 else parts[0]).astype(BF)

    loop(total // CHUNK, finish)

    def send_rest(i):
        for k in (1, 2):
            for lag in range(1, cols):
                cross_copy(k, lag, in_order(i)).start()

    loop(chain, send_rest)

    small_sum(0, 0)

    def partial_rows(t):
        cut = span(t * cols + b, share)
        value = dot(r.gq[cut, :], r.w[0], NT) + dot(r.gk[cut, :], r.w[1], NT)
        value = value + dot(r.gv[cut, :], r.w[2], NT)
        for slot in range(cols - 1):
            for k in range(3):
                value = value + dot(r.peer_in[slot, k, t], r.peer_w[slot, k], NT)
        return value.astype(BF)

    def bias_rows(c):
        ones = jnp.ones((8, CHUNK), BF)
        for t, src in ((0, r.gq), (1, r.gv)):
            value = dot(ones, src[span(c, CHUNK), :])

            @pl.when(c == 0)
            def _(t=t, value=value):
                r.bias_sum[0, t] = value

            @pl.when(c > 0)
            def _(t=t, value=value):
                r.bias_sum[0, t] += value

    loop(total // CHUNK, bias_rows)
    bias_copy(0).start()

    def head_grads(rows_of):
        def one(t):
            for k in range(3):
                value = dot(rows_of(k, t), r.normed[t], TN)

                @pl.when(t == 0)
                def _(k=k, value=value):
                    r.acc[k] = value

                @pl.when(t > 0)
                def _(k=k, value=value):
                    r.acc[k] += value

        loop(chain, one)

    def head_copy(off):
        return remote(
            r.peer_acc.at[off - 1],
            r.peer_got.at[off - 1],
            r.sw.at[off],
            r.rw.at[off],
            (dp, a, lax.rem(b - off + cols, cols)),
        )

    def cross_sum(t):
        for k in range(3):
            for lag in range(1, cols):
                cross_copy(k, lag, t).wait_recv()
        own = grads[0](t)
        own[...] = partial_rows(t)

    chain_service(grads, 0, cross_sum)
    chain_finish(weights, r.done)
    for kind in (0, 1):
        share_copy(share_weights, kind).start()
    weights_keep = pltpu.make_async_copy(r.done, r.up_sum.at[part], r.sl.at[1])
    weights_keep.start()
    chain_service(grads, 1, cross_sum)
    for off in range(1, cols):
        head_grads(lambda k, t: r.peer_in[off - 1, k, t])
        r.peer_acc[off - 1] = r.acc[...].astype(BF)
        head_copy(off).start()
    head_grads(lambda k, t: (r.gq, r.gk, r.gv)[k][span(t * cols + b, share), :])
    out_keep.wait()
    others(lambda m: out_copy(me, m).wait_recv())
    add_rows(r.local.at[0], *[r.out_in.at[m] for m in range(n)])

    def later(s, _):
        chain_service(grads, s, cross_sum)
        return 0

    lax.fori_loop(2, chain - 1, later, 0)
    for k in range(3):
        total_k = r.acc[k]
        for off in range(1, cols):
            if k == 0:
                head_copy(off).wait_recv()
            total_k = total_k + r.peer_got[off - 1, k].astype(F32)
        r.local[1 + k] = total_k.astype(BF)

    def local_core(slot):
        return remote(
            r.local.at[far_part if slot else core_part], r.local_in.at[slot], r.st.at[slot], r.rt.at[slot], core_id
        )

    local_side = remote(r.local.at[side_part], r.local_side, r.sy.at[0], r.ry.at[0], side_id)
    for slot in (1, 0):
        local_core(slot).start()
    small_sum(0, 1)
    for slot in (1, 0):
        local_core(slot).wait_recv()
        spot = r.local.at[side_part if slot else part]
        add_rows(spot, spot, r.local_in.at[slot])
        if slot == 1:
            local_side.start()
    bias_copy(0).wait_recv()
    r.bias_sum[1] = r.bias_sum[0] + r.bias_in[0]
    bias_copy(1).start()
    share_copy(share_weights, 0, arriving=True).wait_recv()
    share_copy(share_weights, 2).start()
    local_side.wait_recv()
    bias_copy(1).wait_recv()
    r.bias_out[...] = r.bias_sum[1] + r.bias_in[1]
    add_rows(r.local_done, r.local.at[part], r.local_side)
    for kind in (0, 1):
        share_copy(share_local, kind).start()
    local_keep = pltpu.make_async_copy(r.local_done, r.head_sum.at[part], r.sl.at[2])
    local_keep.start()
    chain_finish(grads, r.gn)
    step = 32 if share % 32 == 0 else 16

    def norm_back(i, sums):
        cut = span(i, step)
        values = r.tokens[cut, :].astype(F32)
        grad = r.gn[cut, :]
        centered = values - jnp.mean(values, axis=-1, keepdims=True)
        scale = lax.rsqrt(jnp.mean(centered * centered, axis=-1, keepdims=True) + epsilon)
        unit = centered * scale
        scaled = grad * r.gain[...]
        along = jnp.mean(scaled * unit, axis=-1, keepdims=True)
        back = (scaled - jnp.mean(scaled, axis=-1, keepdims=True) - unit * along) * scale
        r.input_grad[cut, :] = (r.grad_hidden[cut, :] + back).astype(BF)
        gains = jnp.sum(grad * unit, axis=0, keepdims=True)
        return sums[0] + gains, sums[1] + jnp.sum(grad, axis=0, keepdims=True)

    zero = jnp.zeros((1, model), F32)
    gains, shifts = lax.fori_loop(0, share // step, norm_back, (zero, zero))
    upper = lax.broadcasted_iota(jnp.int32, (8, model), 0) == 0
    r.small[1, 0] = jnp.where(upper, gains, shifts)
    small_start(1, 0)
    small_sum(0, 2)
    share_copy(share_local, 0, arriving=True).wait_recv()
    share_copy(share_local, 2).start()
    for stage in range(3):
        small_sum(1, stage)

    weights_keep.wait()
    local_keep.wait()
    for flow in (share_weights, share_local):
        for kind in range(3):
            share_copy(flow, kind).wait_send()
            if kind > 0:
                share_copy(flow, kind, arriving=True).wait_recv()
    for slot in (1, 0):
        local_core(slot).wait_send()
    local_side.wait_send()
    for off in range(1, cols):
        head_copy(off).wait_send()
    for stage in range(2):
        bias_copy(stage).wait_send()
    for which in range(2):
        for stage in range(3):
            for copy in small_copies(which, stage):
                copy.wait_send()
    others(lambda m: row_copy(m, me).wait_send())
    others(lambda m: out_copy(m, me).wait_send())
    chain_drain(weights)
    chain_drain(grads)

    def drain(t):
        side_copy(t).wait_send()
        for slot in (1, 0):
            for k in (0, 1):
                core_copy(t, slot, k).wait_send()
        for lag in range(1, cols):
            for k in range(3):
                cross_copy(k, lag, t).wait_send()

    loop(chain, drain)


def rear(
    n, grad_rows, q_ext, k_ext, v_ext, lse, self_bias, attended, w_qkv, peer_w, normed, tokens, grad_hidden, gain,
    early, grad_up, grad_down, grad_out,
):
    chain, cols = mp_parts(n)
    heads, total, _ = q_ext.shape
    _, share, width = grad_rows.shape
    model = w_qkv.shape[1]
    rows = 2 * (grad_up.shape[0] // chain // PARTS)
    vmem = pl.BlockSpec(memory_space=pltpu.VMEM)
    anywhere = pl.BlockSpec(memory_space=pl.ANY)
    dma = pltpu.SemaphoreType.DMA
    head = pltpu.VMEM((total, width), BF)
    most = max(chain, cols, PARTS) - 1
    return pl.pallas_call(
        functools.partial(rear_kernel, n),
        name="rear",
        out_shape=(
            jax.ShapeDtypeStruct((PARTS, rows, model), BF),
            jax.ShapeDtypeStruct((PARTS, width, model), BF),
            jax.ShapeDtypeStruct((2, 8, width), F32),
            jax.ShapeDtypeStruct((share, model), BF),
            jax.ShapeDtypeStruct((2, 8, model), F32),
        ),
        in_specs=[vmem] * 14 + [anywhere] * 3,
        out_specs=(anywhere, anywhere, vmem, vmem, vmem),
        scratch_shapes=[
            head,
            pltpu.VMEM((heads, LANES, total), BF),
            pltpu.VMEM((heads, total, LANES), F32),
            pltpu.VMEM((heads, total, LANES), F32),
            head,
            head,
            head,
            pltpu.VMEM((chain, 2, rows, model), BF),
            pltpu.VMEM((chain * 2 * rows, model), BF),
            pltpu.VMEM((max(chain * rows, chain * share), model), BF),
            pltpu.VMEM((2, chain, rows, model), BF),
            pltpu.VMEM((rows, model), BF),
            pltpu.VMEM((n, width, model), BF),
            pltpu.VMEM((PARTS, width, model), BF),
            pltpu.VMEM((2, width, model), BF),
            pltpu.VMEM((width, model), BF),
            pltpu.VMEM((width, model), BF),
            pltpu.VMEM((3, width, model), F32),
            pltpu.VMEM((cols - 1, 3, chain, share, width), BF),
            pltpu.VMEM((cols - 1, 3, width, model), BF),
            pltpu.VMEM((cols - 1, 3, width, model), BF),
            pltpu.VMEM((2, chain, share, model), BF),
            pltpu.VMEM((share, model), F32),
            pltpu.VMEM((2, 3, 8, model), F32),
            pltpu.VMEM((2, 3, most, 8, model), F32),
            pltpu.VMEM((2, 2, 8, width), F32),
            pltpu.VMEM((2, 2, 8, width), F32),
            dma((n,)),
            dma((n,)),
            dma((n,)),
            dma((n,)),
            dma((chain, 2, 2)),
            dma((chain, 2, 2)),
            dma((chain, 2, 2)),
            dma((chain,)),
            dma((chain,)),
            dma((2, chain)),
            dma((2, chain)),
            dma((3,)),
            dma((3,)),
            dma((2,)),
            dma((2,)),
            dma((1,)),
            dma((1,)),
            dma((3,)),
            dma((3,)),
            dma((3, cols, chain)),
            dma((3, cols, chain)),
            dma((cols,)),
            dma((cols,)),
            dma((2, chain)),
            dma((2, chain)),
            dma((2, 3, most)),
            dma((2, 3, most)),
            dma((2,)),
            dma((2,)),
            dma((3,)),
        ],
        compiler_params=pltpu.CompilerParams(
            collective_id=1, has_side_effects=True, vmem_limit_bytes=VMEM_BYTES
        ),
    )(
        grad_rows, q_ext, k_ext, v_ext, lse, self_bias, attended, w_qkv, peer_w, normed, tokens, grad_hidden,
        gain[None, :], early, grad_up, grad_down, grad_out,
    )


def body(
    n,
    groups,
    tokens,
    image_ids,
    lengths,
    w_qkv,
    bias_query,
    bias_value,
    w_out,
    w_up,
    bias_up,
    w_down,
    out_biases,
    norm_gain,
    norm_bias,
    cotangent,
):
    share_rows = tokens.shape[0]
    a, b = lax.axis_index("mz"), lax.axis_index("mx")
    chain, cols = mp_parts(n)
    model_index = a * cols + b
    model, hidden = w_up.shape
    width = w_out.shape[0]

    def shifted(values, off):
        return lax.ppermute(values, "mx", [(i, (i + off) % cols) for i in range(cols)])

    def pair_sum(partial):
        blocks = jnp.split(partial, cols)
        total = blocks[0].astype(F32)
        for off in range(1, cols):
            total = total + shifted(blocks[off].astype(BF), cols - off).astype(F32)
        return total

    (
        gathered_one, q_ext, k_ext, v_ext, log_totals, attended, owned,
        up_all, down_all, out_all, bias_all, peer_w, self_bias, hidden_one, rows_two, grad_mlp,
    ) = front(
        n,
        image_ids,
        lengths,
        tokens,
        cotangent,
        norm_gain,
        norm_bias,
        out_biases,
        w_qkv,
        bias_query,
        bias_value,
        w_up,
        w_down,
        w_out,
        bias_up,
    )
    grad_out = grad_mlp[0].astype(F32)
    rows_two = rows_two.reshape(cols * share_rows, model)
    grad_mlp = grad_mlp.reshape(cols * share_rows, model)
    owned = jnp.transpose(owned, (1, 0, 2)).reshape(share_rows, -1)
    bias_all = bias_all[:, 0].reshape(-1)
    pre_act = jnp.dot(rows_two, up_all, preferred_element_type=F32) + bias_all
    activated = exact_gelu(pre_act).astype(BF)
    grad_act = jnp.einsum("rd,fd->rf", grad_mlp, down_all, preferred_element_type=F32)
    _, gelu_back = jax.vjp(exact_gelu, pre_act)
    grad_pre = gelu_back(grad_act)[0].astype(BF)
    grad_normed_two = pair_sum(jnp.einsum("rf,df->rd", grad_pre, up_all, preferred_element_type=F32))
    output_full = (
        hidden_one
        + pair_sum(jnp.dot(activated, down_all, preferred_element_type=F32))
        + out_biases[1]
    )
    grad_up_all = jnp.einsum("rf,rd->fd", grad_pre, rows_two, preferred_element_type=F32)
    grad_down_all = jnp.einsum("rf,rd->fd", activated, grad_mlp, preferred_element_type=F32)
    grad_bias_up = jnp.sum(grad_pre, axis=0, dtype=F32)

    _, norm_two_back = jax.vjp(layer_norm, hidden_one, norm_gain[1], norm_bias[1])
    grad_from_two, gain_two, shift_two = norm_two_back(grad_normed_two)
    grad_hidden = grad_out + grad_from_two
    grad_proj = grad_hidden.astype(BF)
    grad_w_out = jnp.einsum("re,rd->ed", owned, grad_proj, preferred_element_type=F32).astype(BF)
    grad_rows = jnp.einsum(
        "rd,ned->nre", grad_proj, out_all.reshape(n, width, model), preferred_element_type=F32
    ).astype(BF)
    bias_rows = lax.dynamic_update_slice(
        jnp.zeros((chain, cols, hidden), F32), grad_bias_up.reshape(chain, 1, hidden), (0, b, 0)
    )
    early = [gain_two, shift_two, jnp.sum(grad_hidden, axis=0), jnp.sum(grad_out, axis=0)]
    early = jnp.concatenate([jnp.stack(early), bias_rows.reshape(-1, model)])
    hidden_sum, head_sum, bias_sum, input_grad, small = rear(
        n,
        grad_rows,
        q_ext,
        k_ext,
        v_ext,
        log_totals,
        self_bias,
        attended,
        w_qkv,
        peer_w,
        gathered_one,
        tokens,
        grad_hidden,
        norm_gain[0],
        early,
        grad_up_all.astype(BF),
        grad_down_all.astype(BF),
        grad_w_out.reshape(n, width, model),
    )
    if groups > 1:
        hidden_sum, head_sum, bias_sum, small = lax.psum((hidden_sum, head_sum, bias_sum, small), "dg")
    half = hidden // PARTS
    grad_w_up = hidden_sum[:, :half].reshape(hidden, model).T.astype(F32)
    grad_w_down = hidden_sum[:, half:].reshape(hidden, model).astype(F32)
    grad_w_out = head_sum[0].astype(F32)
    grad_w_qkv = jnp.transpose(head_sum[1:], (0, 2, 1)).astype(F32)
    grad_bias_query, grad_bias_value = bias_sum[:, 0]
    grad_bias_up = lax.dynamic_slice_in_dim(
        small[0, 4:].reshape(-1), model_index * hidden, hidden, 0
    )
    return (
        output_full.astype(BF),
        input_grad,
        grad_w_qkv,
        grad_bias_query,
        grad_bias_value,
        grad_w_out,
        grad_w_up,
        grad_bias_up,
        grad_w_down,
        small[0, 2:4],
        jnp.stack([small[1, 0], small[0, 0]]),
        jnp.stack([small[1, 1], small[0, 1]]),
    )


def solution(mesh):
    n = mesh.shape["mp"]
    chain, cols = mp_parts(n)
    groups = mesh.shape["dp"] // PARTS
    dp, mp = ("dg", "dp"), ("mz", "mx")
    every = dp + mp
    split = jax.sharding.Mesh(mesh.devices.reshape(groups, PARTS, chain, cols), every)
    in_specs = (
        P(every, None),
        P(dp),
        P(dp, None),
        P(None, None, mp),
        P(mp),
        P(mp),
        P(mp, None),
        P(None, mp),
        P(mp),
        P(mp, None),
        P(),
        P(),
        P(),
        P(every, None),
    )
    out_specs = (
        P(every, None),
        P(every, None),
        P(None, None, mp),
        P(mp),
        P(mp),
        P(mp, None),
        P(None, mp),
        P(mp),
        P(mp, None),
        P(),
        P(),
        P(),
    )
    return jax.shard_map(
        functools.partial(body, n, groups),
        mesh=split,
        in_specs=in_specs,
        out_specs=out_specs,
        check_vma=False,
    )
```

```python
import functools
import types

import jax
import jax.numpy as jnp
from jax import lax
from jax.experimental import pallas as pl
from jax.experimental.pallas import tpu as pltpu
from jax.sharding import PartitionSpec as P

HEAD_DIM = 64
LANES = 128
CHUNK = 768
MASKED = -1e30
MESH = pl.DeviceIdType.MESH
VMEM_BYTES = 67_043_328
BF = jnp.bfloat16
F32 = jnp.float32
NN = (((1,), (0,)), ((), ()))
NT = (((1,), (1,)), ((), ()))
TN = (((0,), (0,)), ((), ()))
SCALE = HEAD_DIM ** (-0.5)
PARTS = 4
epsilon = 1e-06


def dot(left, right, dims=NN):
    return lax.dot_general(left, right, dims, preferred_element_type=F32)


def layer_norm(values, gain_vec, shift_vec):
    row_mean = jnp.mean(values, axis=-1, keepdims=True)
    centered = values - row_mean
    variance = jnp.mean(centered * centered, axis=-1, keepdims=True)
    return centered * lax.rsqrt(variance + epsilon) * gain_vec + shift_vec


def exact_gelu(values):
    return jax.nn.gelu(values, approximate=False)


def mp_parts(n):
    chain = min(4, n)
    return chain, n // chain


def column_sum(values):
    ones = jnp.ones((8, values.shape[1]), BF)
    high = values.astype(BF)
    low = (values - high.astype(F32)).astype(BF)
    return dot(ones, high, NT) + dot(ones, low, NT)


def split_three(column):
    high = column.astype(BF)
    rest = column - high.astype(F32)
    middle = rest.astype(BF)
    return high, middle, (rest - middle.astype(F32)).astype(BF)


def attend_chunk(c, heads, q_ref, k_ref, v_ref, vt_ref, self_ref, att_ref, lse_ref):
    rows = pl.ds(pl.multiple_of(c * CHUNK, CHUNK), CHUNK)
    pieces = []
    scores = [dot(k_ref[h], q_ref[h, rows, :], NT) for h in range(heads)]
    for h in range(heads):
        own = q_ref[h, rows, :HEAD_DIM].astype(F32) * k_ref[h, rows, :HEAD_DIM].astype(F32)
        own = column_sum(own)[:1] + self_ref[:1, rows]
        top = jnp.maximum(jnp.max(scores[h], axis=0, keepdims=True), own)
        weights = jnp.exp(scores[h] - top).astype(BF)
        own_weight = jnp.exp(own - top).astype(BF).astype(F32)
        summed = dot(vt_ref[h], weights) + vt_ref[h, :, rows].astype(F32) * own_weight
        total = summed[HEAD_DIM : HEAD_DIM + 1]
        pieces.append(summed[:HEAD_DIM] / total)
        lse_ref[h, :, rows] = jnp.broadcast_to(top + jnp.log(total), (8, CHUNK))
    stacked = jnp.concatenate(pieces, axis=0) if heads > 1 else pieces[0]
    att_ref[rows, :] = stacked.T.astype(BF)


def front_kernel(
    n,
    ids_ref,
    lengths_ref,
    tokens_ref,
    cot_ref,
    gain_ref,
    shift_ref,
    out_bias_ref,
    w_ref,
    bias_ref,
    up_ref,
    down_ref,
    out_ref,
    bup_ref,
    normed_ref,
    q_ref,
    k_ref,
    v_ref,
    lse_ref,
    att_ref,
    owned_ref,
    ups_ref,
    downs_ref,
    outs_out,
    bups_ref,
    peers_ref,
    self_ref,
    hidden_ref,
    pair_two,
    pair_cot,
    blocks,
    outs_ref,
    two,
    cot,
    peer_w,
    peer_b,
    proj_out,
    proj_in,
    vt_ref,
    owned,
    ssz,
    rsz,
    ssx,
    rsx,
    spw,
    rpw,
    spb,
    rpb,
    ssa,
    rsa,
    wsz,
    wrz,
    wsx,
    wrx,
    gs,
    gr,
    os,
    orr,
    bs,
    br,
    spp,
    rpp,
    local_sem,
):
    chain, cols = mp_parts(n)
    share, _ = tokens_ref.shape
    width = w_ref.shape[2]
    heads = width // HEAD_DIM
    hidden = up_ref.shape[1]
    up_rows, down_rows, out_rows = (r.shape[0] // PARTS for r in (up_ref, down_ref, out_ref))
    dg, dp = lax.axis_index("dg"), lax.axis_index("dp")
    a, b = lax.axis_index("mz"), lax.axis_index("mx")
    me = a * cols + b
    part = lax.rem(dp, PARTS)
    core_dp = dp + 1 - 2 * lax.rem(dp, 2)
    side_dp = dp + 2 - 4 * lax.rem(dp // 2, 2)
    core_part, side_part = lax.rem(core_dp, PARTS), lax.rem(side_dp, PARTS)
    far_part = PARTS - 1 - part

    barrier = pltpu.get_barrier_semaphore()
    for off in range(1, n):
        other = lax.rem(me + off, n)
        pl.semaphore_signal(
            barrier,
            inc=1,
            device_id=(dg, dp, other // cols, lax.rem(other, cols)),
            device_id_type=MESH,
        )
    for peer in (core_dp, side_dp):
        pl.semaphore_signal(barrier, inc=1, device_id=(dg, peer, a, b), device_id_type=MESH)
    pl.semaphore_wait(barrier, n + 1)

    def remote(src, dst, send, recv, device):
        return pltpu.make_async_remote_copy(
            src_ref=src,
            dst_ref=dst,
            send_sem=send,
            recv_sem=recv,
            device_id=(dg,) + device,
            device_id_type=MESH,
        )

    def span(index, size):
        return pl.ds(pl.multiple_of(index * size, size), size)

    def can(way):
        return (a < chain - 1) if way == 0 else (a > 0)

    def chain_peer(way):
        return (dp, jnp.clip(a + (1 if way == 0 else -1), 0, chain - 1), b)

    def cross_peer(off):
        return (dp, a, lax.rem(b + off, cols))

    def back_peer(off):
        return (dp, a, lax.rem(b - off + cols, cols))

    def chain_copy(row, way):
        spot = blocks.at[row]
        return remote(spot, spot, ssz.at[way, row], rsz.at[way, row], chain_peer(way))

    def cross_copy(row, off):
        return remote(
            proj_out.at[off - 1, row],
            proj_in.at[off - 1, row],
            ssx.at[off, row],
            rsx.at[off, row],
            back_peer(off),
        )

    def peer_copies(off):
        return [
            remote(w_ref, peer_w.at[off - 1], spw.at[off], rpw.at[off], cross_peer(off)),
            remote(bias_ref, peer_b.at[off - 1], spb.at[off], rpb.at[off], cross_peer(off)),
        ]

    def piece(i, row, of_part):
        if i == 0:
            return outs_ref.at[row * cols + b, span(of_part, out_rows)]
        if i == 1:
            return ups_ref.at[span(of_part, up_rows), span(row, hidden)]
        return downs_ref.at[span(row * PARTS + of_part, down_rows)]

    def own_piece(i):
        if i == 0:
            return out_ref.at[span(part, out_rows)]
        if i == 1:
            return up_ref.at[span(part, up_rows)]
        return down_ref.at[span(part, down_rows)]

    def weight_copy(i, row, way, own=False):
        spot = piece(i, row, part)
        sems = wsz.at[i, way, row], wrz.at[i, way, row]
        return remote(own_piece(i) if own else spot, spot, *sems, chain_peer(way))

    def out_cross(block, off, own=False):
        spot = outs_ref.at[block, span(part, out_rows)]
        sems = wsx.at[off, block // cols], wrx.at[off, block // cols]
        return remote(own_piece(0) if own else spot, spot, *sems, cross_peer(off))

    def group_copy(kind, i, row, arriving=False):
        sent = side_part if kind == 2 else part
        got = (side_part, core_part, far_part)[kind]
        spot = piece(i, row, got if arriving else sent)
        sems = gs.at[kind, i - 1, row], gr.at[kind, i - 1, row]
        return remote(spot, spot, *sems, (side_dp if kind == 0 else core_dp, a, b))

    def out_group(kind, arriving=False):
        sent = side_part if kind == 2 else part
        got = (side_part, core_part, far_part)[kind]
        spot = outs_ref.at[:, span(got if arriving else sent, out_rows)]
        return remote(spot, spot, os.at[kind], orr.at[kind], (side_dp if kind == 0 else core_dp, a, b))

    def bias_copy(off, arriving=False):
        spot = bups_ref.at[lax.rem(a - off + chain, chain) if arriving else a]
        return remote(bup_ref, spot, bs.at[off], br.at[off], (dp, lax.rem(a + off, chain), b))

    def start_own(way):
        for i in (1, 2):
            weight_copy(i, a, way, own=True).start()

    stay = [
        pltpu.make_async_copy(up_ref, ups_ref.at[:, span(a, hidden)], local_sem.at[1]),
        pltpu.make_async_copy(down_ref, downs_ref.at[span(a, hidden)], local_sem.at[2]),
        pltpu.make_async_copy(own_piece(0), piece(0, a, part), local_sem.at[3]),
        pltpu.make_async_copy(bup_ref, bups_ref.at[a], local_sem.at[4]),
    ]

    for off in range(1, cols):
        for copy in peer_copies(off):
            copy.start()
    normed = layer_norm(tokens_ref[...].astype(F32), gain_ref[:1], shift_ref[:1])
    blocks[a] = normed.astype(BF)

    total = n * share
    slot = total // 2
    first_id, last_id = ids_ref[0], ids_ref[total - 1]
    first_length, last_length = (
        jnp.where(k == 0, lengths_ref[0, 0], lengths_ref[0, 1]) for k in (first_id, last_id)
    )
    last_start = jnp.where(first_id == last_id, 0, slot)

    def row_facts(index):
        late = index >= slot
        inside = index - jnp.where(late, last_start, 0) < jnp.where(late, last_length, first_length)
        return jnp.where(late, last_id, first_id), inside

    def place(block, out_q, out_k, out_v):
        rows = span(block, share)
        lane = lax.broadcasted_iota(jnp.int32, (share, LANES - HEAD_DIM), 1)
        image, inside = row_facts(
            block * share + lax.broadcasted_iota(jnp.int32, (share, LANES - HEAD_DIM), 0)
        )
        tail_q = jnp.where(lane == image, 1.0, 0.0).astype(BF)
        hidden_key = jnp.where((lane == image) & inside, 0.0, MASKED)
        tail_k = jnp.where(lane < 2, hidden_key, 0.0).astype(BF)
        tail_v = jnp.where(lane < 3, 1.0, 0.0).astype(BF)
        for h in range(heads):
            cut = slice(h * HEAD_DIM, (h + 1) * HEAD_DIM)
            q_ref[h, rows, :] = jnp.concatenate(
                [out_q[:, cut] * jnp.asarray(SCALE, BF), tail_q], axis=1
            )
            k_ref[h, rows, :] = jnp.concatenate([out_k[:, cut], tail_k], axis=1)
            v_ref[h, rows, :] = jnp.concatenate([out_v[:, cut], tail_v], axis=1)

    def project(row):
        values = blocks[row]
        place(
            row * cols + b,
            (dot(values, w_ref[0]) + bias_ref[0, :1]).astype(BF),
            dot(values, w_ref[1]).astype(BF),
            (dot(values, w_ref[2]) + bias_ref[1, :1]).astype(BF),
        )

    def project_peer(row):
        def one(slot, _):
            values = blocks[row]
            proj_out[slot, row, 0] = (dot(values, peer_w[slot, 0]) + peer_b[slot, 0, :1]).astype(BF)
            proj_out[slot, row, 1] = dot(values, peer_w[slot, 1]).astype(BF)
            proj_out[slot, row, 2] = (dot(values, peer_w[slot, 2]) + peer_b[slot, 1, :1]).astype(BF)
            return 0

        lax.fori_loop(0, cols - 1, one, 0)
        for off in range(1, cols):
            cross_copy(row, off).start()

    for way in (0, 1):

        @pl.when(can(way))
        def _(way=way):
            chain_copy(a, way).start()
            weight_copy(0, a, way, own=True).start()

    def pair_copy(i, off):
        src, dst = ((two, pair_two), (cot, pair_cot))[i]
        return remote(src, dst.at[off], spp.at[i, off], rpp.at[i, off], cross_peer(off))

    pair_stay = [
        pltpu.make_async_copy(two, pair_two.at[0], local_sem.at[6]),
        pltpu.make_async_copy(cot, pair_cot.at[0], local_sem.at[7]),
    ]
    for copy in stay:
        copy.start()

    @pl.when(a == 0)
    def _():
        start_own(0)

    @pl.when(a == chain - 1)
    def _():
        start_own(1)

    project(a)
    _, self_inside = row_facts(lax.broadcasted_iota(jnp.int32, (8, total), 1))
    self_ref[...] = jnp.where(self_inside, MASKED, 0.0)

    def mask_cot(i, _):
        cut = span(i, 16)
        _, inside = row_facts(
            me * share + i * 16 + lax.broadcasted_iota(jnp.int32, (16, cot.shape[1]), 0)
        )
        cot[cut, :] = jnp.where(inside, cot_ref[cut, :].astype(F32), 0.0).astype(BF)
        return 0

    lax.fori_loop(0, share // 16, mask_cot, 0)

    def visit(step, _):
        for way in (0, 1):
            there = a - step if way == 0 else a + step
            inside = (there >= 0) & (there < chain)
            row = jnp.clip(there, 0, chain - 1)

            @pl.when(inside)
            def _(way=way, row=row):
                chain_copy(row, way).wait_recv()

                @pl.when(can(way))
                def _():
                    chain_copy(row, way).start()

                weight_copy(0, row, way).wait_recv()

                @pl.when(can(way))
                def _():
                    weight_copy(0, row, way).start()

        @pl.when((step == a) & can(0))
        def _():
            start_own(0)

        @pl.when((step == chain - 1 - a) & can(1))
        def _():
            start_own(1)

        @pl.when(step == 1)
        def _():
            for off in range(1, cols):
                for copy in peer_copies(off):
                    copy.wait_recv()

        def one(j, _):
            gone = step - jnp.where(j == 0, 1, 0)
            there = jnp.where(j == 1, a - gone, a + gone)

            @pl.when((there >= 0) & (there < chain) & ((j > 0) | (step == 1)))
            def _():
                @pl.when(j > 0)
                def _():
                    project(there)

                project_peer(there)

            return 0

        lax.fori_loop(0, 3, one, 0)
        return 0

    lax.fori_loop(1, chain, visit, 0)

    stay[2].wait()
    for off in range(1, cols):
        out_cross(me, off, own=True).start()

    def out_send(i, _):
        row = lax.rem(a + i, chain)
        for off in range(1, cols):
            out_cross(row * cols + b, off).start()
        return 0

    lax.fori_loop(1, chain, out_send, 0)

    def receive(i, _):
        row = lax.rem(a + i, chain)
        for off in range(1, cols):
            cross_copy(row, off).wait_recv()
            block = row * cols + lax.rem(b + off, cols)
            place(block, *[proj_in[off - 1, row, t] for t in range(3)])
        return 0

    lax.fori_loop(0, chain, receive, 0)
    keep = pltpu.make_async_copy(blocks, normed_ref, local_sem.at[0])
    keep.start()
    keep_peers = pltpu.make_async_copy(peer_w, peers_ref, local_sem.at[5])
    keep_peers.start()

    def gather_out(row, _):
        for off in range(1, cols):
            out_cross(row * cols + lax.rem(b - off + cols, cols), off).wait_recv()
        return 0

    lax.fori_loop(0, chain, gather_out, 0)
    out_group(0).start()
    out_group(1).start()
    for off in range(1, chain):
        bias_copy(off).start()

    def both_ways(step, act):
        for way in (0, 1):
            there = a - step if way == 0 else a + step

            @pl.when((there >= 0) & (there < chain))
            def _(way=way, there=there):
                act(way, jnp.clip(there, 0, chain - 1))

    def weights_pass(way, row):
        for i in (1, 2):
            weight_copy(i, row, way).wait_recv()

            @pl.when(can(way))
            def _(i=i):
                weight_copy(i, row, way).start()

            group_copy(0, i, row).start()
            group_copy(1, i, row).start()

    def weights_side(way, row):
        for i in (1, 2):
            group_copy(0, i, row, arriving=True).wait_recv()
            group_copy(2, i, row).start()

    both_ways(1, weights_pass)

    def flip(c, _):
        rows = span(c, CHUNK)
        for h in range(heads):
            vt_ref[h, :, rows] = v_ref[h, rows, :].astype(F32).T.astype(BF)
        return 0

    lax.fori_loop(0, n * share // CHUNK, flip, 0)

    def own_copy(target, source):
        return remote(
            att_ref.at[span(target, share)],
            owned.at[source],
            ssa.at[target],
            rsa.at[source],
            (dp, target // cols, lax.rem(target, cols)),
        )

    def attend(c, _):
        attend_chunk(c, heads, q_ref, k_ref, v_ref, vt_ref, self_ref, att_ref, lse_ref)

        def send(target, _):
            end = (target + 1) * share

            @pl.when((end <= (c + 1) * CHUNK) & (end > c * CHUNK) & (target != me))
            def _():
                own_copy(target, me).start()

            return 0

        lax.fori_loop(0, n, send, 0)

        @pl.when(c == 0)
        def _():
            out_group(0, arriving=True).wait_recv()
            out_group(2).start()

        @pl.when(c > 0)
        def _():
            both_ways(c + 1, weights_pass)
            both_ways(c, weights_side)

        return 0

    lax.fori_loop(0, n * share // CHUNK, attend, 0)
    owned[me] = att_ref[span(me, share), :]
    for off in range(1, cols):
        pair_copy(1, off).start()
    pair_stay[1].start()
    for kind in (1, 2):
        out_group(kind, arriving=True).wait_recv()
    keep_out = pltpu.make_async_copy(outs_ref, outs_out, local_sem.at[3])
    keep_out.start()

    def collect(other, _):
        @pl.when(other != me)
        def _():
            own_copy(other, me).wait_send()
            own_copy(me, other).wait_recv()

        return 0

    lax.fori_loop(0, n, collect, 0)
    hidden_ref[...] = tokens_ref[...].astype(F32) + out_bias_ref[:1]

    def out_project(m, _):
        hidden_ref[...] += dot(owned[m], outs_ref[m])
        return 0

    lax.fori_loop(0, n, out_project, 0)

    def norm_two(i, _):
        cut = span(i, 16)
        two[cut, :] = layer_norm(hidden_ref[cut, :], gain_ref[1:], shift_ref[1:]).astype(BF)
        return 0

    lax.fori_loop(0, share // 16, norm_two, 0)
    for off in range(1, cols):
        pair_copy(0, off).start()
    pair_stay[0].start()
    both_ways(chain - 1, weights_side)
    owned_ref[...] = owned[...]
    for off in range(1, cols):
        for i in (0, 1):
            pair_copy(i, off).wait_send()
            pair_copy(i, off).wait_recv()
    for copy in pair_stay:
        copy.wait()
    keep_out.wait()
    keep.wait()
    keep_peers.wait()
    for off in range(1, cols):
        for copy in peer_copies(off):
            copy.wait_send()
    for i in (0, 1, 3):
        stay[i].wait()
    for off in range(1, chain):
        bias_copy(off).wait_send()
        bias_copy(off, arriving=True).wait_recv()
    for kind in range(3):
        out_group(kind).wait_send()

    def drain(row, _):
        for off in range(1, cols):
            cross_copy(row, off).wait_send()
            out_cross(row * cols + b, off).wait_send()

        @pl.when((row <= a) & (a < chain - 1))
        def _():
            chain_copy(row, 0).wait_send()
            for i in range(3):
                weight_copy(i, row, 0).wait_send()

        @pl.when((row >= a) & (a > 0))
        def _():
            chain_copy(row, 1).wait_send()
            for i in range(3):
                weight_copy(i, row, 1).wait_send()

        @pl.when(row != a)
        def _():
            for i in (1, 2):
                for kind in range(3):
                    group_copy(kind, i, row).wait_send()
                    if kind > 0:
                        group_copy(kind, i, row, arriving=True).wait_recv()

        return 0

    lax.fori_loop(0, chain, drain, 0)


def front(
    n, image_ids, lengths, tokens, cotangent, gain, shift, out_biases, w_qkv, bias_query, bias_value, w_up, w_down,
    w_out, bias_up,
):
    chain, cols = mp_parts(n)
    share, model = tokens.shape
    width = w_qkv.shape[2]
    heads = width // HEAD_DIM
    hidden = w_up.shape[1]
    rows = n * share
    vmem = pl.BlockSpec(memory_space=pltpu.VMEM)
    anywhere = pl.BlockSpec(memory_space=pl.ANY)
    ext = jax.ShapeDtypeStruct((heads, rows, LANES), BF)
    dma = pltpu.SemaphoreType.DMA
    return pl.pallas_call(
        functools.partial(front_kernel, n),
        name="front",
        out_shape=(
            jax.ShapeDtypeStruct((chain, share, model), BF),
            ext,
            ext,
            ext,
            jax.ShapeDtypeStruct((heads, 8, rows), F32),
            jax.ShapeDtypeStruct((rows, width), BF),
            jax.ShapeDtypeStruct((n, share, width), BF),
            jax.ShapeDtypeStruct((model, chain * hidden), BF),
            jax.ShapeDtypeStruct((chain * hidden, model), BF),
            jax.ShapeDtypeStruct((n, width, model), BF),
            jax.ShapeDtypeStruct((chain, 8, hidden), F32),
            jax.ShapeDtypeStruct((cols - 1,) + w_qkv.shape, BF),
            jax.ShapeDtypeStruct((8, rows), F32),
            jax.ShapeDtypeStruct((share, model), F32),
            jax.ShapeDtypeStruct((cols, share, model), BF),
            jax.ShapeDtypeStruct((cols, share, model), BF),
        ),
        in_specs=[pl.BlockSpec(memory_space=pltpu.SMEM)] * 2 + [vmem] * 11,
        out_specs=(anywhere,) + (vmem,) * 6 + (anywhere,) * 5 + (vmem,) * 2 + (anywhere,) * 2,
        scratch_shapes=[
            pltpu.VMEM((chain, share, model), BF),
            pltpu.VMEM((n, width, model), BF),
            pltpu.VMEM((share, model), BF),
            pltpu.VMEM((share, model), BF),
            pltpu.VMEM((cols - 1,) + w_qkv.shape, BF),
            pltpu.VMEM((cols - 1, 2, 8, width), F32),
            pltpu.VMEM((cols - 1, chain, 3, share, width), BF),
            pltpu.VMEM((cols - 1, chain, 3, share, width), BF),
            pltpu.VMEM((heads, LANES, rows), BF),
            pltpu.VMEM((n, share, width), BF),
            dma((2, chain)),
            dma((2, chain)),
            dma((cols, chain)),
            dma((cols, chain)),
            dma((cols,)),
            dma((cols,)),
            dma((cols,)),
            dma((cols,)),
            dma((n,)),
            dma((n,)),
            dma((3, 2, chain)),
            dma((3, 2, chain)),
            dma((cols, chain)),
            dma((cols, chain)),
            dma((3, 2, chain)),
            dma((3, 2, chain)),
            dma((3,)),
            dma((3,)),
            dma((chain,)),
            dma((chain,)),
            dma((2, cols)),
            dma((2, cols)),
            dma((8,)),
        ],
        compiler_params=pltpu.CompilerParams(
            collective_id=0, has_side_effects=True, vmem_limit_bytes=VMEM_BYTES
        ),
    )(
        image_ids,
        lengths,
        tokens,
        cotangent,
        gain,
        shift,
        out_biases,
        w_qkv,
        jnp.broadcast_to(jnp.stack([bias_query, bias_value])[:, None, :], (2, 8, width)),
        w_up,
        w_down,
        w_out,
        jnp.broadcast_to(bias_up[None, :], (8, hidden)),
    )


def attend_back_chunk(
    c, heads, q_ref, k_ref, v_ref, kt_ref, lse_ref, self_ref, att_ref, grad_ref, gq_ref, dk_ref, dv_ref
):
    rows = pl.ds(pl.multiple_of(c * CHUNK, CHUNK), CHUNK)
    grads = grad_ref[rows, :].astype(F32)
    products = grads * att_ref[rows, :].astype(F32)
    outs = []
    for h in range(heads):
        cut = slice(h * HEAD_DIM, (h + 1) * HEAD_DIM)
        inner = jnp.sum(products[:, cut], axis=1, keepdims=True)
        parts = split_three(-inner)
        lane = lax.broadcasted_iota(jnp.int32, (CHUNK, LANES - HEAD_DIM), 1)
        tail = jnp.zeros((CHUNK, LANES - HEAD_DIM), F32)
        for i, part in enumerate(parts):
            tail = jnp.where(lane == i, part.astype(F32), tail)
        grad_ext = jnp.concatenate([grads[:, cut], tail], axis=1).astype(BF)
        query = q_ref[h, rows, :]
        key_own = k_ref[h, rows, :]
        scores = dot(k_ref[h], query, NT)
        lse = lse_ref[h, :1, rows]
        probs = jnp.exp(scores - lse)
        shifted = dot(v_ref[h], grad_ext, NT)
        own = column_sum(query[:, :HEAD_DIM].astype(F32) * key_own[:, :HEAD_DIM].astype(F32))
        own_prob = jnp.exp(own + self_ref[:, rows] - lse)
        own_shifted = column_sum(v_ref[h, rows, :].astype(F32) * grad_ext.astype(F32))
        lower = lax.broadcasted_iota(jnp.int32, (8, CHUNK), 0) < 4
        both = jnp.where(lower, own_prob, own_prob * own_shifted).T
        own_prob, own_score = both[:, :1], both[:, 4:5]
        grad_scores = (probs * shifted).astype(BF)
        dv = dot(probs.astype(BF), grad_ext)
        dk = dot(grad_scores, query)
        dq = dot(kt_ref[h], grad_scores).T
        dq = (dq + own_score * key_own.astype(F32)) * SCALE
        outs.append(dq[:, :HEAD_DIM])

        @pl.when(c == 0)
        def _(h=h, dv=dv, dk=dk):
            dv_ref[h] = dv
            dk_ref[h] = dk

        @pl.when(c > 0)
        def _(h=h, dv=dv, dk=dk):
            dv_ref[h] += dv
            dk_ref[h] += dk

        dv_ref[h, rows, :] += own_prob * grad_ext.astype(F32)
        dk_ref[h, rows, :] += own_score * query.astype(F32)
    stacked = jnp.concatenate(outs, axis=1) if heads > 1 else outs[0]
    gq_ref[rows, :] = stacked.astype(BF)


REAR_REFS = (
    "gatt",
    "q",
    "k",
    "v",
    "lse",
    "self_bias",
    "att",
    "w",
    "peer_w",
    "normed",
    "tokens",
    "grad_hidden",
    "gain",
    "early",
    "up",
    "down",
    "out",
    "up_sum",
    "head_sum",
    "bias_out",
    "input_grad",
    "small_out",
    "grad",
    "kt",
    "dk",
    "dv",
    "gq",
    "gk",
    "gv",
    "kept",
    "pool_core",
    "pool_side",
    "way_in",
    "out_in",
    "local_in",
    "local_side",
    "acc",
    "peer_in",
    "peer_got",
    "way_gn",
    "gn",
    "small",
    "small_in",
    "bias_sum",
    "bias_in",
    "sa",
    "ra",
    "so",
    "ro",
    "sc",
    "rc",
    "sk",
    "ss",
    "rs",
    "sz",
    "rz",
    "sg",
    "rg",
    "st",
    "rt",
    "sy",
    "ry",
    "sh",
    "rh",
    "sx",
    "rx",
    "sw",
    "rw",
    "sn",
    "rn",
    "sm",
    "rm",
    "sb",
    "rb",
    "sl",
)


def rear_kernel(n, *refs):
    r = types.SimpleNamespace(**dict(zip(REAR_REFS, refs)))
    chain, cols = mp_parts(n)
    heads, total, _ = r.q.shape
    _, share, width = r.gatt.shape
    model = r.w.shape[1]
    hidden = r.up.shape[0] // chain
    rows, out_rows = hidden // PARTS, width // PARTS
    block_rows = 2 * rows + cols * out_rows
    done_rows = 2 * rows + out_rows
    local_rows = 3 * width // PARTS
    head_base = (cols - 1) * 3 * width
    done_base = head_base + 3 * width
    local = r.pool_core.at[pl.ds(head_base, 3 * width)]
    done = r.pool_core.at[pl.ds(done_base, block_rows)]
    local_done = r.pool_core.at[pl.ds(done_base + block_rows, local_rows)]
    dg, dp = lax.axis_index("dg"), lax.axis_index("dp")
    a, b = lax.axis_index("mz"), lax.axis_index("mx")
    me = a * cols + b
    part = lax.rem(dp, PARTS)
    core_dp = dp + 1 - 2 * lax.rem(dp, 2)
    side_dp = dp + 2 - 4 * lax.rem(dp // 2, 2)
    core_part, side_part = lax.rem(core_dp, PARTS), lax.rem(side_dp, PARTS)
    far_part = PARTS - 1 - part
    core_id, side_id = (core_dp, a, b), (side_dp, a, b)
    far_id = (PARTS - 1 - dp, a, b)

    def mp_id(index):
        return dp, index // cols, lax.rem(index, cols)

    barrier = pltpu.get_barrier_semaphore()
    for off in range(1, n):
        pl.semaphore_signal(
            barrier, inc=1, device_id=(dg,) + mp_id(lax.rem(me + off, n)), device_id_type=MESH
        )
    for peer in (core_id, side_id, far_id):
        pl.semaphore_signal(barrier, inc=1, device_id=(dg,) + peer, device_id_type=MESH)
    pl.semaphore_wait(barrier, n + 2)

    def remote(src, dst, send, recv, device):
        return pltpu.make_async_remote_copy(
            src_ref=src,
            dst_ref=dst,
            send_sem=send,
            recv_sem=recv,
            device_id=(dg,) + device,
            device_id_type=MESH,
        )

    def span(index, size):
        return pl.ds(pl.multiple_of(index * size, size), size)

    def in_order(i):
        low = jnp.where(chain - 1 - i > a, chain - 1 - i, chain - 2 - i)
        high = jnp.where(i < a, i, i + 1)
        return jnp.where(i == chain - 1, a, jnp.where(2 * a < chain, low, high))

    def add_rows(dst, *terms):
        count = dst.shape[0]
        step = 32 if count % 32 == 0 else 16

        def one(i, _):
            cut = span(i, step)
            value = terms[0][cut, :].astype(F32)
            for term in terms[1:]:
                value = value + term[cut, :].astype(F32)
            dst[cut, :] = value.astype(dst.dtype)
            return 0

        lax.fori_loop(0, count // step, one, 0)

    def loop(count, act):
        def one(i, _):
            act(i)
            return 0

        lax.fori_loop(0, count, one, 0)

    def others(act):
        def one(m):
            @pl.when(m != me)
            def _():
                act(m)

        loop(n, one)

    def row_copy(target, source):
        return remote(
            r.gatt.at[target], r.grad.at[span(source, share)], r.sa.at[target], r.ra.at[source], mp_id(target)
        )

    def source_rows(i, t, which):
        if i < 2:
            return (r.up, r.down)[i].at[span(t * PARTS + which, rows)]
        return r.out.at[t * cols + lax.rem(b + i - 2, cols), span(which, out_rows)]

    def offset(i):
        return i * rows if i < 2 else 2 * rows + (i - 2) * out_rows

    def core_copy(t, slot, i):
        src = source_rows(i, t, far_part if slot else core_part)
        base = pl.multiple_of((t * 2 + slot) * block_rows + offset(i), 16)
        return remote(
            src, r.pool_core.at[pl.ds(base, src.shape[0])], r.sc.at[t, slot, i], r.rc.at[t, slot, i], core_id
        )

    def keep_copy(t, slot, i):
        src = source_rows(i, t, side_part if slot else part)
        return pltpu.make_async_copy(
            src, r.kept.at[t, slot, pl.ds(offset(i), src.shape[0])], r.sk.at[t, slot, i]
        )

    def side_copy(t):
        return remote(r.kept.at[t, 1], r.pool_side.at[span(t, block_rows)], r.ss.at[t], r.rs.at[t], side_id)

    def chain_id(way):
        return dp, jnp.clip(a + (1 if way == 0 else -1), 0, chain - 1), b

    def hop_of(way):
        return a if way == 0 else chain - 1 - a

    def ahead(way, t):
        return (t > a) if way == 0 else (t < a)

    def chain_copy(flow, way, t, fresh=False):
        own, inbox, send, recv = flow
        spot = inbox.at[way, t]
        return remote(own(t) if fresh else spot, spot, send.at[way, t], recv.at[way, t], chain_id(way))

    def chain_service(flow, s, prepare):
        own, inbox = flow[:2]
        for way in (0, 1):
            hop = hop_of(way)
            t = chain - 1 + a - s if way == 0 else s - hop
            active = (t > a) & (t < chain) if way == 0 else (t >= 0) & (t < a)
            spot = jnp.clip(t, 0, chain - 1)

            @pl.when(active)
            def _(way=way, t=spot):
                prepare(t)

            @pl.when(active & (hop == 0))
            def _(way=way, t=spot):
                chain_copy(flow, way, t, fresh=True).start()

            @pl.when(active & (hop > 0))
            def _(way=way, t=spot):
                chain_copy(flow, way, t).wait_recv()
                add_rows(inbox.at[way, t], inbox.at[way, t], own(t))
                chain_copy(flow, way, t).start()

    def chain_finish(flow, dst, prepare):
        own, inbox = flow[:2]
        prepare(a)

        @pl.when(a > 0)
        def _():
            chain_copy(flow, 0, a).wait_recv()

        @pl.when(a < chain - 1)
        def _():
            chain_copy(flow, 1, a).wait_recv()

        @pl.when((a > 0) & (a < chain - 1))
        def _():
            add_rows(dst, own(a), inbox.at[0, a], inbox.at[1, a])

        @pl.when(a == 0)
        def _():
            add_rows(dst, own(a), inbox.at[1, a])

        @pl.when(a == chain - 1)
        def _():
            add_rows(dst, own(a), inbox.at[0, a])

    def chain_drain(flow):
        def one(t):
            for way in (0, 1):

                @pl.when(ahead(way, t))
                def _(way=way):
                    chain_copy(flow, way, t).wait_send()

        loop(chain, one)

    def share_copy(share_flow, kind, arriving=False):
        own, everyone, send, recv = share_flow
        sent = side_part if kind == 2 else part
        got = (side_part, core_part, far_part)[kind]
        spot = everyone.at[got if arriving else sent]
        src = spot if kind == 2 or arriving else own
        return remote(src, spot, send.at[kind], recv.at[kind], side_id if kind == 0 else core_id)

    weights = (lambda t: r.kept.at[t, 0], r.way_in, r.sz, r.rz)
    grads = (lambda t: r.pool_side.at[span(t, share)], r.way_gn, r.sn, r.rn)
    share_weights = (done.at[pl.ds(0, done_rows)], r.up_sum, r.sg, r.rg)
    share_local = (local_done, r.head_sum, r.sh, r.rh)

    def small_peers(stage):
        if stage == 0:
            return [core_id, side_id, far_id]
        if stage == 1:
            return [(dp, a, lax.rem(b + off, cols)) for off in range(1, cols)]
        return [(dp, lax.rem(a + off, chain), b) for off in range(1, chain)]

    def small_copies(which, stage):
        src = r.early if which == 0 and stage == 0 else r.small.at[which, stage]
        return [
            remote(src, r.small_in.at[which, stage, i], r.sm.at[which, stage, i], r.rm.at[which, stage, i], peer)
            for i, peer in enumerate(small_peers(stage))
        ]

    def small_start(which, stage):
        for copy in small_copies(which, stage):
            copy.start()

    def small_sum(which, stage):
        value = r.early[...] if which == 0 and stage == 0 else r.small[which, stage]
        for i, copy in enumerate(small_copies(which, stage)):
            copy.wait_recv()
            value = value + r.small_in[which, stage, i]
        if stage < 2:
            r.small[which, stage + 1] = value
            small_start(which, stage + 1)
        else:
            r.small_out[which] = value

    def bias_copy(stage):
        return remote(
            r.bias_sum.at[stage], r.bias_in.at[stage], r.sb.at[stage], r.rb.at[stage], (core_id, side_id)[stage]
        )

    others(lambda m: row_copy(m, me).start())
    small_start(0, 0)

    def start_core(i):
        t = in_order(i)
        for slot in (1, 0):
            for k in range(2 + cols):
                core_copy(t, slot, k).start()
                keep_copy(t, slot, k).start()

    loop(chain, start_core)
    r.grad[span(me, share), :] = r.gatt[me]

    def flip(c):
        cut = span(c, CHUNK)
        for h in range(heads):
            r.kt[h, :, cut] = r.k[h, cut, :].astype(F32).T.astype(BF)

    loop(total // CHUNK, flip)

    def core_sum(i):
        t = in_order(i)
        for slot in (1, 0):
            for k in range(2 + cols):
                keep_copy(t, slot, k).wait()
                core_copy(t, slot, k).wait_recv()
            add_rows(r.kept.at[t, slot], r.kept.at[t, slot], r.pool_core.at[span(t * 2 + slot, block_rows)])
            if slot == 1:
                side_copy(t).start()

    loop(chain, core_sum)
    others(lambda m: row_copy(me, m).wait_recv())

    def side_sum(t):
        side_copy(t).wait_recv()
        add_rows(r.kept.at[t, 0], r.kept.at[t, 0], r.pool_side.at[span(t, block_rows)])

    def cross_copy(k, lag, t):
        return remote(
            (r.gq, r.gk, r.gv)[k].at[span(t * cols + lax.rem(b + lag, cols), share)],
            r.peer_in.at[lag - 1, k, t],
            r.sx.at[k, lag, t],
            r.rx.at[k, lag, t],
            (dp, a, lax.rem(b + lag, cols)),
        )

    chain_service(weights, 0, side_sum)

    def attend(c):
        attend_back_chunk(
            c, heads, r.q, r.k, r.v, r.kt, r.lse, r.self_bias, r.att, r.grad, r.gq, r.dk, r.dv
        )

        def send(t):
            for lag in range(1, cols):
                end = (t * cols + lax.rem(b + lag, cols) + 1) * share

                @pl.when((end <= (c + 1) * CHUNK) & (end > c * CHUNK))
                def _(lag=lag):
                    cross_copy(0, lag, t).start()

        loop(chain, send)

        @pl.when(c < chain - 2)
        def _():
            chain_service(weights, c + 1, side_sum)


    loop(total // CHUNK, attend)

    def finish(c):
        cut = span(c, CHUNK)
        for src, dst in ((r.dk, r.gk), (r.dv, r.gv)):
            parts = [src[h, cut, :HEAD_DIM] for h in range(heads)]
            dst[cut, :] = (jnp.concatenate(parts, axis=1) if heads > 1 else parts[0]).astype(BF)

    loop(total // CHUNK, finish)

    def send_rest(i):
        for k in (1, 2):
            for lag in range(1, cols):
                cross_copy(k, lag, in_order(i)).start()

    loop(chain, send_rest)
    def out_copy(lag):
        return remote(
            done.at[pl.ds(offset(2 + lag), out_rows)],
            r.out_in.at[lag - 1],
            r.so.at[lag],
            r.ro.at[lag],
            (dp, a, lax.rem(b + lag, cols)),
        )

    chain_finish(weights, done, side_sum)
    for lag in range(1, cols):
        out_copy(lag).start()

    small_sum(0, 0)

    def partial_rows(t):
        cut = span(t * cols + b, share)
        value = dot(r.gq[cut, :], r.w[0], NT) + dot(r.gk[cut, :], r.w[1], NT)
        value = value + dot(r.gv[cut, :], r.w[2], NT)
        for slot in range(cols - 1):
            for k in range(3):
                value = value + dot(r.peer_in[slot, k, t], r.peer_w[slot, k], NT)
        return value.astype(BF)

    def bias_rows(c):
        ones = jnp.ones((8, CHUNK), BF)
        for t, src in ((0, r.gq), (1, r.gv)):
            value = dot(ones, src[span(c, CHUNK), :])

            @pl.when(c == 0)
            def _(t=t, value=value):
                r.bias_sum[0, t] = value

            @pl.when(c > 0)
            def _(t=t, value=value):
                r.bias_sum[0, t] += value

    loop(total // CHUNK, bias_rows)
    bias_copy(0).start()

    def head_grads(rows_of):
        def one(t):
            for k in range(3):
                value = dot(rows_of(k, t), r.normed[t], TN)

                @pl.when(t == 0)
                def _(k=k, value=value):
                    r.acc[k] = value

                @pl.when(t > 0)
                def _(k=k, value=value):
                    r.acc[k] += value

        loop(chain, one)

    def head_copy(off):
        return remote(
            r.pool_core.at[pl.ds((off - 1) * 3 * width, 3 * width)],
            r.peer_got.at[off - 1],
            r.sw.at[off],
            r.rw.at[off],
            (dp, a, lax.rem(b - off + cols, cols)),
        )

    def cross_wait(t):
        for k in range(3):
            for lag in range(1, cols):
                cross_copy(k, lag, t).wait_recv()

    def cross_sum(t):
        own = grads[0](t)
        own[...] = partial_rows(t)

    def first_sum(t):
        cross_wait(t)
        cross_sum(t)

    def wait_rest(i):
        @pl.when((i > 0) | ((a > 0) & (a < chain - 1)))
        def _():
            cross_wait(in_order(i))

    chain_service(grads, 0, first_sum)
    for lag in range(1, cols):
        out_copy(lag).wait_recv()
    spot = done.at[pl.ds(offset(2), out_rows)]
    add_rows(spot, spot, *[r.out_in.at[lag - 1] for lag in range(1, cols)])
    for kind in (0, 1):
        share_copy(share_weights, kind).start()
    weights_keep = pltpu.make_async_copy(done.at[pl.ds(0, done_rows)], r.up_sum.at[part], r.sl.at[1])
    weights_keep.start()
    loop(chain, wait_rest)
    chain_service(grads, 1, cross_sum)
    for off in range(1, cols):
        head_grads(lambda k, t: r.peer_in[off - 1, k, t])
        for k in range(3):
            r.pool_core[pl.ds(((off - 1) * 3 + k) * width, width), :] = r.acc[k].astype(BF)
        head_copy(off).start()
    head_grads(lambda k, t: (r.gq, r.gk, r.gv)[k][span(t * cols + b, share), :])
    def later(s, _):
        chain_service(grads, s, cross_sum)
        return 0

    lax.fori_loop(2, chain - 1, later, 0)
    for k in range(3):
        total_k = r.acc[k]
        for off in range(1, cols):
            if k == 0:
                head_copy(off).wait_recv()
            total_k = total_k + r.peer_got[off - 1, pl.ds(k * width, width)].astype(F32)
        local[span(k, width), :] = total_k.astype(BF)

    def local_core(slot):
        return remote(
            local.at[span(far_part if slot else core_part, local_rows)], r.local_in.at[slot], r.st.at[slot], r.rt.at[slot], core_id
        )

    local_side = remote(local.at[span(side_part, local_rows)], r.local_side, r.sy.at[0], r.ry.at[0], side_id)
    for slot in (1, 0):
        local_core(slot).start()
    small_sum(0, 1)
    for slot in (1, 0):
        local_core(slot).wait_recv()
        spot = local.at[span(side_part if slot else part, local_rows)]
        add_rows(spot, spot, r.local_in.at[slot])
        if slot == 1:
            local_side.start()
    bias_copy(0).wait_recv()
    r.bias_sum[1] = r.bias_sum[0] + r.bias_in[0]
    bias_copy(1).start()
    share_copy(share_weights, 0, arriving=True).wait_recv()
    share_copy(share_weights, 2).start()
    local_side.wait_recv()
    bias_copy(1).wait_recv()
    r.bias_out[...] = r.bias_sum[1] + r.bias_in[1]
    add_rows(local_done, local.at[span(part, local_rows)], r.local_side)
    for kind in (0, 1):
        share_copy(share_local, kind).start()
    local_keep = pltpu.make_async_copy(local_done, r.head_sum.at[part], r.sl.at[2])
    local_keep.start()
    chain_finish(grads, r.gn, cross_sum)
    step = 32 if share % 32 == 0 else 16

    def norm_back(i, sums):
        cut = span(i, step)
        values = r.tokens[cut, :].astype(F32)
        grad = r.gn[cut, :]
        centered = values - jnp.mean(values, axis=-1, keepdims=True)
        scale = lax.rsqrt(jnp.mean(centered * centered, axis=-1, keepdims=True) + epsilon)
        unit = centered * scale
        scaled = grad * r.gain[...]
        along = jnp.mean(scaled * unit, axis=-1, keepdims=True)
        back = (scaled - jnp.mean(scaled, axis=-1, keepdims=True) - unit * along) * scale
        r.input_grad[cut, :] = (r.grad_hidden[cut, :] + back).astype(BF)
        gains = jnp.sum(grad * unit, axis=0, keepdims=True)
        return sums[0] + gains, sums[1] + jnp.sum(grad, axis=0, keepdims=True)

    zero = jnp.zeros((1, model), F32)
    gains, shifts = lax.fori_loop(0, share // step, norm_back, (zero, zero))
    upper = lax.broadcasted_iota(jnp.int32, (8, model), 0) == 0
    r.small[1, 0] = jnp.where(upper, gains, shifts)
    small_start(1, 0)
    small_sum(0, 2)
    share_copy(share_local, 0, arriving=True).wait_recv()
    share_copy(share_local, 2).start()
    for stage in range(3):
        small_sum(1, stage)

    weights_keep.wait()
    local_keep.wait()
    for flow in (share_weights, share_local):
        for kind in range(3):
            share_copy(flow, kind).wait_send()
            if kind > 0:
                share_copy(flow, kind, arriving=True).wait_recv()
    for slot in (1, 0):
        local_core(slot).wait_send()
    local_side.wait_send()
    for off in range(1, cols):
        head_copy(off).wait_send()
        out_copy(off).wait_send()
    for stage in range(2):
        bias_copy(stage).wait_send()
    for which in range(2):
        for stage in range(3):
            for copy in small_copies(which, stage):
                copy.wait_send()
    others(lambda m: row_copy(m, me).wait_send())
    chain_drain(weights)
    chain_drain(grads)

    def drain(t):
        side_copy(t).wait_send()
        for slot in (1, 0):
            for k in range(2 + cols):
                core_copy(t, slot, k).wait_send()
        for lag in range(1, cols):
            for k in range(3):
                cross_copy(k, lag, t).wait_send()

    loop(chain, drain)


def rear(
    n, grad_rows, q_ext, k_ext, v_ext, lse, self_bias, attended, w_qkv, peer_w, normed, tokens, grad_hidden, gain,
    early, grad_up, grad_down, grad_out,
):
    chain, cols = mp_parts(n)
    heads, total, _ = q_ext.shape
    _, share, width = grad_rows.shape
    model = w_qkv.shape[1]
    rows = 2 * (grad_up.shape[0] // chain // PARTS)
    block, done = rows + cols * width // PARTS, rows + width // PARTS
    local = 3 * width // PARTS
    vmem = pl.BlockSpec(memory_space=pltpu.VMEM)
    anywhere = pl.BlockSpec(memory_space=pl.ANY)
    dma = pltpu.SemaphoreType.DMA
    head = pltpu.VMEM((total, width), BF)
    most = max(chain, cols, PARTS) - 1
    return pl.pallas_call(
        functools.partial(rear_kernel, n),
        name="rear",
        out_shape=(
            jax.ShapeDtypeStruct((PARTS, done, model), BF),
            jax.ShapeDtypeStruct((PARTS, local, model), BF),
            jax.ShapeDtypeStruct((2, 8, width), F32),
            jax.ShapeDtypeStruct((share, model), BF),
            jax.ShapeDtypeStruct((2, 8, model), F32),
        ),
        in_specs=[vmem] * 14 + [anywhere] * 3,
        out_specs=(anywhere, anywhere, vmem, vmem, vmem),
        scratch_shapes=[
            head,
            pltpu.VMEM((heads, LANES, total), BF),
            pltpu.VMEM((heads, total, LANES), F32),
            pltpu.VMEM((heads, total, LANES), F32),
            head,
            head,
            head,
            pltpu.VMEM((chain, 2, block, model), BF),
            pltpu.VMEM((chain * 2 * block, model), BF),
            pltpu.VMEM((chain * max(block, share), model), BF),
            pltpu.VMEM((2, chain, block, model), BF),
            pltpu.VMEM((cols - 1, width // PARTS, model), BF),
            pltpu.VMEM((2, local, model), BF),
            pltpu.VMEM((local, model), BF),
            pltpu.VMEM((3, width, model), F32),
            pltpu.VMEM((cols - 1, 3, chain, share, width), BF),
            pltpu.VMEM((cols - 1, 3 * width, model), BF),
            pltpu.VMEM((2, chain, share, model), BF),
            pltpu.VMEM((share, model), F32),
            pltpu.VMEM((2, 3, 8, model), F32),
            pltpu.VMEM((2, 3, most, 8, model), F32),
            pltpu.VMEM((2, 2, 8, width), F32),
            pltpu.VMEM((2, 2, 8, width), F32),
            dma((n,)),
            dma((n,)),
            dma((cols,)),
            dma((cols,)),
            dma((chain, 2, 2 + cols)),
            dma((chain, 2, 2 + cols)),
            dma((chain, 2, 2 + cols)),
            dma((chain,)),
            dma((chain,)),
            dma((2, chain)),
            dma((2, chain)),
            dma((3,)),
            dma((3,)),
            dma((2,)),
            dma((2,)),
            dma((1,)),
            dma((1,)),
            dma((3,)),
            dma((3,)),
            dma((3, cols, chain)),
            dma((3, cols, chain)),
            dma((cols,)),
            dma((cols,)),
            dma((2, chain)),
            dma((2, chain)),
            dma((2, 3, most)),
            dma((2, 3, most)),
            dma((2,)),
            dma((2,)),
            dma((3,)),
        ],
        compiler_params=pltpu.CompilerParams(
            collective_id=1, has_side_effects=True, vmem_limit_bytes=VMEM_BYTES
        ),
    )(
        grad_rows, q_ext, k_ext, v_ext, lse, self_bias, attended, w_qkv, peer_w, normed, tokens, grad_hidden,
        gain[None, :], early, grad_up, grad_down, grad_out,
    )


def body(
    n,
    groups,
    tokens,
    image_ids,
    lengths,
    w_qkv,
    bias_query,
    bias_value,
    w_out,
    w_up,
    bias_up,
    w_down,
    out_biases,
    norm_gain,
    norm_bias,
    cotangent,
):
    share_rows = tokens.shape[0]
    a, b = lax.axis_index("mz"), lax.axis_index("mx")
    chain, cols = mp_parts(n)
    model_index = a * cols + b
    model, hidden = w_up.shape
    width = w_out.shape[0]

    def shifted(values, off):
        return lax.ppermute(values, "mx", [(i, (i + off) % cols) for i in range(cols)])

    def pair_sum(partial):
        blocks = jnp.split(partial, cols)
        total = blocks[0].astype(F32)
        for off in range(1, cols):
            total = total + shifted(blocks[off].astype(BF), cols - off).astype(F32)
        return total

    (
        gathered_one, q_ext, k_ext, v_ext, log_totals, attended, owned,
        up_all, down_all, out_all, bias_all, peer_w, self_bias, hidden_one, rows_two, grad_mlp,
    ) = front(
        n,
        image_ids,
        lengths,
        tokens,
        cotangent,
        norm_gain,
        norm_bias,
        out_biases,
        w_qkv,
        bias_query,
        bias_value,
        w_up,
        w_down,
        w_out,
        bias_up,
    )
    grad_out = grad_mlp[0].astype(F32)
    rows_two = rows_two.reshape(cols * share_rows, model)
    grad_mlp = grad_mlp.reshape(cols * share_rows, model)
    owned = jnp.transpose(owned, (1, 0, 2)).reshape(share_rows, -1)
    bias_all = bias_all[:, 0].reshape(-1)
    pre_act = jnp.dot(rows_two, up_all, preferred_element_type=F32) + bias_all
    activated = exact_gelu(pre_act).astype(BF)
    grad_act = jnp.einsum("rd,fd->rf", grad_mlp, down_all, preferred_element_type=F32)
    _, gelu_back = jax.vjp(exact_gelu, pre_act)
    grad_pre = gelu_back(grad_act)[0].astype(BF)
    grad_normed_two = pair_sum(jnp.einsum("rf,df->rd", grad_pre, up_all, preferred_element_type=F32))
    output_full = (
        hidden_one
        + pair_sum(jnp.dot(activated, down_all, preferred_element_type=F32))
        + out_biases[1]
    )
    grad_up_all = jnp.einsum("rf,rd->fd", grad_pre, rows_two, preferred_element_type=F32)
    grad_down_all = jnp.einsum("rf,rd->fd", activated, grad_mlp, preferred_element_type=F32)
    grad_bias_up = jnp.sum(grad_pre, axis=0, dtype=F32)

    _, norm_two_back = jax.vjp(layer_norm, hidden_one, norm_gain[1], norm_bias[1])
    grad_from_two, gain_two, shift_two = norm_two_back(grad_normed_two)
    grad_hidden = grad_out + grad_from_two
    grad_proj = grad_hidden.astype(BF)
    grad_w_out = jnp.einsum("re,rd->ed", owned, grad_proj, preferred_element_type=F32).astype(BF)
    grad_rows = jnp.einsum(
        "rd,ned->nre", grad_proj, out_all.reshape(n, width, model), preferred_element_type=F32
    ).astype(BF)
    bias_rows = lax.dynamic_update_slice(
        jnp.zeros((chain, cols, hidden), F32), grad_bias_up.reshape(chain, 1, hidden), (0, b, 0)
    )
    early = [gain_two, shift_two, jnp.sum(grad_hidden, axis=0), jnp.sum(grad_out, axis=0)]
    early = jnp.concatenate([jnp.stack(early), bias_rows.reshape(-1, model)])
    hidden_sum, head_sum, bias_sum, input_grad, small = rear(
        n,
        grad_rows,
        q_ext,
        k_ext,
        v_ext,
        log_totals,
        self_bias,
        attended,
        w_qkv,
        peer_w,
        gathered_one,
        tokens,
        grad_hidden,
        norm_gain[0],
        early,
        grad_up_all.astype(BF),
        grad_down_all.astype(BF),
        grad_w_out.reshape(n, width, model),
    )
    if groups > 1:
        hidden_sum, head_sum, bias_sum, small = lax.psum((hidden_sum, head_sum, bias_sum, small), "dg")
    half = hidden // PARTS
    grad_w_up = hidden_sum[:, :half].reshape(hidden, model).T.astype(F32)
    grad_w_down = hidden_sum[:, half : 2 * half].reshape(hidden, model).astype(F32)
    grad_w_out = hidden_sum[:, 2 * half :].reshape(width, model).astype(F32)
    grad_w_qkv = jnp.transpose(head_sum.reshape(3, width, model), (0, 2, 1)).astype(F32)
    grad_bias_query, grad_bias_value = bias_sum[:, 0]
    grad_bias_up = lax.dynamic_slice_in_dim(
        small[0, 4:].reshape(-1), model_index * hidden, hidden, 0
    )
    return (
        output_full.astype(BF),
        input_grad,
        grad_w_qkv,
        grad_bias_query,
        grad_bias_value,
        grad_w_out,
        grad_w_up,
        grad_bias_up,
        grad_w_down,
        small[0, 2:4],
        jnp.stack([small[1, 0], small[0, 0]]),
        jnp.stack([small[1, 1], small[0, 1]]),
    )


def solution(mesh):
    n = mesh.shape["mp"]
    chain, cols = mp_parts(n)
    groups = mesh.shape["dp"] // PARTS
    dp, mp = ("dg", "dp"), ("mz", "mx")
    every = dp + mp
    split = jax.sharding.Mesh(mesh.devices.reshape(groups, PARTS, chain, cols), every)
    in_specs = (
        P(every, None),
        P(dp),
        P(dp, None),
        P(None, None, mp),
        P(mp),
        P(mp),
        P(mp, None),
        P(None, mp),
        P(mp),
        P(mp, None),
        P(),
        P(),
        P(),
        P(every, None),
    )
    out_specs = (
        P(every, None),
        P(every, None),
        P(None, None, mp),
        P(mp),
        P(mp),
        P(mp, None),
        P(None, mp),
        P(mp),
        P(mp, None),
        P(),
        P(),
        P(),
    )
    return jax.shard_map(
        functools.partial(body, n, groups),
        mesh=split,
        in_specs=in_specs,
        out_specs=out_specs,
        check_vma=False,
    )
```

```python
import functools
import math
import types

import jax
import jax.numpy as jnp
from jax import lax
from jax.experimental import pallas as pl
from jax.experimental.pallas import tpu as pltpu
from jax.sharding import PartitionSpec as P

HEAD_DIM = 64
LANES = 128
CHUNK = 768
MASKED = -1e30
MESH = pl.DeviceIdType.MESH
VMEM_BYTES = 67_043_328
BF = jnp.bfloat16
F32 = jnp.float32
NN = (((1,), (0,)), ((), ()))
NT = (((1,), (1,)), ((), ()))
TN = (((0,), (0,)), ((), ()))
SCALE = HEAD_DIM ** (-0.5)
PARTS = 4
epsilon = 1e-06


def dot(left, right, dims=NN):
    return lax.dot_general(left, right, dims, preferred_element_type=F32)


def layer_norm(values, gain_vec, shift_vec):
    row_mean = jnp.mean(values, axis=-1, keepdims=True)
    centered = values - row_mean
    variance = jnp.mean(centered * centered, axis=-1, keepdims=True)
    return centered * lax.rsqrt(variance + epsilon) * gain_vec + shift_vec


def gelu_parts(values):
    share = 0.5 + 0.5 * lax.erf(values * math.sqrt(0.5))
    return share, jnp.exp(-0.5 * values * values) * (1 / math.sqrt(2 * math.pi))


def mp_parts(n):
    chain = min(4, n)
    return chain, n // chain


def column_sum(values):
    ones = jnp.ones((8, values.shape[1]), BF)
    high = values.astype(BF)
    low = (values - high.astype(F32)).astype(BF)
    return dot(ones, high, NT) + dot(ones, low, NT)


def split_three(column):
    high = column.astype(BF)
    rest = column - high.astype(F32)
    middle = rest.astype(BF)
    return high, middle, (rest - middle.astype(F32)).astype(BF)


def attend_chunk(c, heads, q_ref, k_ref, v_ref, vt_ref, self_ref, att_ref, lse_ref):
    rows = pl.ds(pl.multiple_of(c * CHUNK, CHUNK), CHUNK)
    pieces = []
    scores = [dot(k_ref[h], q_ref[h, rows, :], NT) for h in range(heads)]
    for h in range(heads):
        own = q_ref[h, rows, :HEAD_DIM].astype(F32) * k_ref[h, rows, :HEAD_DIM].astype(F32)
        own = column_sum(own)[:1] + self_ref[:1, rows]
        top = jnp.maximum(jnp.max(scores[h], axis=0, keepdims=True), own)
        weights = jnp.exp(scores[h] - top).astype(BF)
        own_weight = jnp.exp(own - top).astype(BF).astype(F32)
        summed = dot(vt_ref[h], weights) + vt_ref[h, :, rows].astype(F32) * own_weight
        total = summed[HEAD_DIM : HEAD_DIM + 1]
        pieces.append(summed[:HEAD_DIM] / total)
        lse_ref[h, :, rows] = jnp.broadcast_to(top + jnp.log(total), (8, CHUNK))
    stacked = jnp.concatenate(pieces, axis=0) if heads > 1 else pieces[0]
    att_ref[rows, :] = stacked.T.astype(BF)


def front_kernel(
    n,
    ids_ref,
    lengths_ref,
    tokens_ref,
    cot_ref,
    gain_ref,
    shift_ref,
    out_bias_ref,
    w_ref,
    bias_ref,
    up_ref,
    down_ref,
    out_ref,
    bup_ref,
    normed_ref,
    q_ref,
    k_ref,
    v_ref,
    lse_ref,
    att_ref,
    owned_ref,
    ups_ref,
    downs_ref,
    outs_out,
    bups_ref,
    peers_ref,
    self_ref,
    hidden_ref,
    pair_two,
    pair_cot,
    blocks,
    outs_ref,
    two,
    cot,
    peer_w,
    peer_b,
    proj_out,
    proj_in,
    vt_ref,
    owned,
    ssz,
    rsz,
    ssx,
    rsx,
    spw,
    rpw,
    spb,
    rpb,
    ssa,
    rsa,
    wsz,
    wrz,
    wsx,
    wrx,
    gs,
    gr,
    os,
    orr,
    bs,
    br,
    spp,
    rpp,
    local_sem,
):
    chain, cols = mp_parts(n)
    share, _ = tokens_ref.shape
    width = w_ref.shape[2]
    heads = width // HEAD_DIM
    hidden = up_ref.shape[1]
    up_rows, down_rows, out_rows = (r.shape[0] // PARTS for r in (up_ref, down_ref, out_ref))
    dg, dp = lax.axis_index("dg"), lax.axis_index("dp")
    a, b = lax.axis_index("mz"), lax.axis_index("mx")
    me = a * cols + b
    part = lax.rem(dp, PARTS)
    core_dp = dp + 1 - 2 * lax.rem(dp, 2)
    side_dp = dp + 2 - 4 * lax.rem(dp // 2, 2)
    core_part, side_part = lax.rem(core_dp, PARTS), lax.rem(side_dp, PARTS)
    far_part = PARTS - 1 - part

    barrier = pltpu.get_barrier_semaphore()
    for off in range(1, n):
        other = lax.rem(me + off, n)
        pl.semaphore_signal(
            barrier,
            inc=1,
            device_id=(dg, dp, other // cols, lax.rem(other, cols)),
            device_id_type=MESH,
        )
    for peer in (core_dp, side_dp):
        pl.semaphore_signal(barrier, inc=1, device_id=(dg, peer, a, b), device_id_type=MESH)
    pl.semaphore_wait(barrier, n + 1)

    def remote(src, dst, send, recv, device):
        return pltpu.make_async_remote_copy(
            src_ref=src,
            dst_ref=dst,
            send_sem=send,
            recv_sem=recv,
            device_id=(dg,) + device,
            device_id_type=MESH,
        )

    def span(index, size):
        return pl.ds(pl.multiple_of(index * size, size), size)

    def can(way):
        return (a < chain - 1) if way == 0 else (a > 0)

    def chain_peer(way):
        return (dp, jnp.clip(a + (1 if way == 0 else -1), 0, chain - 1), b)

    def cross_peer(off):
        return (dp, a, lax.rem(b + off, cols))

    def back_peer(off):
        return (dp, a, lax.rem(b - off + cols, cols))

    def chain_copy(row, way):
        spot = blocks.at[row]
        return remote(spot, spot, ssz.at[way, row], rsz.at[way, row], chain_peer(way))

    def cross_copy(row, off):
        return remote(
            proj_out.at[off - 1, row],
            proj_in.at[off - 1, row],
            ssx.at[off, row],
            rsx.at[off, row],
            back_peer(off),
        )

    def peer_copies(off):
        return [
            remote(w_ref, peer_w.at[off - 1], spw.at[off], rpw.at[off], cross_peer(off)),
            remote(bias_ref, peer_b.at[off - 1], spb.at[off], rpb.at[off], cross_peer(off)),
        ]

    def piece(i, row, of_part):
        if i == 0:
            return outs_ref.at[row * cols + b, span(of_part, out_rows)]
        if i == 1:
            return ups_ref.at[span(of_part, up_rows), span(row, hidden)]
        return downs_ref.at[span(row * PARTS + of_part, down_rows)]

    def own_piece(i):
        if i == 0:
            return out_ref.at[span(part, out_rows)]
        if i == 1:
            return up_ref.at[span(part, up_rows)]
        return down_ref.at[span(part, down_rows)]

    def weight_copy(i, row, way, own=False):
        spot = piece(i, row, part)
        sems = wsz.at[i, way, row], wrz.at[i, way, row]
        return remote(own_piece(i) if own else spot, spot, *sems, chain_peer(way))

    def out_cross(block, off, own=False):
        spot = outs_ref.at[block, span(part, out_rows)]
        sems = wsx.at[off, block // cols], wrx.at[off, block // cols]
        return remote(own_piece(0) if own else spot, spot, *sems, cross_peer(off))

    def group_copy(kind, i, row, arriving=False):
        sent = side_part if kind == 2 else part
        got = (side_part, core_part, far_part)[kind]
        spot = piece(i, row, got if arriving else sent)
        sems = gs.at[kind, i - 1, row], gr.at[kind, i - 1, row]
        return remote(spot, spot, *sems, (side_dp if kind == 0 else core_dp, a, b))

    def out_group(kind, arriving=False):
        sent = side_part if kind == 2 else part
        got = (side_part, core_part, far_part)[kind]
        spot = outs_ref.at[:, span(got if arriving else sent, out_rows)]
        return remote(spot, spot, os.at[kind], orr.at[kind], (side_dp if kind == 0 else core_dp, a, b))

    def bias_copy(off, arriving=False):
        spot = bups_ref.at[lax.rem(a - off + chain, chain) if arriving else a]
        return remote(bup_ref, spot, bs.at[off], br.at[off], (dp, lax.rem(a + off, chain), b))

    def start_own(way):
        for i in (1, 2):
            weight_copy(i, a, way, own=True).start()

    stay = [
        pltpu.make_async_copy(up_ref, ups_ref.at[:, span(a, hidden)], local_sem.at[1]),
        pltpu.make_async_copy(down_ref, downs_ref.at[span(a, hidden)], local_sem.at[2]),
        pltpu.make_async_copy(own_piece(0), piece(0, a, part), local_sem.at[3]),
        pltpu.make_async_copy(bup_ref, bups_ref.at[a], local_sem.at[4]),
    ]

    for off in range(1, cols):
        for copy in peer_copies(off):
            copy.start()

    def norm_one(i, _):
        cut = span(i, 16)
        values = layer_norm(tokens_ref[cut, :].astype(F32), gain_ref[:1], shift_ref[:1])
        blocks[a, cut, :] = values.astype(BF)
        return 0

    lax.fori_loop(0, share // 16, norm_one, 0)

    total = n * share
    slot = total // 2
    first_id, last_id = ids_ref[0], ids_ref[total - 1]
    first_length, last_length = (
        jnp.where(k == 0, lengths_ref[0, 0], lengths_ref[0, 1]) for k in (first_id, last_id)
    )
    last_start = jnp.where(first_id == last_id, 0, slot)

    def row_facts(index):
        late = index >= slot
        inside = index - jnp.where(late, last_start, 0) < jnp.where(late, last_length, first_length)
        return jnp.where(late, last_id, first_id), inside

    def place(block, out_q, out_k, out_v):
        rows = span(block, share)
        lane = lax.broadcasted_iota(jnp.int32, (share, LANES - HEAD_DIM), 1)
        image, inside = row_facts(
            block * share + lax.broadcasted_iota(jnp.int32, (share, LANES - HEAD_DIM), 0)
        )
        tail_q = jnp.where(lane == image, 1.0, 0.0).astype(BF)
        hidden_key = jnp.where((lane == image) & inside, 0.0, MASKED)
        tail_k = jnp.where(lane < 2, hidden_key, 0.0).astype(BF)
        tail_v = jnp.where(lane < 3, 1.0, 0.0).astype(BF)
        for h in range(heads):
            cut = slice(h * HEAD_DIM, (h + 1) * HEAD_DIM)
            q_ref[h, rows, :] = jnp.concatenate(
                [out_q[:, cut] * jnp.asarray(SCALE, BF), tail_q], axis=1
            )
            k_ref[h, rows, :] = jnp.concatenate([out_k[:, cut], tail_k], axis=1)
            v_ref[h, rows, :] = jnp.concatenate([out_v[:, cut], tail_v], axis=1)

    def project(row):
        values = blocks[row]
        place(
            row * cols + b,
            (dot(values, w_ref[0]) + bias_ref[0, :1]).astype(BF),
            dot(values, w_ref[1]).astype(BF),
            (dot(values, w_ref[2]) + bias_ref[1, :1]).astype(BF),
        )

    def project_peer(row):
        def one(slot, _):
            values = blocks[row]
            proj_out[slot, row, 0] = (dot(values, peer_w[slot, 0]) + peer_b[slot, 0, :1]).astype(BF)
            proj_out[slot, row, 1] = dot(values, peer_w[slot, 1]).astype(BF)
            proj_out[slot, row, 2] = (dot(values, peer_w[slot, 2]) + peer_b[slot, 1, :1]).astype(BF)
            return 0

        lax.fori_loop(0, cols - 1, one, 0)
        for off in range(1, cols):
            cross_copy(row, off).start()

    for way in (0, 1):

        @pl.when(can(way))
        def _(way=way):
            chain_copy(a, way).start()
            weight_copy(0, a, way, own=True).start()

    def pair_copy(i, off):
        src, dst = ((two, pair_two), (cot, pair_cot))[i]
        return remote(src, dst.at[off], spp.at[i, off], rpp.at[i, off], cross_peer(off))

    pair_stay = [
        pltpu.make_async_copy(two, pair_two.at[0], local_sem.at[6]),
        pltpu.make_async_copy(cot, pair_cot.at[0], local_sem.at[7]),
    ]
    for copy in stay:
        copy.start()

    @pl.when(a == 0)
    def _():
        start_own(0)

    @pl.when(a == chain - 1)
    def _():
        start_own(1)

    project(a)
    _, self_inside = row_facts(lax.broadcasted_iota(jnp.int32, (8, total), 1))
    self_ref[...] = jnp.where(self_inside, MASKED, 0.0)

    def mask_cot(i, _):
        cut = span(i, 16)
        _, inside = row_facts(
            me * share + i * 16 + lax.broadcasted_iota(jnp.int32, (16, cot.shape[1]), 0)
        )
        cot[cut, :] = jnp.where(inside, cot_ref[cut, :].astype(F32), 0.0).astype(BF)
        return 0

    lax.fori_loop(0, share // 16, mask_cot, 0)

    def visit(step, _):
        for way in (0, 1):
            there = a - step if way == 0 else a + step
            inside = (there >= 0) & (there < chain)
            row = jnp.clip(there, 0, chain - 1)

            @pl.when(inside)
            def _(way=way, row=row):
                chain_copy(row, way).wait_recv()

                @pl.when(can(way))
                def _():
                    chain_copy(row, way).start()

                weight_copy(0, row, way).wait_recv()

                @pl.when(can(way))
                def _():
                    weight_copy(0, row, way).start()

        @pl.when((step == a) & can(0))
        def _():
            start_own(0)

        @pl.when((step == chain - 1 - a) & can(1))
        def _():
            start_own(1)

        @pl.when(step == 1)
        def _():
            for off in range(1, cols):
                for copy in peer_copies(off):
                    copy.wait_recv()

        def one(j, _):
            gone = step - jnp.where(j == 0, 1, 0)
            there = jnp.where(j == 1, a - gone, a + gone)

            @pl.when((there >= 0) & (there < chain) & ((j > 0) | (step == 1)))
            def _():
                @pl.when(j > 0)
                def _():
                    project(there)

                project_peer(there)

            return 0

        lax.fori_loop(0, 3, one, 0)
        return 0

    lax.fori_loop(1, chain, visit, 0)

    stay[2].wait()
    for off in range(1, cols):
        out_cross(me, off, own=True).start()

    def out_send(i, _):
        row = lax.rem(a + i, chain)
        for off in range(1, cols):
            out_cross(row * cols + b, off).start()
        return 0

    lax.fori_loop(1, chain, out_send, 0)

    def receive(i, _):
        row = lax.rem(a + i, chain)
        for off in range(1, cols):
            cross_copy(row, off).wait_recv()
            block = row * cols + lax.rem(b + off, cols)
            place(block, *[proj_in[off - 1, row, t] for t in range(3)])
        return 0

    lax.fori_loop(0, chain, receive, 0)
    keep = pltpu.make_async_copy(blocks, normed_ref, local_sem.at[0])
    keep.start()
    keep_peers = pltpu.make_async_copy(peer_w, peers_ref, local_sem.at[5])
    keep_peers.start()

    def gather_out(row, _):
        for off in range(1, cols):
            out_cross(row * cols + lax.rem(b - off + cols, cols), off).wait_recv()
        return 0

    lax.fori_loop(0, chain, gather_out, 0)
    out_group(0).start()
    out_group(1).start()
    for off in range(1, chain):
        bias_copy(off).start()

    def both_ways(step, act):
        for way in (0, 1):
            there = a - step if way == 0 else a + step

            @pl.when((there >= 0) & (there < chain))
            def _(way=way, there=there):
                act(way, jnp.clip(there, 0, chain - 1))

    def weights_pass(way, row):
        for i in (1, 2):
            weight_copy(i, row, way).wait_recv()

            @pl.when(can(way))
            def _(i=i):
                weight_copy(i, row, way).start()

            group_copy(0, i, row).start()
            group_copy(1, i, row).start()

    def weights_side(way, row):
        for i in (1, 2):
            group_copy(0, i, row, arriving=True).wait_recv()
            group_copy(2, i, row).start()

    both_ways(1, weights_pass)

    def flip(c, _):
        rows = span(c, CHUNK)
        for h in range(heads):
            vt_ref[h, :, rows] = v_ref[h, rows, :].astype(F32).T.astype(BF)
        return 0

    lax.fori_loop(0, n * share // CHUNK, flip, 0)

    def own_copy(target, source):
        return remote(
            att_ref.at[span(target, share)],
            owned.at[source],
            ssa.at[target],
            rsa.at[source],
            (dp, target // cols, lax.rem(target, cols)),
        )

    def attend(c, _):
        attend_chunk(c, heads, q_ref, k_ref, v_ref, vt_ref, self_ref, att_ref, lse_ref)

        def send(target, _):
            end = (target + 1) * share

            @pl.when((end <= (c + 1) * CHUNK) & (end > c * CHUNK) & (target != me))
            def _():
                own_copy(target, me).start()

            return 0

        lax.fori_loop(0, n, send, 0)

        @pl.when(c == 0)
        def _():
            out_group(0, arriving=True).wait_recv()
            out_group(2).start()

        @pl.when(c > 0)
        def _():
            both_ways(c + 1, weights_pass)
            both_ways(c, weights_side)

        return 0

    lax.fori_loop(0, n * share // CHUNK, attend, 0)
    owned[me] = att_ref[span(me, share), :]
    for off in range(1, cols):
        pair_copy(1, off).start()
    pair_stay[1].start()
    for kind in (1, 2):
        out_group(kind, arriving=True).wait_recv()
    keep_out = pltpu.make_async_copy(outs_ref, outs_out, local_sem.at[3])
    keep_out.start()

    def collect(other, _):
        @pl.when(other != me)
        def _():
            own_copy(other, me).wait_send()
            own_copy(me, other).wait_recv()

        return 0

    lax.fori_loop(0, n, collect, 0)
    hidden_ref[...] = tokens_ref[...].astype(F32) + out_bias_ref[:1]

    def out_project(m, _):
        hidden_ref[...] += dot(owned[m], outs_ref[m])
        return 0

    lax.fori_loop(0, n, out_project, 0)

    def norm_two(i, _):
        cut = span(i, 16)
        two[cut, :] = layer_norm(hidden_ref[cut, :], gain_ref[1:], shift_ref[1:]).astype(BF)
        return 0

    lax.fori_loop(0, share // 16, norm_two, 0)
    for off in range(1, cols):
        pair_copy(0, off).start()
    pair_stay[0].start()
    both_ways(chain - 1, weights_side)
    owned_ref[...] = owned[...]
    for off in range(1, cols):
        for i in (0, 1):
            pair_copy(i, off).wait_send()
            pair_copy(i, off).wait_recv()
    for copy in pair_stay:
        copy.wait()
    keep_out.wait()
    keep.wait()
    keep_peers.wait()
    for off in range(1, cols):
        for copy in peer_copies(off):
            copy.wait_send()
    for i in (0, 1, 3):
        stay[i].wait()
    for off in range(1, chain):
        bias_copy(off).wait_send()
        bias_copy(off, arriving=True).wait_recv()
    for kind in range(3):
        out_group(kind).wait_send()

    def drain(row, _):
        for off in range(1, cols):
            cross_copy(row, off).wait_send()
            out_cross(row * cols + b, off).wait_send()

        @pl.when((row <= a) & (a < chain - 1))
        def _():
            chain_copy(row, 0).wait_send()
            for i in range(3):
                weight_copy(i, row, 0).wait_send()

        @pl.when((row >= a) & (a > 0))
        def _():
            chain_copy(row, 1).wait_send()
            for i in range(3):
                weight_copy(i, row, 1).wait_send()

        @pl.when(row != a)
        def _():
            for i in (1, 2):
                for kind in range(3):
                    group_copy(kind, i, row).wait_send()
                    if kind > 0:
                        group_copy(kind, i, row, arriving=True).wait_recv()

        return 0

    lax.fori_loop(0, chain, drain, 0)


def front(
    n, image_ids, lengths, tokens, cotangent, gain, shift, out_biases, w_qkv, bias_query, bias_value, w_up, w_down,
    w_out, bias_up,
):
    chain, cols = mp_parts(n)
    share, model = tokens.shape
    width = w_qkv.shape[2]
    heads = width // HEAD_DIM
    hidden = w_up.shape[1]
    rows = n * share
    vmem = pl.BlockSpec(memory_space=pltpu.VMEM)
    anywhere = pl.BlockSpec(memory_space=pl.ANY)
    ext = jax.ShapeDtypeStruct((heads, rows, LANES), BF)
    dma = pltpu.SemaphoreType.DMA
    return pl.pallas_call(
        functools.partial(front_kernel, n),
        name="front",
        out_shape=(
            jax.ShapeDtypeStruct((chain, share, model), BF),
            ext,
            ext,
            ext,
            jax.ShapeDtypeStruct((heads, 8, rows), F32),
            jax.ShapeDtypeStruct((rows, width), BF),
            jax.ShapeDtypeStruct((n, share, width), BF),
            jax.ShapeDtypeStruct((model, chain * hidden), BF),
            jax.ShapeDtypeStruct((chain * hidden, model), BF),
            jax.ShapeDtypeStruct((n, width, model), BF),
            jax.ShapeDtypeStruct((chain, 8, hidden), F32),
            jax.ShapeDtypeStruct((cols - 1,) + w_qkv.shape, BF),
            jax.ShapeDtypeStruct((8, rows), F32),
            jax.ShapeDtypeStruct((share, model), F32),
            jax.ShapeDtypeStruct((cols, share, model), BF),
            jax.ShapeDtypeStruct((cols, share, model), BF),
        ),
        in_specs=[pl.BlockSpec(memory_space=pltpu.SMEM)] * 2 + [vmem] * 11,
        out_specs=(anywhere,) + (vmem,) * 6 + (anywhere,) * 5 + (vmem,) * 2 + (anywhere,) * 2,
        scratch_shapes=[
            pltpu.VMEM((chain, share, model), BF),
            pltpu.VMEM((n, width, model), BF),
            pltpu.VMEM((share, model), BF),
            pltpu.VMEM((share, model), BF),
            pltpu.VMEM((cols - 1,) + w_qkv.shape, BF),
            pltpu.VMEM((cols - 1, 2, 8, width), F32),
            pltpu.VMEM((cols - 1, chain, 3, share, width), BF),
            pltpu.VMEM((cols - 1, chain, 3, share, width), BF),
            pltpu.VMEM((heads, LANES, rows), BF),
            pltpu.VMEM((n, share, width), BF),
            dma((2, chain)),
            dma((2, chain)),
            dma((cols, chain)),
            dma((cols, chain)),
            dma((cols,)),
            dma((cols,)),
            dma((cols,)),
            dma((cols,)),
            dma((n,)),
            dma((n,)),
            dma((3, 2, chain)),
            dma((3, 2, chain)),
            dma((cols, chain)),
            dma((cols, chain)),
            dma((3, 2, chain)),
            dma((3, 2, chain)),
            dma((3,)),
            dma((3,)),
            dma((chain,)),
            dma((chain,)),
            dma((2, cols)),
            dma((2, cols)),
            dma((8,)),
        ],
        compiler_params=pltpu.CompilerParams(
            collective_id=0, has_side_effects=True, vmem_limit_bytes=VMEM_BYTES
        ),
    )(
        image_ids,
        lengths,
        tokens,
        cotangent,
        gain,
        shift,
        out_biases,
        w_qkv,
        jnp.broadcast_to(jnp.stack([bias_query, bias_value])[:, None, :], (2, 8, width)),
        w_up,
        w_down,
        w_out,
        jnp.broadcast_to(bias_up[None, :], (8, hidden)),
    )


def attend_back_chunk(
    c, heads, q_ref, k_ref, v_ref, kt_ref, lse_ref, self_ref, att_ref, grad_ref, gq_ref, dk_ref, dv_ref
):
    rows = pl.ds(pl.multiple_of(c * CHUNK, CHUNK), CHUNK)
    grads = grad_ref[rows, :].astype(F32)
    products = grads * att_ref[rows, :].astype(F32)
    outs = []
    for h in range(heads):
        cut = slice(h * HEAD_DIM, (h + 1) * HEAD_DIM)
        inner = jnp.sum(products[:, cut], axis=1, keepdims=True)
        parts = split_three(-inner)
        lane = lax.broadcasted_iota(jnp.int32, (CHUNK, LANES - HEAD_DIM), 1)
        tail = jnp.zeros((CHUNK, LANES - HEAD_DIM), F32)
        for i, part in enumerate(parts):
            tail = jnp.where(lane == i, part.astype(F32), tail)
        grad_ext = jnp.concatenate([grads[:, cut], tail], axis=1).astype(BF)
        query = q_ref[h, rows, :]
        key_own = k_ref[h, rows, :]
        scores = dot(k_ref[h], query, NT)
        lse = lse_ref[h, :1, rows]
        probs = jnp.exp(scores - lse)
        shifted = dot(v_ref[h], grad_ext, NT)
        own = column_sum(query[:, :HEAD_DIM].astype(F32) * key_own[:, :HEAD_DIM].astype(F32))
        own_prob = jnp.exp(own + self_ref[:, rows] - lse)
        own_shifted = column_sum(v_ref[h, rows, :].astype(F32) * grad_ext.astype(F32))
        lower = lax.broadcasted_iota(jnp.int32, (8, CHUNK), 0) < 4
        both = jnp.where(lower, own_prob, own_prob * own_shifted).T
        own_prob, own_score = both[:, :1], both[:, 4:5]
        grad_scores = (probs * shifted).astype(BF)
        dv = dot(probs.astype(BF), grad_ext)
        dk = dot(grad_scores, query)
        dq = dot(kt_ref[h], grad_scores).T
        dq = (dq + own_score * key_own.astype(F32)) * SCALE
        outs.append(dq[:, :HEAD_DIM])

        @pl.when(c == 0)
        def _(h=h, dv=dv, dk=dk):
            dv_ref[h] = dv
            dk_ref[h] = dk

        @pl.when(c > 0)
        def _(h=h, dv=dv, dk=dk):
            dv_ref[h] += dv
            dk_ref[h] += dk

        dv_ref[h, rows, :] += own_prob * grad_ext.astype(F32)
        dk_ref[h, rows, :] += own_score * query.astype(F32)
    stacked = jnp.concatenate(outs, axis=1) if heads > 1 else outs[0]
    gq_ref[rows, :] = stacked.astype(BF)


REAR_REFS = (
    "gatt",
    "q",
    "k",
    "v",
    "lse",
    "self_bias",
    "att",
    "w",
    "peer_w",
    "normed",
    "tokens",
    "grad_hidden",
    "gain",
    "early",
    "up",
    "down",
    "out",
    "up_sum",
    "down_sum",
    "out_sum",
    "head_sum",
    "bias_out",
    "input_grad",
    "small_out",
    "grad",
    "kt",
    "dk",
    "dv",
    "gq",
    "gk",
    "gv",
    "kept",
    "pool_core",
    "pool_side",
    "way_in",
    "out_in",
    "local_in",
    "local_side",
    "acc",
    "peer_in",
    "peer_got",
    "way_gn",
    "gn",
    "small",
    "small_in",
    "bias_sum",
    "bias_in",
    "sa",
    "ra",
    "so",
    "ro",
    "sc",
    "rc",
    "sk",
    "ss",
    "rs",
    "sz",
    "rz",
    "sg",
    "rg",
    "st",
    "rt",
    "sy",
    "ry",
    "sh",
    "rh",
    "sx",
    "rx",
    "sw",
    "rw",
    "sn",
    "rn",
    "sm",
    "rm",
    "sb",
    "rb",
    "sl",
)


def rear_kernel(n, *refs):
    r = types.SimpleNamespace(**dict(zip(REAR_REFS, refs)))
    chain, cols = mp_parts(n)
    heads, total, _ = r.q.shape
    _, share, width = r.gatt.shape
    model = r.w.shape[1]
    hidden = r.up.shape[0] // chain
    rows, out_rows = hidden // PARTS, width // PARTS
    block_rows = 2 * rows + cols * out_rows
    local_rows = 3 * width // PARTS
    head_base = (cols - 1) * 3 * width
    done_base = head_base + 3 * width
    local = r.pool_core.at[pl.ds(head_base, 3 * width)]
    done = r.pool_core.at[pl.ds(done_base, block_rows)]
    local_done = r.pool_core.at[pl.ds(done_base + block_rows, local_rows)]
    dg, dp = lax.axis_index("dg"), lax.axis_index("dp")
    a, b = lax.axis_index("mz"), lax.axis_index("mx")
    me = a * cols + b
    part = lax.rem(dp, PARTS)
    core_dp = dp + 1 - 2 * lax.rem(dp, 2)
    side_dp = dp + 2 - 4 * lax.rem(dp // 2, 2)
    core_part, side_part = lax.rem(core_dp, PARTS), lax.rem(side_dp, PARTS)
    far_part = PARTS - 1 - part
    core_id, side_id = (core_dp, a, b), (side_dp, a, b)
    far_id = (PARTS - 1 - dp, a, b)

    def mp_id(index):
        return dp, index // cols, lax.rem(index, cols)

    barrier = pltpu.get_barrier_semaphore()
    for off in range(1, n):
        pl.semaphore_signal(
            barrier, inc=1, device_id=(dg,) + mp_id(lax.rem(me + off, n)), device_id_type=MESH
        )
    for peer in (core_id, side_id, far_id):
        pl.semaphore_signal(barrier, inc=1, device_id=(dg,) + peer, device_id_type=MESH)
    pl.semaphore_wait(barrier, n + 2)

    def remote(src, dst, send, recv, device):
        return pltpu.make_async_remote_copy(
            src_ref=src,
            dst_ref=dst,
            send_sem=send,
            recv_sem=recv,
            device_id=(dg,) + device,
            device_id_type=MESH,
        )

    def span(index, size):
        return pl.ds(pl.multiple_of(index * size, size), size)

    def in_order(i):
        low = jnp.where(chain - 1 - i > a, chain - 1 - i, chain - 2 - i)
        high = jnp.where(i < a, i, i + 1)
        return jnp.where(i == chain - 1, a, jnp.where(2 * a < chain, low, high))

    def add_rows(dst, *terms):
        count = dst.shape[0]
        step = 32 if count % 32 == 0 else 16

        def one(i, _):
            cut = span(i, step)
            value = terms[0][cut, :].astype(F32)
            for term in terms[1:]:
                value = value + term[cut, :].astype(F32)
            dst[cut, :] = value.astype(dst.dtype)
            return 0

        lax.fori_loop(0, count // step, one, 0)

    def loop(count, act):
        def one(i, _):
            act(i)
            return 0

        lax.fori_loop(0, count, one, 0)

    def others(act):
        def one(m):
            @pl.when(m != me)
            def _():
                act(m)

        loop(n, one)

    def row_copy(target, source):
        return remote(
            r.gatt.at[target], r.grad.at[span(source, share)], r.sa.at[target], r.ra.at[source], mp_id(target)
        )

    def source_rows(i, t, which):
        if i < 2:
            return (r.up, r.down)[i].at[span(t * PARTS + which, rows)]
        return r.out.at[t * cols + lax.rem(b + i - 2, cols), span(which, out_rows)]

    def offset(i):
        return i * rows if i < 2 else 2 * rows + (i - 2) * out_rows

    def core_copy(t, slot, i):
        src = source_rows(i, t, far_part if slot else core_part)
        base = pl.multiple_of((t * 2 + slot) * block_rows + offset(i), 16)
        return remote(
            src, r.pool_core.at[pl.ds(base, src.shape[0])], r.sc.at[t, slot, i], r.rc.at[t, slot, i], core_id
        )

    def keep_copy(t, slot, i):
        src = source_rows(i, t, side_part if slot else part)
        return pltpu.make_async_copy(
            src, r.kept.at[t, slot, pl.ds(offset(i), src.shape[0])], r.sk.at[t, slot, i]
        )

    def side_copy(t):
        return remote(r.kept.at[t, 1], r.pool_side.at[span(t, block_rows)], r.ss.at[t], r.rs.at[t], side_id)

    def chain_id(way):
        return dp, jnp.clip(a + (1 if way == 0 else -1), 0, chain - 1), b

    def hop_of(way):
        return a if way == 0 else chain - 1 - a

    def ahead(way, t):
        return (t > a) if way == 0 else (t < a)

    def chain_copy(flow, way, t, fresh=False):
        own, inbox, send, recv = flow
        spot = inbox.at[way, t]
        return remote(own(t) if fresh else spot, spot, send.at[way, t], recv.at[way, t], chain_id(way))

    def chain_service(flow, s, prepare):
        own, inbox = flow[:2]
        for way in (0, 1):
            hop = hop_of(way)
            t = chain - 1 + a - s if way == 0 else s - hop
            active = (t > a) & (t < chain) if way == 0 else (t >= 0) & (t < a)
            spot = jnp.clip(t, 0, chain - 1)

            @pl.when(active)
            def _(way=way, t=spot):
                prepare(t)

            @pl.when(active & (hop == 0))
            def _(way=way, t=spot):
                chain_copy(flow, way, t, fresh=True).start()

            @pl.when(active & (hop > 0))
            def _(way=way, t=spot):
                chain_copy(flow, way, t).wait_recv()
                add_rows(inbox.at[way, t], inbox.at[way, t], own(t))
                chain_copy(flow, way, t).start()

    def chain_finish(flow, dst, prepare):
        own, inbox = flow[:2]
        prepare(a)

        @pl.when(a > 0)
        def _():
            chain_copy(flow, 0, a).wait_recv()

        @pl.when(a < chain - 1)
        def _():
            chain_copy(flow, 1, a).wait_recv()

        @pl.when((a > 0) & (a < chain - 1))
        def _():
            add_rows(dst, own(a), inbox.at[0, a], inbox.at[1, a])

        @pl.when(a == 0)
        def _():
            add_rows(dst, own(a), inbox.at[1, a])

        @pl.when(a == chain - 1)
        def _():
            add_rows(dst, own(a), inbox.at[0, a])

    def chain_drain(flow):
        def one(t):
            for way in (0, 1):

                @pl.when(ahead(way, t))
                def _(way=way):
                    chain_copy(flow, way, t).wait_send()

        loop(chain, one)

    def share_copy(share_flow, kind, arriving=False):
        own, everyone, send, recv = share_flow
        sent = side_part if kind == 2 else part
        got = (side_part, core_part, far_part)[kind]
        spot = everyone.at[got if arriving else sent]
        src = spot if kind == 2 or arriving else own
        return remote(src, spot, send.at[kind], recv.at[kind], side_id if kind == 0 else core_id)

    weights = (lambda t: r.kept.at[t, 0], r.way_in, r.sz, r.rz)
    grads = (lambda t: r.pool_side.at[span(t, share)], r.way_gn, r.sn, r.rn)
    share_weights = [
        (done.at[pl.ds(0, rows)], r.up_sum, r.sg.at[0], r.rg.at[0]),
        (done.at[pl.ds(rows, rows)], r.down_sum, r.sg.at[1], r.rg.at[1]),
        (done.at[pl.ds(2 * rows, out_rows)], r.out_sum, r.sg.at[2], r.rg.at[2]),
    ]
    share_local = (local_done, r.head_sum, r.sh, r.rh)

    def small_peers(stage):
        if stage == 0:
            return [core_id, side_id, far_id]
        if stage == 1:
            return [(dp, a, lax.rem(b + off, cols)) for off in range(1, cols)]
        return [(dp, lax.rem(a + off, chain), b) for off in range(1, chain)]

    def small_copies(which, stage):
        src = r.early if which == 0 and stage == 0 else r.small.at[which, stage]
        return [
            remote(src, r.small_in.at[which, stage, i], r.sm.at[which, stage, i], r.rm.at[which, stage, i], peer)
            for i, peer in enumerate(small_peers(stage))
        ]

    def small_start(which, stage):
        for copy in small_copies(which, stage):
            copy.start()

    def small_sum(which, stage):
        value = r.early[...] if which == 0 and stage == 0 else r.small[which, stage]
        for i, copy in enumerate(small_copies(which, stage)):
            copy.wait_recv()
            value = value + r.small_in[which, stage, i]
        if stage < 2:
            r.small[which, stage + 1] = value
            small_start(which, stage + 1)
        else:
            r.small_out[which] = value

    def bias_copy(stage):
        return remote(
            r.bias_sum.at[stage], r.bias_in.at[stage], r.sb.at[stage], r.rb.at[stage], (core_id, side_id)[stage]
        )

    others(lambda m: row_copy(m, me).start())
    small_start(0, 0)

    def start_core(i):
        t = in_order(i)
        for slot in (1, 0):
            for k in range(2 + cols):
                core_copy(t, slot, k).start()
                keep_copy(t, slot, k).start()

    loop(chain, start_core)
    r.grad[span(me, share), :] = r.gatt[me]

    def flip(c):
        cut = span(c, CHUNK)
        for h in range(heads):
            r.kt[h, :, cut] = r.k[h, cut, :].astype(F32).T.astype(BF)

    loop(total // CHUNK, flip)

    def core_sum(i):
        t = in_order(i)
        for slot in (1, 0):
            for k in range(2 + cols):
                keep_copy(t, slot, k).wait()
                core_copy(t, slot, k).wait_recv()
            add_rows(r.kept.at[t, slot], r.kept.at[t, slot], r.pool_core.at[span(t * 2 + slot, block_rows)])
            if slot == 1:
                side_copy(t).start()

    loop(chain, core_sum)
    others(lambda m: row_copy(me, m).wait_recv())

    def side_sum(t):
        side_copy(t).wait_recv()
        add_rows(r.kept.at[t, 0], r.kept.at[t, 0], r.pool_side.at[span(t, block_rows)])

    def cross_copy(k, lag, t):
        return remote(
            (r.gq, r.gk, r.gv)[k].at[span(t * cols + lax.rem(b + lag, cols), share)],
            r.peer_in.at[lag - 1, k, t],
            r.sx.at[k, lag, t],
            r.rx.at[k, lag, t],
            (dp, a, lax.rem(b + lag, cols)),
        )

    chain_service(weights, 0, side_sum)

    def attend(c):
        attend_back_chunk(
            c, heads, r.q, r.k, r.v, r.kt, r.lse, r.self_bias, r.att, r.grad, r.gq, r.dk, r.dv
        )

        def send(t):
            for lag in range(1, cols):
                end = (t * cols + lax.rem(b + lag, cols) + 1) * share

                @pl.when((end <= (c + 1) * CHUNK) & (end > c * CHUNK))
                def _(lag=lag):
                    cross_copy(0, lag, t).start()

        loop(chain, send)

        @pl.when(c < chain - 2)
        def _():
            chain_service(weights, c + 1, side_sum)


    loop(total // CHUNK, attend)

    def finish(c):
        cut = span(c, CHUNK)
        for src, dst in ((r.dk, r.gk), (r.dv, r.gv)):
            parts = [src[h, cut, :HEAD_DIM] for h in range(heads)]
            dst[cut, :] = (jnp.concatenate(parts, axis=1) if heads > 1 else parts[0]).astype(BF)

    loop(total // CHUNK, finish)

    def send_rest(i):
        for k in (1, 2):
            for lag in range(1, cols):
                cross_copy(k, lag, in_order(i)).start()

    loop(chain, send_rest)
    def out_copy(lag):
        return remote(
            done.at[pl.ds(offset(2 + lag), out_rows)],
            r.out_in.at[lag - 1],
            r.so.at[lag],
            r.ro.at[lag],
            (dp, a, lax.rem(b + lag, cols)),
        )

    chain_finish(weights, done, side_sum)
    for lag in range(1, cols):
        out_copy(lag).start()

    small_sum(0, 0)

    def partial_rows(t):
        cut = span(t * cols + b, share)
        value = dot(r.gq[cut, :], r.w[0], NT) + dot(r.gk[cut, :], r.w[1], NT)
        value = value + dot(r.gv[cut, :], r.w[2], NT)
        for slot in range(cols - 1):
            for k in range(3):
                value = value + dot(r.peer_in[slot, k, t], r.peer_w[slot, k], NT)
        return value.astype(BF)

    def bias_rows(c):
        ones = jnp.ones((8, CHUNK), BF)
        for t, src in ((0, r.gq), (1, r.gv)):
            value = dot(ones, src[span(c, CHUNK), :])

            @pl.when(c == 0)
            def _(t=t, value=value):
                r.bias_sum[0, t] = value

            @pl.when(c > 0)
            def _(t=t, value=value):
                r.bias_sum[0, t] += value

    loop(total // CHUNK, bias_rows)
    bias_copy(0).start()

    def head_grads(rows_of):
        def one(t):
            for k in range(3):
                value = dot(rows_of(k, t), r.normed[t], TN)

                @pl.when(t == 0)
                def _(k=k, value=value):
                    r.acc[k] = value

                @pl.when(t > 0)
                def _(k=k, value=value):
                    r.acc[k] += value

        loop(chain, one)

    def head_copy(off):
        return remote(
            r.pool_core.at[pl.ds((off - 1) * 3 * width, 3 * width)],
            r.peer_got.at[off - 1],
            r.sw.at[off],
            r.rw.at[off],
            (dp, a, lax.rem(b - off + cols, cols)),
        )

    def cross_wait(t):
        for k in range(3):
            for lag in range(1, cols):
                cross_copy(k, lag, t).wait_recv()

    def cross_sum(t):
        own = grads[0](t)
        own[...] = partial_rows(t)

    def first_sum(t):
        cross_wait(t)
        cross_sum(t)

    def wait_rest(i):
        @pl.when((i > 0) | ((a > 0) & (a < chain - 1)))
        def _():
            cross_wait(in_order(i))

    chain_service(grads, 0, first_sum)
    for lag in range(1, cols):
        out_copy(lag).wait_recv()
    spot = done.at[pl.ds(offset(2), out_rows)]
    add_rows(spot, spot, *[r.out_in.at[lag - 1] for lag in range(1, cols)])
    weights_keep = []
    for i, flow in enumerate(share_weights):
        for kind in (0, 1):
            share_copy(flow, kind).start()
        weights_keep.append(pltpu.make_async_copy(flow[0], flow[1].at[part], r.sl.at[i]))
        weights_keep[i].start()
    loop(chain, wait_rest)
    chain_service(grads, 1, cross_sum)
    for off in range(1, cols):
        head_grads(lambda k, t: r.peer_in[off - 1, k, t])
        for k in range(3):
            r.pool_core[pl.ds(((off - 1) * 3 + k) * width, width), :] = r.acc[k].astype(BF)
        head_copy(off).start()
    head_grads(lambda k, t: (r.gq, r.gk, r.gv)[k][span(t * cols + b, share), :])
    def later(s, _):
        chain_service(grads, s, cross_sum)
        return 0

    lax.fori_loop(2, chain - 1, later, 0)
    for k in range(3):
        total_k = r.acc[k]
        for off in range(1, cols):
            if k == 0:
                head_copy(off).wait_recv()
            total_k = total_k + r.peer_got[off - 1, pl.ds(k * width, width)].astype(F32)
        local[span(k, width), :] = total_k.astype(BF)

    def local_core(slot):
        return remote(
            local.at[span(far_part if slot else core_part, local_rows)], r.local_in.at[slot], r.st.at[slot], r.rt.at[slot], core_id
        )

    local_side = remote(local.at[span(side_part, local_rows)], r.local_side, r.sy.at[0], r.ry.at[0], side_id)
    for slot in (1, 0):
        local_core(slot).start()
    small_sum(0, 1)
    for slot in (1, 0):
        local_core(slot).wait_recv()
        spot = local.at[span(side_part if slot else part, local_rows)]
        add_rows(spot, spot, r.local_in.at[slot])
        if slot == 1:
            local_side.start()
    bias_copy(0).wait_recv()
    r.bias_sum[1] = r.bias_sum[0] + r.bias_in[0]
    bias_copy(1).start()
    for flow in share_weights:
        share_copy(flow, 0, arriving=True).wait_recv()
        share_copy(flow, 2).start()
    local_side.wait_recv()
    bias_copy(1).wait_recv()
    r.bias_out[...] = r.bias_sum[1] + r.bias_in[1]
    add_rows(local_done, local.at[span(part, local_rows)], r.local_side)
    for kind in (0, 1):
        share_copy(share_local, kind).start()
    local_keep = pltpu.make_async_copy(local_done, r.head_sum.at[part], r.sl.at[3])
    local_keep.start()
    chain_finish(grads, r.gn, cross_sum)
    step = 32 if share % 32 == 0 else 16

    def norm_back(i, sums):
        cut = span(i, step)
        values = r.tokens[cut, :].astype(F32)
        grad = r.gn[cut, :]
        centered = values - jnp.mean(values, axis=-1, keepdims=True)
        scale = lax.rsqrt(jnp.mean(centered * centered, axis=-1, keepdims=True) + epsilon)
        unit = centered * scale
        scaled = grad * r.gain[...]
        along = jnp.mean(scaled * unit, axis=-1, keepdims=True)
        back = (scaled - jnp.mean(scaled, axis=-1, keepdims=True) - unit * along) * scale
        r.input_grad[cut, :] = (r.grad_hidden[cut, :] + back).astype(BF)
        gains = jnp.sum(grad * unit, axis=0, keepdims=True)
        return sums[0] + gains, sums[1] + jnp.sum(grad, axis=0, keepdims=True)

    zero = jnp.zeros((1, model), F32)
    gains, shifts = lax.fori_loop(0, share // step, norm_back, (zero, zero))
    upper = lax.broadcasted_iota(jnp.int32, (8, model), 0) == 0
    r.small[1, 0] = jnp.where(upper, gains, shifts)
    small_start(1, 0)
    small_sum(0, 2)
    share_copy(share_local, 0, arriving=True).wait_recv()
    share_copy(share_local, 2).start()
    for stage in range(3):
        small_sum(1, stage)

    for copy in weights_keep:
        copy.wait()
    local_keep.wait()
    for flow in share_weights + [share_local]:
        for kind in range(3):
            share_copy(flow, kind).wait_send()
            if kind > 0:
                share_copy(flow, kind, arriving=True).wait_recv()
    for slot in (1, 0):
        local_core(slot).wait_send()
    local_side.wait_send()
    for off in range(1, cols):
        head_copy(off).wait_send()
        out_copy(off).wait_send()
    for stage in range(2):
        bias_copy(stage).wait_send()
    for which in range(2):
        for stage in range(3):
            for copy in small_copies(which, stage):
                copy.wait_send()
    others(lambda m: row_copy(m, me).wait_send())
    chain_drain(weights)
    chain_drain(grads)

    def drain(t):
        side_copy(t).wait_send()
        for slot in (1, 0):
            for k in range(2 + cols):
                core_copy(t, slot, k).wait_send()
        for lag in range(1, cols):
            for k in range(3):
                cross_copy(k, lag, t).wait_send()

    loop(chain, drain)


def rear(
    n, grad_rows, q_ext, k_ext, v_ext, lse, self_bias, attended, w_qkv, peer_w, normed, tokens, grad_hidden, gain,
    early, grad_up, grad_down, grad_out,
):
    chain, cols = mp_parts(n)
    heads, total, _ = q_ext.shape
    _, share, width = grad_rows.shape
    model = w_qkv.shape[1]
    rows = 2 * (grad_up.shape[0] // chain // PARTS)
    block = rows + cols * width // PARTS
    local = 3 * width // PARTS
    vmem = pl.BlockSpec(memory_space=pltpu.VMEM)
    anywhere = pl.BlockSpec(memory_space=pl.ANY)
    dma = pltpu.SemaphoreType.DMA
    head = pltpu.VMEM((total, width), BF)
    most = max(chain, cols, PARTS) - 1
    return pl.pallas_call(
        functools.partial(rear_kernel, n),
        name="rear",
        out_shape=(
            jax.ShapeDtypeStruct((PARTS, rows // 2, model), BF),
            jax.ShapeDtypeStruct((PARTS, rows // 2, model), BF),
            jax.ShapeDtypeStruct((PARTS, width // PARTS, model), BF),
            jax.ShapeDtypeStruct((PARTS, local, model), BF),
            jax.ShapeDtypeStruct((2, 8, width), F32),
            jax.ShapeDtypeStruct((share, model), BF),
            jax.ShapeDtypeStruct((2, 8, model), F32),
        ),
        in_specs=[vmem] * 14 + [anywhere] * 3,
        out_specs=(anywhere,) * 4 + (vmem,) * 3,
        scratch_shapes=[
            head,
            pltpu.VMEM((heads, LANES, total), BF),
            pltpu.VMEM((heads, total, LANES), F32),
            pltpu.VMEM((heads, total, LANES), F32),
            head,
            head,
            head,
            pltpu.VMEM((chain, 2, block, model), BF),
            pltpu.VMEM((chain * 2 * block, model), BF),
            pltpu.VMEM((chain * max(block, share), model), BF),
            pltpu.VMEM((2, chain, block, model), BF),
            pltpu.VMEM((cols - 1, width // PARTS, model), BF),
            pltpu.VMEM((2, local, model), BF),
            pltpu.VMEM((local, model), BF),
            pltpu.VMEM((3, width, model), F32),
            pltpu.VMEM((cols - 1, 3, chain, share, width), BF),
            pltpu.VMEM((cols - 1, 3 * width, model), BF),
            pltpu.VMEM((2, chain, share, model), BF),
            pltpu.VMEM((share, model), F32),
            pltpu.VMEM((2, 3, 8, model), F32),
            pltpu.VMEM((2, 3, most, 8, model), F32),
            pltpu.VMEM((2, 2, 8, width), F32),
            pltpu.VMEM((2, 2, 8, width), F32),
            dma((n,)),
            dma((n,)),
            dma((cols,)),
            dma((cols,)),
            dma((chain, 2, 2 + cols)),
            dma((chain, 2, 2 + cols)),
            dma((chain, 2, 2 + cols)),
            dma((chain,)),
            dma((chain,)),
            dma((2, chain)),
            dma((2, chain)),
            dma((3, 3)),
            dma((3, 3)),
            dma((2,)),
            dma((2,)),
            dma((1,)),
            dma((1,)),
            dma((3,)),
            dma((3,)),
            dma((3, cols, chain)),
            dma((3, cols, chain)),
            dma((cols,)),
            dma((cols,)),
            dma((2, chain)),
            dma((2, chain)),
            dma((2, 3, most)),
            dma((2, 3, most)),
            dma((2,)),
            dma((2,)),
            dma((4,)),
        ],
        compiler_params=pltpu.CompilerParams(
            collective_id=1, has_side_effects=True, vmem_limit_bytes=VMEM_BYTES
        ),
    )(
        grad_rows, q_ext, k_ext, v_ext, lse, self_bias, attended, w_qkv, peer_w, normed, tokens, grad_hidden,
        gain[None, :], early, grad_up, grad_down, grad_out,
    )


def body(
    n,
    groups,
    tokens,
    image_ids,
    lengths,
    w_qkv,
    bias_query,
    bias_value,
    w_out,
    w_up,
    bias_up,
    w_down,
    out_biases,
    norm_gain,
    norm_bias,
    cotangent,
):
    share_rows = tokens.shape[0]
    a, b = lax.axis_index("mz"), lax.axis_index("mx")
    chain, cols = mp_parts(n)
    model_index = a * cols + b
    model, hidden = w_up.shape
    width = w_out.shape[0]

    def shifted(values, off):
        return lax.ppermute(values, "mx", [(i, (i + off) % cols) for i in range(cols)])

    def pair_sum(partial):
        blocks = jnp.split(partial, cols)
        total = blocks[0].astype(F32)
        for off in range(1, cols):
            total = total + shifted(blocks[off].astype(BF), cols - off).astype(F32)
        return total

    (
        gathered_one, q_ext, k_ext, v_ext, log_totals, attended, owned,
        up_all, down_all, out_all, bias_all, peer_w, self_bias, hidden_one, rows_two, grad_mlp,
    ) = front(
        n,
        image_ids,
        lengths,
        tokens,
        cotangent,
        norm_gain,
        norm_bias,
        out_biases,
        w_qkv,
        bias_query,
        bias_value,
        w_up,
        w_down,
        w_out,
        bias_up,
    )
    grad_out = grad_mlp[0].astype(F32)
    rows_two = rows_two.reshape(cols * share_rows, model)
    grad_mlp = grad_mlp.reshape(cols * share_rows, model)
    owned = jnp.transpose(owned, (1, 0, 2)).reshape(share_rows, -1)
    bias_all = bias_all[:, 0].reshape(-1)
    pre_act = jnp.dot(rows_two, up_all, preferred_element_type=F32) + bias_all
    below, density = gelu_parts(pre_act)
    activated = (pre_act * below).astype(BF)
    grad_act = jnp.einsum("rd,fd->rf", grad_mlp, down_all, preferred_element_type=F32)
    grad_pre = (grad_act * (below + pre_act * density)).astype(BF)
    grad_normed_two = pair_sum(jnp.einsum("rf,df->rd", grad_pre, up_all, preferred_element_type=F32))
    output_full = (
        hidden_one
        + pair_sum(jnp.dot(activated, down_all, preferred_element_type=F32))
        + out_biases[1]
    )
    grad_up_all = jnp.einsum("rf,rd->fd", grad_pre, rows_two, preferred_element_type=F32)
    grad_down_all = jnp.einsum("rf,rd->fd", activated, grad_mlp, preferred_element_type=F32)
    grad_bias_up = jnp.sum(grad_pre, axis=0, dtype=F32)

    _, norm_two_back = jax.vjp(layer_norm, hidden_one, norm_gain[1], norm_bias[1])
    grad_from_two, gain_two, shift_two = norm_two_back(grad_normed_two)
    grad_hidden = grad_out + grad_from_two
    grad_proj = grad_hidden.astype(BF)
    grad_w_out = jnp.einsum("re,rd->ed", owned, grad_proj, preferred_element_type=F32).astype(BF)
    grad_rows = jnp.einsum(
        "rd,ned->nre", grad_proj, out_all.reshape(n, width, model), preferred_element_type=F32
    ).astype(BF)
    bias_rows = lax.dynamic_update_slice(
        jnp.zeros((chain, cols, hidden), F32), grad_bias_up.reshape(chain, 1, hidden), (0, b, 0)
    )
    early = [gain_two, shift_two, jnp.sum(grad_hidden, axis=0), jnp.sum(grad_out, axis=0)]
    early = jnp.concatenate([jnp.stack(early), bias_rows.reshape(-1, model)])
    up_sum, down_sum, out_sum, head_sum, bias_sum, input_grad, small = rear(
        n,
        grad_rows,
        q_ext,
        k_ext,
        v_ext,
        log_totals,
        self_bias,
        attended,
        w_qkv,
        peer_w,
        gathered_one,
        tokens,
        grad_hidden,
        norm_gain[0],
        early,
        grad_up_all.astype(BF),
        grad_down_all.astype(BF),
        grad_w_out.reshape(n, width, model),
    )
    if groups > 1:
        up_sum, down_sum, out_sum, head_sum, bias_sum, small = lax.psum(
            (up_sum, down_sum, out_sum, head_sum, bias_sum, small), "dg"
        )
    grad_w_up = up_sum.reshape(hidden, model).T.astype(F32)
    grad_w_down = down_sum.reshape(hidden, model).astype(F32)
    grad_w_out = out_sum.reshape(width, model).astype(F32)
    grad_w_qkv = jnp.transpose(head_sum.reshape(3, width, model), (0, 2, 1)).astype(F32)
    grad_bias_query, grad_bias_value = bias_sum[:, 0]
    grad_bias_up = lax.dynamic_slice_in_dim(
        small[0, 4:].reshape(-1), model_index * hidden, hidden, 0
    )
    return (
        output_full.astype(BF),
        input_grad,
        grad_w_qkv,
        grad_bias_query,
        grad_bias_value,
        grad_w_out,
        grad_w_up,
        grad_bias_up,
        grad_w_down,
        small[0, 2:4],
        jnp.stack([small[1, 0], small[0, 0]]),
        jnp.stack([small[1, 1], small[0, 1]]),
    )


def solution(mesh):
    n = mesh.shape["mp"]
    chain, cols = mp_parts(n)
    groups = mesh.shape["dp"] // PARTS
    dp, mp = ("dg", "dp"), ("mz", "mx")
    every = dp + mp
    split = jax.sharding.Mesh(mesh.devices.reshape(groups, PARTS, chain, cols), every)
    in_specs = (
        P(every, None),
        P(dp),
        P(dp, None),
        P(None, None, mp),
        P(mp),
        P(mp),
        P(mp, None),
        P(None, mp),
        P(mp),
        P(mp, None),
        P(),
        P(),
        P(),
        P(every, None),
    )
    out_specs = (
        P(every, None),
        P(every, None),
        P(None, None, mp),
        P(mp),
        P(mp),
        P(mp, None),
        P(None, mp),
        P(mp),
        P(mp, None),
        P(),
        P(),
        P(),
    )
    return jax.shard_map(
        functools.partial(body, n, groups),
        mesh=split,
        in_specs=in_specs,
        out_specs=out_specs,
        check_vma=False,
    )
```

```python
import functools
import math
import types

import jax
import jax.numpy as jnp
from jax import lax
from jax.experimental import pallas as pl
from jax.experimental.pallas import tpu as pltpu
from jax.sharding import PartitionSpec as P

HEAD_DIM = 64
LANES = 128
CHUNK = 768
MASKED = -1e30
MESH = pl.DeviceIdType.MESH
VMEM_BYTES = 67_043_328
BF = jnp.bfloat16
F32 = jnp.float32
NN = (((1,), (0,)), ((), ()))
NT = (((1,), (1,)), ((), ()))
TN = (((0,), (0,)), ((), ()))
SCALE = HEAD_DIM ** (-0.5)
PARTS = 4
epsilon = 1e-06


def dot(left, right, dims=NN):
    return lax.dot_general(left, right, dims, preferred_element_type=F32)


def layer_norm(values, gain_vec, shift_vec):
    row_mean = jnp.mean(values, axis=-1, keepdims=True)
    centered = values - row_mean
    variance = jnp.mean(centered * centered, axis=-1, keepdims=True)
    return centered * lax.rsqrt(variance + epsilon) * gain_vec + shift_vec


def gelu_parts(values):
    share = 0.5 + 0.5 * lax.erf(values * math.sqrt(0.5))
    return share, jnp.exp(-0.5 * values * values) * (1 / math.sqrt(2 * math.pi))


def mp_parts(n):
    chain = min(4, n)
    return chain, n // chain


def column_sum(values):
    ones = jnp.ones((8, values.shape[1]), BF)
    high = values.astype(BF)
    low = (values - high.astype(F32)).astype(BF)
    return dot(ones, high, NT) + dot(ones, low, NT)


def split_three(column):
    high = column.astype(BF)
    rest = column - high.astype(F32)
    middle = rest.astype(BF)
    return high, middle, (rest - middle.astype(F32)).astype(BF)


def attend_chunk(c, heads, q_ref, k_ref, v_ref, vt_ref, self_ref, att_ref, lse_ref):
    rows = pl.ds(pl.multiple_of(c * CHUNK, CHUNK), CHUNK)
    pieces = []
    scores = [dot(k_ref[h], q_ref[h, rows, :], NT) for h in range(heads)]
    for h in range(heads):
        own = q_ref[h, rows, :HEAD_DIM].astype(F32) * k_ref[h, rows, :HEAD_DIM].astype(F32)
        own = column_sum(own)[:1] + self_ref[:1, rows]
        top = jnp.maximum(jnp.max(scores[h], axis=0, keepdims=True), own)
        weights = jnp.exp(scores[h] - top).astype(BF)
        own_weight = jnp.exp(own - top).astype(BF).astype(F32)
        summed = dot(vt_ref[h], weights) + vt_ref[h, :, rows].astype(F32) * own_weight
        total = summed[HEAD_DIM : HEAD_DIM + 1]
        pieces.append(summed[:HEAD_DIM] / total)
        lse_ref[h, :, rows] = jnp.broadcast_to(top + jnp.log(total), (8, CHUNK))
    stacked = jnp.concatenate(pieces, axis=0) if heads > 1 else pieces[0]
    att_ref[rows, :] = stacked.T.astype(BF)


def front_kernel(
    n,
    ids_ref,
    lengths_ref,
    tokens_ref,
    cot_ref,
    gain_ref,
    shift_ref,
    out_bias_ref,
    w_ref,
    bias_ref,
    up_ref,
    down_ref,
    out_ref,
    bup_ref,
    normed_ref,
    q_ref,
    k_ref,
    v_ref,
    lse_ref,
    att_ref,
    owned_ref,
    ups_ref,
    downs_ref,
    outs_out,
    bups_ref,
    peers_ref,
    self_ref,
    hidden_ref,
    pair_two,
    pair_cot,
    blocks,
    outs_ref,
    two,
    cot,
    peer_w,
    peer_b,
    proj_out,
    proj_in,
    vt_ref,
    owned,
    ssz,
    rsz,
    ssx,
    rsx,
    spw,
    rpw,
    spb,
    rpb,
    ssa,
    rsa,
    wsz,
    wrz,
    wsx,
    wrx,
    gs,
    gr,
    os,
    orr,
    bs,
    br,
    spp,
    rpp,
    local_sem,
):
    chain, cols = mp_parts(n)
    share, _ = tokens_ref.shape
    width = w_ref.shape[2]
    heads = width // HEAD_DIM
    hidden = up_ref.shape[1]
    up_rows, down_rows, out_rows = (r.shape[0] // PARTS for r in (up_ref, down_ref, out_ref))
    dg, dp = lax.axis_index("dg"), lax.axis_index("dp")
    a, b = lax.axis_index("mz"), lax.axis_index("mx")
    me = a * cols + b
    part = lax.rem(dp, PARTS)
    core_dp = dp + 1 - 2 * lax.rem(dp, 2)
    side_dp = dp + 2 - 4 * lax.rem(dp // 2, 2)
    core_part, side_part = lax.rem(core_dp, PARTS), lax.rem(side_dp, PARTS)
    far_part = PARTS - 1 - part

    barrier = pltpu.get_barrier_semaphore()
    for off in range(1, n):
        other = lax.rem(me + off, n)
        pl.semaphore_signal(
            barrier,
            inc=1,
            device_id=(dg, dp, other // cols, lax.rem(other, cols)),
            device_id_type=MESH,
        )
    for peer in (core_dp, side_dp):
        pl.semaphore_signal(barrier, inc=1, device_id=(dg, peer, a, b), device_id_type=MESH)
    pl.semaphore_wait(barrier, n + 1)

    def remote(src, dst, send, recv, device):
        return pltpu.make_async_remote_copy(
            src_ref=src,
            dst_ref=dst,
            send_sem=send,
            recv_sem=recv,
            device_id=(dg,) + device,
            device_id_type=MESH,
        )

    def span(index, size):
        return pl.ds(pl.multiple_of(index * size, size), size)

    def can(way):
        return (a < chain - 1) if way == 0 else (a > 0)

    def chain_peer(way):
        return (dp, jnp.clip(a + (1 if way == 0 else -1), 0, chain - 1), b)

    def cross_peer(off):
        return (dp, a, lax.rem(b + off, cols))

    def back_peer(off):
        return (dp, a, lax.rem(b - off + cols, cols))

    def chain_copy(row, way):
        spot = blocks.at[row]
        return remote(spot, spot, ssz.at[way, row], rsz.at[way, row], chain_peer(way))

    def cross_copy(row, off):
        return remote(
            proj_out.at[off - 1, row],
            proj_in.at[off - 1, row],
            ssx.at[off, row],
            rsx.at[off, row],
            back_peer(off),
        )

    def peer_copies(off):
        return [
            remote(w_ref, peer_w.at[off - 1], spw.at[off], rpw.at[off], cross_peer(off)),
            remote(bias_ref, peer_b.at[off - 1], spb.at[off], rpb.at[off], cross_peer(off)),
        ]

    def piece(i, row, of_part):
        if i == 0:
            return outs_ref.at[row * cols + b, span(of_part, out_rows)]
        if i == 1:
            return ups_ref.at[span(of_part, up_rows), span(row, hidden)]
        return downs_ref.at[span(row * PARTS + of_part, down_rows)]

    def own_piece(i):
        if i == 0:
            return out_ref.at[span(part, out_rows)]
        if i == 1:
            return up_ref.at[span(part, up_rows)]
        return down_ref.at[span(part, down_rows)]

    def weight_copy(i, row, way, own=False):
        spot = piece(i, row, part)
        sems = wsz.at[i, way, row], wrz.at[i, way, row]
        return remote(own_piece(i) if own else spot, spot, *sems, chain_peer(way))

    def out_cross(block, off, own=False):
        spot = outs_ref.at[block, span(part, out_rows)]
        sems = wsx.at[off, block // cols], wrx.at[off, block // cols]
        return remote(own_piece(0) if own else spot, spot, *sems, cross_peer(off))

    def group_copy(kind, i, row, arriving=False):
        sent = side_part if kind == 2 else part
        got = (side_part, core_part, far_part)[kind]
        spot = piece(i, row, got if arriving else sent)
        sems = gs.at[kind, i - 1, row], gr.at[kind, i - 1, row]
        return remote(spot, spot, *sems, (side_dp if kind == 0 else core_dp, a, b))

    def out_group(kind, arriving=False):
        sent = side_part if kind == 2 else part
        got = (side_part, core_part, far_part)[kind]
        spot = outs_ref.at[:, span(got if arriving else sent, out_rows)]
        return remote(spot, spot, os.at[kind], orr.at[kind], (side_dp if kind == 0 else core_dp, a, b))

    def bias_copy(off, arriving=False):
        spot = bups_ref.at[lax.rem(a - off + chain, chain) if arriving else a]
        return remote(bup_ref, spot, bs.at[off], br.at[off], (dp, lax.rem(a + off, chain), b))

    def start_own(way):
        for i in (1, 2):
            weight_copy(i, a, way, own=True).start()

    stay = [
        pltpu.make_async_copy(up_ref, ups_ref.at[:, span(a, hidden)], local_sem.at[1]),
        pltpu.make_async_copy(down_ref, downs_ref.at[span(a, hidden)], local_sem.at[2]),
        pltpu.make_async_copy(own_piece(0), piece(0, a, part), local_sem.at[3]),
        pltpu.make_async_copy(bup_ref, bups_ref.at[a], local_sem.at[4]),
    ]

    for off in range(1, cols):
        for copy in peer_copies(off):
            copy.start()

    def norm_one(i, _):
        cut = span(i, 16)
        values = layer_norm(tokens_ref[cut, :].astype(F32), gain_ref[:1], shift_ref[:1])
        blocks[a, cut, :] = values.astype(BF)
        return 0

    lax.fori_loop(0, share // 16, norm_one, 0)

    total = n * share
    slot = total // 2
    first_id, last_id = ids_ref[0], ids_ref[total - 1]
    first_length, last_length = (
        jnp.where(k == 0, lengths_ref[0, 0], lengths_ref[0, 1]) for k in (first_id, last_id)
    )
    last_start = jnp.where(first_id == last_id, 0, slot)

    def row_facts(index):
        late = index >= slot
        inside = index - jnp.where(late, last_start, 0) < jnp.where(late, last_length, first_length)
        return jnp.where(late, last_id, first_id), inside

    def place(block, out_q, out_k, out_v):
        rows = span(block, share)
        lane = lax.broadcasted_iota(jnp.int32, (share, LANES - HEAD_DIM), 1)
        image, inside = row_facts(
            block * share + lax.broadcasted_iota(jnp.int32, (share, LANES - HEAD_DIM), 0)
        )
        tail_q = jnp.where(lane == image, 1.0, 0.0).astype(BF)
        hidden_key = jnp.where((lane == image) & inside, 0.0, MASKED)
        tail_k = jnp.where(lane < 2, hidden_key, 0.0).astype(BF)
        tail_v = jnp.where(lane < 3, 1.0, 0.0).astype(BF)
        for h in range(heads):
            cut = slice(h * HEAD_DIM, (h + 1) * HEAD_DIM)
            q_ref[h, rows, :] = jnp.concatenate(
                [out_q[:, cut] * jnp.asarray(SCALE, BF), tail_q], axis=1
            )
            k_ref[h, rows, :] = jnp.concatenate([out_k[:, cut], tail_k], axis=1)
            v_ref[h, rows, :] = jnp.concatenate([out_v[:, cut], tail_v], axis=1)

    def project(row):
        values = blocks[row]
        place(
            row * cols + b,
            (dot(values, w_ref[0]) + bias_ref[0, :1]).astype(BF),
            dot(values, w_ref[1]).astype(BF),
            (dot(values, w_ref[2]) + bias_ref[1, :1]).astype(BF),
        )

    def project_peer(row):
        def one(slot, _):
            values = blocks[row]
            proj_out[slot, row, 0] = (dot(values, peer_w[slot, 0]) + peer_b[slot, 0, :1]).astype(BF)
            proj_out[slot, row, 1] = dot(values, peer_w[slot, 1]).astype(BF)
            proj_out[slot, row, 2] = (dot(values, peer_w[slot, 2]) + peer_b[slot, 1, :1]).astype(BF)
            return 0

        lax.fori_loop(0, cols - 1, one, 0)
        for off in range(1, cols):
            cross_copy(row, off).start()

    for way in (0, 1):

        @pl.when(can(way))
        def _(way=way):
            chain_copy(a, way).start()
            weight_copy(0, a, way, own=True).start()

    def pair_copy(i, off):
        src, dst = ((two, pair_two), (cot, pair_cot))[i]
        return remote(src, dst.at[off], spp.at[i, off], rpp.at[i, off], cross_peer(off))

    pair_stay = [
        pltpu.make_async_copy(two, pair_two.at[0], local_sem.at[6]),
        pltpu.make_async_copy(cot, pair_cot.at[0], local_sem.at[7]),
    ]
    for copy in stay:
        copy.start()

    @pl.when(a == 0)
    def _():
        start_own(0)

    @pl.when(a == chain - 1)
    def _():
        start_own(1)

    project(a)
    _, self_inside = row_facts(lax.broadcasted_iota(jnp.int32, (8, total), 1))
    self_ref[...] = jnp.where(self_inside, MASKED, 0.0)

    def mask_cot(i, _):
        cut = span(i, 16)
        _, inside = row_facts(
            me * share + i * 16 + lax.broadcasted_iota(jnp.int32, (16, cot.shape[1]), 0)
        )
        cot[cut, :] = jnp.where(inside, cot_ref[cut, :].astype(F32), 0.0).astype(BF)
        return 0

    lax.fori_loop(0, share // 16, mask_cot, 0)

    def visit(step, _):
        for way in (0, 1):
            there = a - step if way == 0 else a + step
            inside = (there >= 0) & (there < chain)
            row = jnp.clip(there, 0, chain - 1)

            @pl.when(inside)
            def _(way=way, row=row):
                chain_copy(row, way).wait_recv()

                @pl.when(can(way))
                def _():
                    chain_copy(row, way).start()

                weight_copy(0, row, way).wait_recv()

                @pl.when(can(way))
                def _():
                    weight_copy(0, row, way).start()

        @pl.when((step == a) & can(0))
        def _():
            start_own(0)

        @pl.when((step == chain - 1 - a) & can(1))
        def _():
            start_own(1)

        @pl.when(step == 1)
        def _():
            for off in range(1, cols):
                for copy in peer_copies(off):
                    copy.wait_recv()

        def one(j, _):
            gone = step - jnp.where(j == 0, 1, 0)
            there = jnp.where(j == 1, a - gone, a + gone)

            @pl.when((there >= 0) & (there < chain) & ((j > 0) | (step == 1)))
            def _():
                @pl.when(j > 0)
                def _():
                    project(there)

                project_peer(there)

            return 0

        lax.fori_loop(0, 3, one, 0)
        return 0

    lax.fori_loop(1, chain, visit, 0)

    stay[2].wait()
    for off in range(1, cols):
        out_cross(me, off, own=True).start()

    def out_send(i, _):
        row = lax.rem(a + i, chain)
        for off in range(1, cols):
            out_cross(row * cols + b, off).start()
        return 0

    lax.fori_loop(1, chain, out_send, 0)

    def receive(i, _):
        row = lax.rem(a + i, chain)
        for off in range(1, cols):
            cross_copy(row, off).wait_recv()
            block = row * cols + lax.rem(b + off, cols)
            place(block, *[proj_in[off - 1, row, t] for t in range(3)])
        return 0

    lax.fori_loop(0, chain, receive, 0)
    keep = pltpu.make_async_copy(blocks, normed_ref, local_sem.at[0])
    keep.start()
    keep_peers = pltpu.make_async_copy(peer_w, peers_ref, local_sem.at[5])
    keep_peers.start()

    def gather_out(row, _):
        for off in range(1, cols):
            out_cross(row * cols + lax.rem(b - off + cols, cols), off).wait_recv()
        return 0

    lax.fori_loop(0, chain, gather_out, 0)
    out_group(0).start()
    out_group(1).start()
    for off in range(1, chain):
        bias_copy(off).start()

    def both_ways(step, act):
        for way in (0, 1):
            there = a - step if way == 0 else a + step

            @pl.when((there >= 0) & (there < chain))
            def _(way=way, there=there):
                act(way, jnp.clip(there, 0, chain - 1))

    def weights_pass(way, row):
        for i in (1, 2):
            weight_copy(i, row, way).wait_recv()

            @pl.when(can(way))
            def _(i=i):
                weight_copy(i, row, way).start()

            group_copy(0, i, row).start()
            group_copy(1, i, row).start()

    def weights_side(way, row):
        for i in (1, 2):
            group_copy(0, i, row, arriving=True).wait_recv()
            group_copy(2, i, row).start()

    both_ways(1, weights_pass)

    def flip(c, _):
        rows = span(c, CHUNK)
        for h in range(heads):
            vt_ref[h, :, rows] = v_ref[h, rows, :].astype(F32).T.astype(BF)
        return 0

    lax.fori_loop(0, n * share // CHUNK, flip, 0)

    def own_copy(target, source):
        return remote(
            att_ref.at[span(target, share)],
            owned.at[source],
            ssa.at[target],
            rsa.at[source],
            (dp, target // cols, lax.rem(target, cols)),
        )

    def attend(c, _):
        attend_chunk(c, heads, q_ref, k_ref, v_ref, vt_ref, self_ref, att_ref, lse_ref)

        def send(target, _):
            end = (target + 1) * share

            @pl.when((end <= (c + 1) * CHUNK) & (end > c * CHUNK) & (target != me))
            def _():
                own_copy(target, me).start()

            return 0

        lax.fori_loop(0, n, send, 0)

        @pl.when(c == 0)
        def _():
            out_group(0, arriving=True).wait_recv()
            out_group(2).start()

        @pl.when(c == n * share // CHUNK - 1)
        def _():
            both_ways(2, weights_pass)
            both_ways(1, weights_side)

        return 0

    lax.fori_loop(0, n * share // CHUNK, attend, 0)
    owned[me] = att_ref[span(me, share), :]
    for off in range(1, cols):
        pair_copy(1, off).start()
    pair_stay[1].start()
    both_ways(3, weights_pass)
    both_ways(2, weights_side)
    for kind in (1, 2):
        out_group(kind, arriving=True).wait_recv()
    keep_out = pltpu.make_async_copy(outs_ref, outs_out, local_sem.at[3])
    keep_out.start()

    def collect(other, _):
        @pl.when(other != me)
        def _():
            own_copy(other, me).wait_send()
            own_copy(me, other).wait_recv()

        return 0

    lax.fori_loop(0, n, collect, 0)
    hidden_ref[...] = tokens_ref[...].astype(F32) + out_bias_ref[:1]

    def out_project(m, _):
        hidden_ref[...] += dot(owned[m], outs_ref[m])
        return 0

    lax.fori_loop(0, n, out_project, 0)

    def norm_two(i, _):
        cut = span(i, 16)
        two[cut, :] = layer_norm(hidden_ref[cut, :], gain_ref[1:], shift_ref[1:]).astype(BF)
        return 0

    lax.fori_loop(0, share // 16, norm_two, 0)
    for off in range(1, cols):
        pair_copy(0, off).start()
    pair_stay[0].start()
    both_ways(chain - 1, weights_side)
    owned_ref[...] = owned[...]
    for off in range(1, cols):
        for i in (0, 1):
            pair_copy(i, off).wait_send()
            pair_copy(i, off).wait_recv()
    for copy in pair_stay:
        copy.wait()
    keep_out.wait()
    keep.wait()
    keep_peers.wait()
    for off in range(1, cols):
        for copy in peer_copies(off):
            copy.wait_send()
    for i in (0, 1, 3):
        stay[i].wait()
    for off in range(1, chain):
        bias_copy(off).wait_send()
        bias_copy(off, arriving=True).wait_recv()
    for kind in range(3):
        out_group(kind).wait_send()

    def drain(row, _):
        for off in range(1, cols):
            cross_copy(row, off).wait_send()
            out_cross(row * cols + b, off).wait_send()

        @pl.when((row <= a) & (a < chain - 1))
        def _():
            chain_copy(row, 0).wait_send()
            for i in range(3):
                weight_copy(i, row, 0).wait_send()

        @pl.when((row >= a) & (a > 0))
        def _():
            chain_copy(row, 1).wait_send()
            for i in range(3):
                weight_copy(i, row, 1).wait_send()

        @pl.when(row != a)
        def _():
            for i in (1, 2):
                for kind in range(3):
                    group_copy(kind, i, row).wait_send()
                    if kind > 0:
                        group_copy(kind, i, row, arriving=True).wait_recv()

        return 0

    lax.fori_loop(0, chain, drain, 0)


def front(
    n, image_ids, lengths, tokens, cotangent, gain, shift, out_biases, w_qkv, bias_query, bias_value, w_up, w_down,
    w_out, bias_up,
):
    chain, cols = mp_parts(n)
    share, model = tokens.shape
    width = w_qkv.shape[2]
    heads = width // HEAD_DIM
    hidden = w_up.shape[1]
    rows = n * share
    vmem = pl.BlockSpec(memory_space=pltpu.VMEM)
    anywhere = pl.BlockSpec(memory_space=pl.ANY)
    ext = jax.ShapeDtypeStruct((heads, rows, LANES), BF)
    dma = pltpu.SemaphoreType.DMA
    return pl.pallas_call(
        functools.partial(front_kernel, n),
        name="front",
        out_shape=(
            jax.ShapeDtypeStruct((chain, share, model), BF),
            ext,
            ext,
            ext,
            jax.ShapeDtypeStruct((heads, 8, rows), F32),
            jax.ShapeDtypeStruct((rows, width), BF),
            jax.ShapeDtypeStruct((n, share, width), BF),
            jax.ShapeDtypeStruct((model, chain * hidden), BF),
            jax.ShapeDtypeStruct((chain * hidden, model), BF),
            jax.ShapeDtypeStruct((n, width, model), BF),
            jax.ShapeDtypeStruct((chain, 8, hidden), F32),
            jax.ShapeDtypeStruct((cols - 1,) + w_qkv.shape, BF),
            jax.ShapeDtypeStruct((8, rows), F32),
            jax.ShapeDtypeStruct((share, model), F32),
            jax.ShapeDtypeStruct((cols, share, model), BF),
            jax.ShapeDtypeStruct((cols, share, model), BF),
        ),
        in_specs=[pl.BlockSpec(memory_space=pltpu.SMEM)] * 2 + [vmem] * 11,
        out_specs=(anywhere,) + (vmem,) * 6 + (anywhere,) * 5 + (vmem,) * 2 + (anywhere,) * 2,
        scratch_shapes=[
            pltpu.VMEM((chain, share, model), BF),
            pltpu.VMEM((n, width, model), BF),
            pltpu.VMEM((share, model), BF),
            pltpu.VMEM((share, model), BF),
            pltpu.VMEM((cols - 1,) + w_qkv.shape, BF),
            pltpu.VMEM((cols - 1, 2, 8, width), F32),
            pltpu.VMEM((cols - 1, chain, 3, share, width), BF),
            pltpu.VMEM((cols - 1, chain, 3, share, width), BF),
            pltpu.VMEM((heads, LANES, rows), BF),
            pltpu.VMEM((n, share, width), BF),
            dma((2, chain)),
            dma((2, chain)),
            dma((cols, chain)),
            dma((cols, chain)),
            dma((cols,)),
            dma((cols,)),
            dma((cols,)),
            dma((cols,)),
            dma((n,)),
            dma((n,)),
            dma((3, 2, chain)),
            dma((3, 2, chain)),
            dma((cols, chain)),
            dma((cols, chain)),
            dma((3, 2, chain)),
            dma((3, 2, chain)),
            dma((3,)),
            dma((3,)),
            dma((chain,)),
            dma((chain,)),
            dma((2, cols)),
            dma((2, cols)),
            dma((8,)),
        ],
        compiler_params=pltpu.CompilerParams(
            collective_id=0, has_side_effects=True, vmem_limit_bytes=VMEM_BYTES
        ),
    )(
        image_ids,
        lengths,
        tokens,
        cotangent,
        gain,
        shift,
        out_biases,
        w_qkv,
        jnp.broadcast_to(jnp.stack([bias_query, bias_value])[:, None, :], (2, 8, width)),
        w_up,
        w_down,
        w_out,
        jnp.broadcast_to(bias_up[None, :], (8, hidden)),
    )


def attend_back_chunk(
    c, heads, q_ref, k_ref, v_ref, kt_ref, lse_ref, self_ref, att_ref, grad_ref, gq_ref, dk_ref, dv_ref
):
    rows = pl.ds(pl.multiple_of(c * CHUNK, CHUNK), CHUNK)
    grads = grad_ref[rows, :].astype(F32)
    products = grads * att_ref[rows, :].astype(F32)
    outs = []
    for h in range(heads):
        cut = slice(h * HEAD_DIM, (h + 1) * HEAD_DIM)
        inner = jnp.sum(products[:, cut], axis=1, keepdims=True)
        parts = split_three(-inner)
        lane = lax.broadcasted_iota(jnp.int32, (CHUNK, LANES - HEAD_DIM), 1)
        tail = jnp.zeros((CHUNK, LANES - HEAD_DIM), F32)
        for i, part in enumerate(parts):
            tail = jnp.where(lane == i, part.astype(F32), tail)
        grad_ext = jnp.concatenate([grads[:, cut], tail], axis=1).astype(BF)
        query = q_ref[h, rows, :]
        key_own = k_ref[h, rows, :]
        scores = dot(k_ref[h], query, NT)
        lse = lse_ref[h, :1, rows]
        probs = jnp.exp(scores - lse)
        shifted = dot(v_ref[h], grad_ext, NT)
        own = column_sum(query[:, :HEAD_DIM].astype(F32) * key_own[:, :HEAD_DIM].astype(F32))
        own_prob = jnp.exp(own + self_ref[:, rows] - lse)
        own_shifted = column_sum(v_ref[h, rows, :].astype(F32) * grad_ext.astype(F32))
        lower = lax.broadcasted_iota(jnp.int32, (8, CHUNK), 0) < 4
        both = jnp.where(lower, own_prob, own_prob * own_shifted).T
        own_prob, own_score = both[:, :1], both[:, 4:5]
        grad_scores = (probs * shifted).astype(BF)
        dv = dot(probs.astype(BF), grad_ext)
        dk = dot(grad_scores, query)
        dq = dot(kt_ref[h], grad_scores).T
        dq = (dq + own_score * key_own.astype(F32)) * SCALE
        outs.append(dq[:, :HEAD_DIM])

        @pl.when(c == 0)
        def _(h=h, dv=dv, dk=dk):
            dv_ref[h] = dv
            dk_ref[h] = dk

        @pl.when(c > 0)
        def _(h=h, dv=dv, dk=dk):
            dv_ref[h] += dv
            dk_ref[h] += dk

        dv_ref[h, rows, :] += own_prob * grad_ext.astype(F32)
        dk_ref[h, rows, :] += own_score * query.astype(F32)
    stacked = jnp.concatenate(outs, axis=1) if heads > 1 else outs[0]
    gq_ref[rows, :] = stacked.astype(BF)


REAR_REFS = (
    "gatt",
    "q",
    "k",
    "v",
    "lse",
    "self_bias",
    "att",
    "w",
    "peer_w",
    "normed",
    "tokens",
    "grad_hidden",
    "gain",
    "early",
    "up",
    "down",
    "out",
    "up_sum",
    "down_sum",
    "out_sum",
    "head_sum",
    "bias_out",
    "input_grad",
    "small_out",
    "grad",
    "kt",
    "dk",
    "dv",
    "gq",
    "gk",
    "gv",
    "kept",
    "pool_core",
    "pool_side",
    "way_in",
    "out_in",
    "local_in",
    "local_side",
    "acc",
    "peer_in",
    "peer_got",
    "way_gn",
    "gn",
    "small",
    "small_in",
    "bias_sum",
    "bias_in",
    "sa",
    "ra",
    "so",
    "ro",
    "sc",
    "rc",
    "sk",
    "ss",
    "rs",
    "sz",
    "rz",
    "sg",
    "rg",
    "st",
    "rt",
    "sy",
    "ry",
    "sh",
    "rh",
    "sx",
    "rx",
    "sw",
    "rw",
    "sn",
    "rn",
    "sm",
    "rm",
    "sb",
    "rb",
    "sl",
)


def rear_kernel(n, *refs):
    r = types.SimpleNamespace(**dict(zip(REAR_REFS, refs)))
    chain, cols = mp_parts(n)
    heads, total, _ = r.q.shape
    _, share, width = r.gatt.shape
    model = r.w.shape[1]
    hidden = r.up.shape[0] // chain
    rows, out_rows = hidden // PARTS, width // PARTS
    block_rows = 2 * rows + cols * out_rows
    local_rows = 3 * width // PARTS
    head_base = (cols - 1) * 3 * width
    done_base = head_base + 3 * width
    local = r.pool_core.at[pl.ds(head_base, 3 * width)]
    done = r.pool_core.at[pl.ds(done_base, block_rows)]
    local_done = r.pool_core.at[pl.ds(done_base + block_rows, local_rows)]
    dg, dp = lax.axis_index("dg"), lax.axis_index("dp")
    a, b = lax.axis_index("mz"), lax.axis_index("mx")
    me = a * cols + b
    part = lax.rem(dp, PARTS)
    core_dp = dp + 1 - 2 * lax.rem(dp, 2)
    side_dp = dp + 2 - 4 * lax.rem(dp // 2, 2)
    core_part, side_part = lax.rem(core_dp, PARTS), lax.rem(side_dp, PARTS)
    far_part = PARTS - 1 - part
    core_id, side_id = (core_dp, a, b), (side_dp, a, b)
    far_id = (PARTS - 1 - dp, a, b)

    def mp_id(index):
        return dp, index // cols, lax.rem(index, cols)

    barrier = pltpu.get_barrier_semaphore()
    for off in range(1, n):
        pl.semaphore_signal(
            barrier, inc=1, device_id=(dg,) + mp_id(lax.rem(me + off, n)), device_id_type=MESH
        )
    for peer in (core_id, side_id, far_id):
        pl.semaphore_signal(barrier, inc=1, device_id=(dg,) + peer, device_id_type=MESH)
    pl.semaphore_wait(barrier, n + 2)

    def remote(src, dst, send, recv, device):
        return pltpu.make_async_remote_copy(
            src_ref=src,
            dst_ref=dst,
            send_sem=send,
            recv_sem=recv,
            device_id=(dg,) + device,
            device_id_type=MESH,
        )

    def span(index, size):
        return pl.ds(pl.multiple_of(index * size, size), size)

    def in_order(i):
        low = jnp.where(chain - 1 - i > a, chain - 1 - i, chain - 2 - i)
        high = jnp.where(i < a, i, i + 1)
        return jnp.where(i == chain - 1, a, jnp.where(2 * a < chain, low, high))

    def add_rows(dst, *terms):
        count = dst.shape[0]
        step = 32 if count % 32 == 0 else 16

        def one(i, _):
            cut = span(i, step)
            value = terms[0][cut, :].astype(F32)
            for term in terms[1:]:
                value = value + term[cut, :].astype(F32)
            dst[cut, :] = value.astype(dst.dtype)
            return 0

        lax.fori_loop(0, count // step, one, 0)

    def loop(count, act):
        def one(i, _):
            act(i)
            return 0

        lax.fori_loop(0, count, one, 0)

    def others(act):
        def one(m):
            @pl.when(m != me)
            def _():
                act(m)

        loop(n, one)

    def row_copy(target, source):
        return remote(
            r.gatt.at[target], r.grad.at[span(source, share)], r.sa.at[target], r.ra.at[source], mp_id(target)
        )

    def source_rows(i, t, which):
        if i < 2:
            return (r.up, r.down)[i].at[span(t * PARTS + which, rows)]
        return r.out.at[t * cols + lax.rem(b + i - 2, cols), span(which, out_rows)]

    def offset(i):
        return i * rows if i < 2 else 2 * rows + (i - 2) * out_rows

    def core_copy(t, slot, i):
        src = source_rows(i, t, far_part if slot else core_part)
        base = pl.multiple_of((t * 2 + slot) * block_rows + offset(i), 16)
        return remote(
            src, r.pool_core.at[pl.ds(base, src.shape[0])], r.sc.at[t, slot, i], r.rc.at[t, slot, i], core_id
        )

    def keep_copy(t, slot, i):
        src = source_rows(i, t, side_part if slot else part)
        return pltpu.make_async_copy(
            src, r.kept.at[t, slot, pl.ds(offset(i), src.shape[0])], r.sk.at[t, slot, i]
        )

    def side_copy(t):
        return remote(r.kept.at[t, 1], r.pool_side.at[span(t, block_rows)], r.ss.at[t], r.rs.at[t], side_id)

    def chain_id(way):
        return dp, jnp.clip(a + (1 if way == 0 else -1), 0, chain - 1), b

    def hop_of(way):
        return a if way == 0 else chain - 1 - a

    def ahead(way, t):
        return (t > a) if way == 0 else (t < a)

    def chain_copy(flow, way, t, fresh=False):
        own, inbox, send, recv = flow
        spot = inbox.at[way, t]
        return remote(own(t) if fresh else spot, spot, send.at[way, t], recv.at[way, t], chain_id(way))

    def chain_service(flow, s, prepare):
        own, inbox = flow[:2]
        for way in (0, 1):
            hop = hop_of(way)
            t = chain - 1 + a - s if way == 0 else s - hop
            active = (t > a) & (t < chain) if way == 0 else (t >= 0) & (t < a)
            spot = jnp.clip(t, 0, chain - 1)

            @pl.when(active)
            def _(way=way, t=spot):
                prepare(t)

            @pl.when(active & (hop == 0))
            def _(way=way, t=spot):
                chain_copy(flow, way, t, fresh=True).start()

            @pl.when(active & (hop > 0))
            def _(way=way, t=spot):
                chain_copy(flow, way, t).wait_recv()
                add_rows(inbox.at[way, t], inbox.at[way, t], own(t))
                chain_copy(flow, way, t).start()

    def chain_finish(flow, dst, prepare):
        own, inbox = flow[:2]
        prepare(a)

        @pl.when(a > 0)
        def _():
            chain_copy(flow, 0, a).wait_recv()

        @pl.when(a < chain - 1)
        def _():
            chain_copy(flow, 1, a).wait_recv()

        @pl.when((a > 0) & (a < chain - 1))
        def _():
            add_rows(dst, own(a), inbox.at[0, a], inbox.at[1, a])

        @pl.when(a == 0)
        def _():
            add_rows(dst, own(a), inbox.at[1, a])

        @pl.when(a == chain - 1)
        def _():
            add_rows(dst, own(a), inbox.at[0, a])

    def chain_drain(flow):
        def one(t):
            for way in (0, 1):

                @pl.when(ahead(way, t))
                def _(way=way):
                    chain_copy(flow, way, t).wait_send()

        loop(chain, one)

    def share_copy(share_flow, kind, arriving=False):
        own, everyone, send, recv = share_flow
        sent = side_part if kind == 2 else part
        got = (side_part, core_part, far_part)[kind]
        spot = everyone.at[got if arriving else sent]
        src = spot if kind == 2 or arriving else own
        return remote(src, spot, send.at[kind], recv.at[kind], side_id if kind == 0 else core_id)

    weights = (lambda t: r.kept.at[t, 0], r.way_in, r.sz, r.rz)
    grads = (lambda t: r.pool_side.at[span(t, share)], r.way_gn, r.sn, r.rn)
    share_weights = [
        (done.at[pl.ds(0, rows)], r.up_sum, r.sg.at[0], r.rg.at[0]),
        (done.at[pl.ds(rows, rows)], r.down_sum, r.sg.at[1], r.rg.at[1]),
        (done.at[pl.ds(2 * rows, out_rows)], r.out_sum, r.sg.at[2], r.rg.at[2]),
    ]
    share_local = (local_done, r.head_sum, r.sh, r.rh)

    def small_peers(stage):
        if stage == 0:
            return [core_id, side_id, far_id]
        if stage == 1:
            return [(dp, a, lax.rem(b + off, cols)) for off in range(1, cols)]
        return [(dp, lax.rem(a + off, chain), b) for off in range(1, chain)]

    def small_copies(which, stage):
        src = r.early if which == 0 and stage == 0 else r.small.at[which, stage]
        return [
            remote(src, r.small_in.at[which, stage, i], r.sm.at[which, stage, i], r.rm.at[which, stage, i], peer)
            for i, peer in enumerate(small_peers(stage))
        ]

    def small_start(which, stage):
        for copy in small_copies(which, stage):
            copy.start()

    def small_sum(which, stage):
        value = r.early[...] if which == 0 and stage == 0 else r.small[which, stage]
        for i, copy in enumerate(small_copies(which, stage)):
            copy.wait_recv()
            value = value + r.small_in[which, stage, i]
        if stage < 2:
            r.small[which, stage + 1] = value
            small_start(which, stage + 1)
        else:
            r.small_out[which] = value

    def bias_copy(stage):
        return remote(
            r.bias_sum.at[stage], r.bias_in.at[stage], r.sb.at[stage], r.rb.at[stage], (core_id, side_id)[stage]
        )

    others(lambda m: row_copy(m, me).start())
    small_start(0, 0)

    def start_core(i):
        t = in_order(i)
        for slot in (1, 0):
            for k in range(2 + cols):
                core_copy(t, slot, k).start()
                keep_copy(t, slot, k).start()

    loop(chain, start_core)
    r.grad[span(me, share), :] = r.gatt[me]

    def flip(c):
        cut = span(c, CHUNK)
        for h in range(heads):
            r.kt[h, :, cut] = r.k[h, cut, :].astype(F32).T.astype(BF)

    loop(total // CHUNK, flip)

    def core_sum(i):
        t = in_order(i)
        for slot in (1, 0):
            for k in range(2 + cols):
                keep_copy(t, slot, k).wait()
                core_copy(t, slot, k).wait_recv()
            add_rows(r.kept.at[t, slot], r.kept.at[t, slot], r.pool_core.at[span(t * 2 + slot, block_rows)])
            if slot == 1:
                side_copy(t).start()

    loop(chain, core_sum)
    others(lambda m: row_copy(me, m).wait_recv())

    def side_sum(t):
        side_copy(t).wait_recv()
        add_rows(r.kept.at[t, 0], r.kept.at[t, 0], r.pool_side.at[span(t, block_rows)])

    def cross_copy(k, lag, t):
        return remote(
            (r.gq, r.gk, r.gv)[k].at[span(t * cols + lax.rem(b + lag, cols), share)],
            r.peer_in.at[lag - 1, k, t],
            r.sx.at[k, lag, t],
            r.rx.at[k, lag, t],
            (dp, a, lax.rem(b + lag, cols)),
        )

    chain_service(weights, 0, side_sum)

    def attend(c):
        attend_back_chunk(
            c, heads, r.q, r.k, r.v, r.kt, r.lse, r.self_bias, r.att, r.grad, r.gq, r.dk, r.dv
        )

        def send(t):
            for lag in range(1, cols):
                end = (t * cols + lax.rem(b + lag, cols) + 1) * share

                @pl.when((end <= (c + 1) * CHUNK) & (end > c * CHUNK))
                def _(lag=lag):
                    cross_copy(0, lag, t).start()

        loop(chain, send)

        @pl.when(c < chain - 2)
        def _():
            chain_service(weights, c + 1, side_sum)


    loop(total // CHUNK, attend)

    def finish(c):
        cut = span(c, CHUNK)
        for src, dst in ((r.dk, r.gk), (r.dv, r.gv)):
            parts = [src[h, cut, :HEAD_DIM] for h in range(heads)]
            dst[cut, :] = (jnp.concatenate(parts, axis=1) if heads > 1 else parts[0]).astype(BF)

    loop(total // CHUNK, finish)

    def send_rest(i):
        for k in (1, 2):
            for lag in range(1, cols):
                cross_copy(k, lag, in_order(i)).start()

    loop(chain, send_rest)
    def out_copy(lag):
        return remote(
            done.at[pl.ds(offset(2 + lag), out_rows)],
            r.out_in.at[lag - 1],
            r.so.at[lag],
            r.ro.at[lag],
            (dp, a, lax.rem(b + lag, cols)),
        )

    chain_finish(weights, done, side_sum)
    for lag in range(1, cols):
        out_copy(lag).start()

    small_sum(0, 0)

    def partial_rows(t):
        cut = span(t * cols + b, share)
        value = dot(r.gq[cut, :], r.w[0], NT) + dot(r.gk[cut, :], r.w[1], NT)
        value = value + dot(r.gv[cut, :], r.w[2], NT)
        for slot in range(cols - 1):
            for k in range(3):
                value = value + dot(r.peer_in[slot, k, t], r.peer_w[slot, k], NT)
        return value.astype(BF)

    def bias_rows(c):
        ones = jnp.ones((8, CHUNK), BF)
        for t, src in ((0, r.gq), (1, r.gv)):
            value = dot(ones, src[span(c, CHUNK), :])

            @pl.when(c == 0)
            def _(t=t, value=value):
                r.bias_sum[0, t] = value

            @pl.when(c > 0)
            def _(t=t, value=value):
                r.bias_sum[0, t] += value

    loop(total // CHUNK, bias_rows)
    bias_copy(0).start()

    def head_grads(rows_of):
        def one(t):
            for k in range(3):
                value = dot(rows_of(k, t), r.normed[t], TN)

                @pl.when(t == 0)
                def _(k=k, value=value):
                    r.acc[k] = value

                @pl.when(t > 0)
                def _(k=k, value=value):
                    r.acc[k] += value

        loop(chain, one)

    def head_copy(off):
        return remote(
            r.pool_core.at[pl.ds((off - 1) * 3 * width, 3 * width)],
            r.peer_got.at[off - 1],
            r.sw.at[off],
            r.rw.at[off],
            (dp, a, lax.rem(b - off + cols, cols)),
        )

    def cross_wait(t):
        for k in range(3):
            for lag in range(1, cols):
                cross_copy(k, lag, t).wait_recv()

    def cross_sum(t):
        own = grads[0](t)
        own[...] = partial_rows(t)

    def first_sum(t):
        cross_wait(t)
        cross_sum(t)

    def wait_rest(i):
        @pl.when((i > 0) | ((a > 0) & (a < chain - 1)))
        def _():
            cross_wait(in_order(i))

    chain_service(grads, 0, first_sum)
    for lag in range(1, cols):
        out_copy(lag).wait_recv()
    spot = done.at[pl.ds(offset(2), out_rows)]
    add_rows(spot, spot, *[r.out_in.at[lag - 1] for lag in range(1, cols)])
    weights_keep = []
    for i, flow in enumerate(share_weights):
        for kind in (0, 1):
            share_copy(flow, kind).start()
        weights_keep.append(pltpu.make_async_copy(flow[0], flow[1].at[part], r.sl.at[i]))
        weights_keep[i].start()
    loop(chain, wait_rest)
    chain_service(grads, 1, cross_sum)
    for off in range(1, cols):
        head_grads(lambda k, t: r.peer_in[off - 1, k, t])
        for k in range(3):
            r.pool_core[pl.ds(((off - 1) * 3 + k) * width, width), :] = r.acc[k].astype(BF)
        head_copy(off).start()
    head_grads(lambda k, t: (r.gq, r.gk, r.gv)[k][span(t * cols + b, share), :])
    def later(s, _):
        chain_service(grads, s, cross_sum)
        return 0

    lax.fori_loop(2, chain - 1, later, 0)
    for k in range(3):
        total_k = r.acc[k]
        for off in range(1, cols):
            if k == 0:
                head_copy(off).wait_recv()
            total_k = total_k + r.peer_got[off - 1, pl.ds(k * width, width)].astype(F32)
        local[span(k, width), :] = total_k.astype(BF)

    def local_core(slot):
        return remote(
            local.at[span(far_part if slot else core_part, local_rows)], r.local_in.at[slot], r.st.at[slot], r.rt.at[slot], core_id
        )

    local_side = remote(local.at[span(side_part, local_rows)], r.local_side, r.sy.at[0], r.ry.at[0], side_id)
    for slot in (1, 0):
        local_core(slot).start()
    small_sum(0, 1)
    for slot in (1, 0):
        local_core(slot).wait_recv()
        spot = local.at[span(side_part if slot else part, local_rows)]
        add_rows(spot, spot, r.local_in.at[slot])
        if slot == 1:
            local_side.start()
    bias_copy(0).wait_recv()
    r.bias_sum[1] = r.bias_sum[0] + r.bias_in[0]
    bias_copy(1).start()
    for flow in share_weights:
        share_copy(flow, 0, arriving=True).wait_recv()
        share_copy(flow, 2).start()
    local_side.wait_recv()
    bias_copy(1).wait_recv()
    r.bias_out[...] = r.bias_sum[1] + r.bias_in[1]
    add_rows(local_done, local.at[span(part, local_rows)], r.local_side)
    for kind in (0, 1):
        share_copy(share_local, kind).start()
    local_keep = pltpu.make_async_copy(local_done, r.head_sum.at[part], r.sl.at[3])
    local_keep.start()
    chain_finish(grads, r.gn, cross_sum)
    step = 32 if share % 32 == 0 else 16

    def norm_back(i, sums):
        cut = span(i, step)
        values = r.tokens[cut, :].astype(F32)
        grad = r.gn[cut, :]
        centered = values - jnp.mean(values, axis=-1, keepdims=True)
        scale = lax.rsqrt(jnp.mean(centered * centered, axis=-1, keepdims=True) + epsilon)
        unit = centered * scale
        scaled = grad * r.gain[...]
        along = jnp.mean(scaled * unit, axis=-1, keepdims=True)
        back = (scaled - jnp.mean(scaled, axis=-1, keepdims=True) - unit * along) * scale
        r.input_grad[cut, :] = (r.grad_hidden[cut, :] + back).astype(BF)
        gains = jnp.sum(grad * unit, axis=0, keepdims=True)
        return sums[0] + gains, sums[1] + jnp.sum(grad, axis=0, keepdims=True)

    zero = jnp.zeros((1, model), F32)
    gains, shifts = lax.fori_loop(0, share // step, norm_back, (zero, zero))
    upper = lax.broadcasted_iota(jnp.int32, (8, model), 0) == 0
    r.small[1, 0] = jnp.where(upper, gains, shifts)
    small_start(1, 0)
    small_sum(0, 2)
    share_copy(share_local, 0, arriving=True).wait_recv()
    share_copy(share_local, 2).start()
    for stage in range(3):
        small_sum(1, stage)

    for copy in weights_keep:
        copy.wait()
    local_keep.wait()
    for flow in share_weights + [share_local]:
        for kind in range(3):
            share_copy(flow, kind).wait_send()
            if kind > 0:
                share_copy(flow, kind, arriving=True).wait_recv()
    for slot in (1, 0):
        local_core(slot).wait_send()
    local_side.wait_send()
    for off in range(1, cols):
        head_copy(off).wait_send()
        out_copy(off).wait_send()
    for stage in range(2):
        bias_copy(stage).wait_send()
    for which in range(2):
        for stage in range(3):
            for copy in small_copies(which, stage):
                copy.wait_send()
    others(lambda m: row_copy(m, me).wait_send())
    chain_drain(weights)
    chain_drain(grads)

    def drain(t):
        side_copy(t).wait_send()
        for slot in (1, 0):
            for k in range(2 + cols):
                core_copy(t, slot, k).wait_send()
        for lag in range(1, cols):
            for k in range(3):
                cross_copy(k, lag, t).wait_send()

    loop(chain, drain)


def rear(
    n, grad_rows, q_ext, k_ext, v_ext, lse, self_bias, attended, w_qkv, peer_w, normed, tokens, grad_hidden, gain,
    early, grad_up, grad_down, grad_out,
):
    chain, cols = mp_parts(n)
    heads, total, _ = q_ext.shape
    _, share, width = grad_rows.shape
    model = w_qkv.shape[1]
    rows = 2 * (grad_up.shape[0] // chain // PARTS)
    block = rows + cols * width // PARTS
    local = 3 * width // PARTS
    vmem = pl.BlockSpec(memory_space=pltpu.VMEM)
    anywhere = pl.BlockSpec(memory_space=pl.ANY)
    dma = pltpu.SemaphoreType.DMA
    head = pltpu.VMEM((total, width), BF)
    most = max(chain, cols, PARTS) - 1
    return pl.pallas_call(
        functools.partial(rear_kernel, n),
        name="rear",
        out_shape=(
            jax.ShapeDtypeStruct((PARTS, rows // 2, model), BF),
            jax.ShapeDtypeStruct((PARTS, rows // 2, model), BF),
            jax.ShapeDtypeStruct((PARTS, width // PARTS, model), BF),
            jax.ShapeDtypeStruct((PARTS, local, model), BF),
            jax.ShapeDtypeStruct((2, 8, width), F32),
            jax.ShapeDtypeStruct((share, model), BF),
            jax.ShapeDtypeStruct((2, 8, model), F32),
        ),
        in_specs=[vmem] * 14 + [anywhere] * 3,
        out_specs=(anywhere,) * 4 + (vmem,) * 3,
        scratch_shapes=[
            head,
            pltpu.VMEM((heads, LANES, total), BF),
            pltpu.VMEM((heads, total, LANES), F32),
            pltpu.VMEM((heads, total, LANES), F32),
            head,
            head,
            head,
            pltpu.VMEM((chain, 2, block, model), BF),
            pltpu.VMEM((chain * 2 * block, model), BF),
            pltpu.VMEM((chain * max(block, share), model), BF),
            pltpu.VMEM((2, chain, block, model), BF),
            pltpu.VMEM((cols - 1, width // PARTS, model), BF),
            pltpu.VMEM((2, local, model), BF),
            pltpu.VMEM((local, model), BF),
            pltpu.VMEM((3, width, model), F32),
            pltpu.VMEM((cols - 1, 3, chain, share, width), BF),
            pltpu.VMEM((cols - 1, 3 * width, model), BF),
            pltpu.VMEM((2, chain, share, model), BF),
            pltpu.VMEM((share, model), F32),
            pltpu.VMEM((2, 3, 8, model), F32),
            pltpu.VMEM((2, 3, most, 8, model), F32),
            pltpu.VMEM((2, 2, 8, width), F32),
            pltpu.VMEM((2, 2, 8, width), F32),
            dma((n,)),
            dma((n,)),
            dma((cols,)),
            dma((cols,)),
            dma((chain, 2, 2 + cols)),
            dma((chain, 2, 2 + cols)),
            dma((chain, 2, 2 + cols)),
            dma((chain,)),
            dma((chain,)),
            dma((2, chain)),
            dma((2, chain)),
            dma((3, 3)),
            dma((3, 3)),
            dma((2,)),
            dma((2,)),
            dma((1,)),
            dma((1,)),
            dma((3,)),
            dma((3,)),
            dma((3, cols, chain)),
            dma((3, cols, chain)),
            dma((cols,)),
            dma((cols,)),
            dma((2, chain)),
            dma((2, chain)),
            dma((2, 3, most)),
            dma((2, 3, most)),
            dma((2,)),
            dma((2,)),
            dma((4,)),
        ],
        compiler_params=pltpu.CompilerParams(
            collective_id=1, has_side_effects=True, vmem_limit_bytes=VMEM_BYTES
        ),
    )(
        grad_rows, q_ext, k_ext, v_ext, lse, self_bias, attended, w_qkv, peer_w, normed, tokens, grad_hidden,
        gain[None, :], early, grad_up, grad_down, grad_out,
    )


def body(
    n,
    groups,
    tokens,
    image_ids,
    lengths,
    w_qkv,
    bias_query,
    bias_value,
    w_out,
    w_up,
    bias_up,
    w_down,
    out_biases,
    norm_gain,
    norm_bias,
    cotangent,
):
    share_rows = tokens.shape[0]
    a, b = lax.axis_index("mz"), lax.axis_index("mx")
    chain, cols = mp_parts(n)
    model_index = a * cols + b
    model, hidden = w_up.shape
    width = w_out.shape[0]

    def shifted(values, off):
        return lax.ppermute(values, "mx", [(i, (i + off) % cols) for i in range(cols)])

    def pair_sum(partial):
        spans = [slice(off * share_rows, (off + 1) * share_rows) for off in range(cols)]
        got = [shifted(partial(spans[off]).astype(BF), cols - off) for off in range(1, cols)]
        total = partial(spans[0])
        for part in got:
            total = total + part.astype(F32)
        return total

    (
        gathered_one, q_ext, k_ext, v_ext, log_totals, attended, owned,
        up_all, down_all, out_all, bias_all, peer_w, self_bias, hidden_one, rows_two, grad_mlp,
    ) = front(
        n,
        image_ids,
        lengths,
        tokens,
        cotangent,
        norm_gain,
        norm_bias,
        out_biases,
        w_qkv,
        bias_query,
        bias_value,
        w_up,
        w_down,
        w_out,
        bias_up,
    )
    grad_out = grad_mlp[0].astype(F32)
    rows_two = rows_two.reshape(cols * share_rows, model)
    grad_mlp = grad_mlp.reshape(cols * share_rows, model)
    owned = jnp.transpose(owned, (1, 0, 2)).reshape(share_rows, -1)
    bias_all = bias_all[:, 0].reshape(-1)
    pre_act = jnp.dot(rows_two, up_all, preferred_element_type=F32) + bias_all
    below, density = gelu_parts(pre_act)
    activated = (pre_act * below).astype(BF)
    grad_act = jnp.einsum("rd,fd->rf", grad_mlp, down_all, preferred_element_type=F32)
    grad_pre = (grad_act * (below + pre_act * density)).astype(BF)
    grad_normed_two = pair_sum(
        lambda cut: jnp.einsum("rf,df->rd", grad_pre[cut], up_all, preferred_element_type=F32)
    )
    output_full = (
        hidden_one
        + pair_sum(lambda cut: jnp.dot(activated[cut], down_all, preferred_element_type=F32))
        + out_biases[1]
    )
    grad_up_all = jnp.einsum("rf,rd->fd", grad_pre, rows_two, preferred_element_type=F32)
    grad_down_all = jnp.einsum("rf,rd->fd", activated, grad_mlp, preferred_element_type=F32)
    grad_bias_up = jnp.sum(grad_pre, axis=0, dtype=F32)

    _, norm_two_back = jax.vjp(layer_norm, hidden_one, norm_gain[1], norm_bias[1])
    grad_from_two, gain_two, shift_two = norm_two_back(grad_normed_two)
    grad_hidden = grad_out + grad_from_two
    grad_proj = grad_hidden.astype(BF)
    grad_w_out = jnp.einsum("re,rd->ed", owned, grad_proj, preferred_element_type=F32).astype(BF)
    grad_rows = jnp.einsum(
        "rd,ned->nre", grad_proj, out_all.reshape(n, width, model), preferred_element_type=F32
    ).astype(BF)
    bias_rows = lax.dynamic_update_slice(
        jnp.zeros((chain, cols, hidden), F32), grad_bias_up.reshape(chain, 1, hidden), (0, b, 0)
    )
    early = [gain_two, shift_two, jnp.sum(grad_hidden, axis=0), jnp.sum(grad_out, axis=0)]
    early = jnp.concatenate([jnp.stack(early), bias_rows.reshape(-1, model)])
    up_sum, down_sum, out_sum, head_sum, bias_sum, input_grad, small = rear(
        n,
        grad_rows,
        q_ext,
        k_ext,
        v_ext,
        log_totals,
        self_bias,
        attended,
        w_qkv,
        peer_w,
        gathered_one,
        tokens,
        grad_hidden,
        norm_gain[0],
        early,
        grad_up_all.astype(BF),
        grad_down_all.astype(BF),
        grad_w_out.reshape(n, width, model),
    )
    if groups > 1:
        up_sum, down_sum, out_sum, head_sum, bias_sum, small = lax.psum(
            (up_sum, down_sum, out_sum, head_sum, bias_sum, small), "dg"
        )
    grad_w_up = up_sum.reshape(hidden, model).T.astype(F32)
    grad_w_down = down_sum.reshape(hidden, model).astype(F32)
    grad_w_out = out_sum.reshape(width, model).astype(F32)
    grad_w_qkv = jnp.transpose(head_sum.reshape(3, width, model), (0, 2, 1)).astype(F32)
    grad_bias_query, grad_bias_value = bias_sum[:, 0]
    grad_bias_up = lax.dynamic_slice_in_dim(
        small[0, 4:].reshape(-1), model_index * hidden, hidden, 0
    )
    return (
        output_full.astype(BF),
        input_grad,
        grad_w_qkv,
        grad_bias_query,
        grad_bias_value,
        grad_w_out,
        grad_w_up,
        grad_bias_up,
        grad_w_down,
        small[0, 2:4],
        jnp.stack([small[1, 0], small[0, 0]]),
        jnp.stack([small[1, 1], small[0, 1]]),
    )


def solution(mesh):
    n = mesh.shape["mp"]
    chain, cols = mp_parts(n)
    groups = mesh.shape["dp"] // PARTS
    dp, mp = ("dg", "dp"), ("mz", "mx")
    every = dp + mp
    split = jax.sharding.Mesh(mesh.devices.reshape(groups, PARTS, chain, cols), every)
    in_specs = (
        P(every, None),
        P(dp),
        P(dp, None),
        P(None, None, mp),
        P(mp),
        P(mp),
        P(mp, None),
        P(None, mp),
        P(mp),
        P(mp, None),
        P(),
        P(),
        P(),
        P(every, None),
    )
    out_specs = (
        P(every, None),
        P(every, None),
        P(None, None, mp),
        P(mp),
        P(mp),
        P(mp, None),
        P(None, mp),
        P(mp),
        P(mp, None),
        P(),
        P(),
        P(),
    )
    return jax.shard_map(
        functools.partial(body, n, groups),
        mesh=split,
        in_specs=in_specs,
        out_specs=out_specs,
        check_vma=False,
    )
```
